512 devices in a mesh: gx: 4 (over x), gy: 8 (over y, core), gz: 16 (over z).
Axes of the slice: x: 4, y: 4, z: 16, core: 2. Of those that a mesh axis runs over, the one named last changes fastest.
Arguments:
- positions: float32 [3, 4, 8, 16, 128], P(None, 'gx', 'gy', 'gz'), may hold values from 0 to 1
- basis: float32 [30, 3, 4, 8, 16, 128], P(None, None, 'gx', 'gy', 'gz'), may hold values from -10 to 10, as said below
- neighbours: int32 [4, 8, 16, 128, 128], P('gx', 'gy', 'gz'), may hold values from 0 to 511
- used_count: int32 [4, 8, 16, 128], P('gx', 'gy', 'gz'), may hold values from 42 to 128
- kinds: int32 [4, 8, 16, 128], P('gx', 'gy', 'gz'), may hold values from 0 to 1
- map_x: int32 [4, 8, 16, 2, 64], P('gx', 'gy', 'gz'), may hold values from 0 to 127
- map_y: int32 [4, 8, 16, 2, 64], P('gx', 'gy', 'gz'), may hold values from 0 to 255
- map_z: int32 [4, 8, 16, 2, 64], P('gx', 'gy', 'gz'), may hold values from 0 to 383
- table: float32 [2, 16, 100], replicated, may hold values from -6 to 6
- fit_w1: float32 [1600, 240], replicated, may hold values from -0.15625 to 0.15625
- fit_b1: float32 [240], replicated, may hold values from -3 to 3
- fit_w2: float32 [240, 240], replicated, may hold values from -0.375 to 0.375
- fit_b2: float32 [240], replicated, may hold values from -3 to 3
- fit_out: float32 [240], replicated, may hold values from -0.375 to 0.375
Outputs:
- next_vector: float32 [3, 4, 8, 16, 128], P(None, 'gx', 'gy', 'gz')
- correlations: float32 [30], replicated
- vector_norm: float32 [], replicated
The draws below stay inside these ranges and needn't reach their ends.
Inputs may be any that keep to these rules, and one draw needn't show every extreme that they name: `basis`: entries of order one; the stored vectors' magnitude varies from brick to brick.
All inputs are finite; a program needn't handle non-finite values.
Results may differ from the reference program's by a relative error of at most 0.0003.
Values sent between devices are 32-bit elements; how exact they have to be, the bound alone decides.
No kernel may reach another device: no remote copies, remote signals or barrier semaphores. Data moves between devices by JAX's collectives and lax.ppermute only.
A program may use at most 64 MiB of HBM per device.

```python
import jax
import jax.numpy as jnp
from jax import lax

ATOMS_DEV = 128
NNEI = 128
NBASIS = 16
M1 = 100
M2 = 16
FIT = 240
NTYPES = 2
KVEC = 30
GRID_X = 4
GRID_Y = 8
GRID_Z = 16
GHOST = 64
EXT = 512


def draw_basis(key, part):
    first_key, second_key, third_key = jax.random.split(jax.random.fold_in(key, 17), 3)
    shape = (KVEC, 3, GRID_X, GRID_Y, GRID_Z, ATOMS_DEV)
    bricks = GRID_X * GRID_Y * GRID_Z
    order = jnp.arange(bricks, dtype=jnp.float32).reshape(1, 1, GRID_X, GRID_Y, GRID_Z, 1)
    fraction = order / max(bricks - 1, 1)
    private = jax.random.truncated_normal(first_key, -3.0, 3.0, shape, jnp.float32)
    shared = jax.random.truncated_normal(second_key, -3.0, 3.0, shape[1:], jnp.float32)
    magnitude = 0.5 * jnp.exp(fraction * jnp.log(4.0))
    mixing = jax.random.uniform(third_key, (KVEC,), jnp.float32, 0.3, 0.9).reshape(KVEC, 1, 1, 1, 1, 1)
    values = (private * jnp.sqrt(1.0 - mixing * mixing) + mixing * shared[None]) * magnitude
    return values.astype(jnp.float32)


def touch_ends(values, key, least, top_value):
    dims = values.shape
    place = [jax.random.randint(jax.random.fold_in(key, axis), (), 0, dims[axis]) for axis in range(len(dims))]
    values = values.at[tuple(place)].set(least)
    longest = dims.index(max(dims))
    place[longest] = (place[longest] + 1) % dims[longest]
    return values.at[tuple(place)].set(top_value)


def block_levels(rng, extent, pieces, smallest, largest):
    gain = 1.0
    for axis_at, shards_of in pieces:
        heights = jax.random.uniform(jax.random.fold_in(jax.random.fold_in(rng, 6), axis_at), (shards_of,), jnp.float32, smallest / len(pieces), largest / len(pieces))
        gain = gain * jnp.repeat(jnp.exp(heights), extent[axis_at] // shards_of).reshape((-1,) + (1,) * (len(extent) - 1 - axis_at))
    return gain


def normal_values(rng, shape, width, reach, kind=jnp.bfloat16):
    return jnp.clip(width * jax.random.normal(rng, shape, jnp.float32), -reach, reach).astype(kind)


def setup_inputs(seed: int = 0) -> dict:
    streams_of = jax.random.split(jax.random.key(seed), 15)
    return {
        "positions": jnp.clip(1.0 * jax.random.uniform(streams_of[0], (3, GRID_X, GRID_Y, GRID_Z, ATOMS_DEV), jnp.float32) ** block_levels(streams_of[0], (3, GRID_X, GRID_Y, GRID_Z, ATOMS_DEV), ((1, 4), (2, 8), (3, 16)), -0.2, 0.2), 0.0, 1.0),
        "basis": draw_basis(jax.random.fold_in(streams_of[14], 71), 0),
        "neighbours": touch_ends(jax.random.randint(streams_of[2], (GRID_X, GRID_Y, GRID_Z, ATOMS_DEV, NNEI), 0, EXT), jax.random.fold_in(streams_of[2], 1), 0, EXT - 1).astype(jnp.int32),
        "used_count": touch_ends(jax.random.randint(streams_of[3], (GRID_X, GRID_Y, GRID_Z, ATOMS_DEV), NNEI // 3, NNEI + 1), jax.random.fold_in(streams_of[3], 1), NNEI // 3, NNEI).astype(jnp.int32),
        "kinds": touch_ends(jax.random.randint(streams_of[4], (GRID_X, GRID_Y, GRID_Z, ATOMS_DEV), 0, NTYPES), jax.random.fold_in(streams_of[4], 1), 0, NTYPES - 1).astype(jnp.int32),
        "map_x": touch_ends(jax.random.randint(streams_of[5], (GRID_X, GRID_Y, GRID_Z, 2, GHOST), 0, ATOMS_DEV), jax.random.fold_in(streams_of[5], 1), 0, ATOMS_DEV - 1).astype(jnp.int32),
        "map_y": touch_ends(jax.random.randint(streams_of[6], (GRID_X, GRID_Y, GRID_Z, 2, GHOST), 0, ATOMS_DEV + 2 * GHOST), jax.random.fold_in(streams_of[6], 1), 0, (ATOMS_DEV + 2 * GHOST) - 1).astype(jnp.int32),
        "map_z": touch_ends(jax.random.randint(streams_of[7], (GRID_X, GRID_Y, GRID_Z, 2, GHOST), 0, ATOMS_DEV + 4 * GHOST), jax.random.fold_in(streams_of[7], 1), 0, (ATOMS_DEV + 4 * GHOST) - 1).astype(jnp.int32),
        "table": normal_values(streams_of[8], (NTYPES, NBASIS, M1), 1.0, 6.0, jnp.float32),
        "fit_w1": normal_values(streams_of[9], (M1 * M2, FIT), (M1 * M2) ** -0.5, 0.15625, jnp.float32),
        "fit_b1": normal_values(streams_of[10], (FIT,), 0.5, 3.0, jnp.float32),
        "fit_w2": normal_values(streams_of[11], (FIT, FIT), FIT ** -0.5, 0.375, jnp.float32),
        "fit_b2": normal_values(streams_of[12], (FIT,), 0.5, 3.0, jnp.float32),
        "fit_out": normal_values(streams_of[13], (FIT,), FIT ** -0.5, 0.375, jnp.float32),
    }


def site_energy(centre, around, filled, onehot, table, fit_w1, fit_b1, fit_w2, fit_b2, fit_out):
    highest = lax.Precision.HIGHEST
    offsets = around - centre[:, :, None]
    square = lax.optimization_barrier(jnp.sum(offsets * offsets, axis=0))
    radius = jnp.sqrt(square + 0.01)
    smooth = jnp.exp(-square) / radius * filled
    radial = jnp.concatenate([smooth[None], smooth[None] * offsets / radius[None]], axis=0)
    scaled = smooth / (1.0 + smooth)
    levels = table.shape[1]
    centres = jnp.arange(levels, dtype=jnp.float32) / (levels - 1)
    spread = (scaled[:, None, :] - centres[None, :, None]) * (levels - 1)
    profile = jnp.exp(-spread * spread)
    pooled = jnp.einsum('bkn,abn->bka', profile, radial, precision=highest) / around.shape[2]
    tables = jnp.einsum('bt,tkm->bkm', onehot, table, precision=highest)
    environment = jnp.einsum('bkm,bka->bma', tables, pooled, precision=highest)
    descriptor = jnp.einsum('bma,bna->bmn', environment, environment[:, :M2], precision=highest)
    descriptor = descriptor.reshape(descriptor.shape[0], -1)
    first_layer = jnp.tanh(jnp.dot(descriptor, fit_w1, precision=highest) + fit_b1)
    second_layer = jnp.tanh(jnp.dot(first_layer, fit_w2, precision=highest) + fit_b2) + first_layer
    return jnp.sum(jnp.dot(second_layer, fit_out, precision=highest))

def device_hvp(ext_places, ext_tangent, neighbour_ids, counts, species, weights):
    atom_count = neighbour_ids.shape[0]
    block_rows = min(atom_count, 128)
    slots = jnp.arange(neighbour_ids.shape[1], dtype=jnp.int32)
    type_ids = jnp.arange(weights[0].shape[0], dtype=jnp.int32)

    def one_block(counter, summed):
        offset = (counter * block_rows).astype(jnp.int32)
        block_ids = lax.dynamic_slice_in_dim(neighbour_ids, offset, block_rows, 0)
        block_counts = lax.dynamic_slice_in_dim(counts, offset, block_rows, 0)
        block_species = lax.dynamic_slice_in_dim(species, offset, block_rows, 0)
        filled = (slots[None, :] < block_counts[:, None]).astype(jnp.float32)
        onehot = (block_species[:, None] == type_ids[None, :]).astype(jnp.float32)

        def energy(places):
            centre = lax.dynamic_slice_in_dim(places, offset, block_rows, 1)
            return site_energy(centre, places[:, block_ids], filled, onehot, *weights)
        return summed + jax.jvp(jax.grad(energy), (ext_places,), (ext_tangent,))[1]
    zeros = jnp.zeros(ext_places.shape, jnp.float32)
    return lax.fori_loop(0, atom_count // block_rows, one_block, zeros)

def take_rows(values, indices):
    wide = jnp.broadcast_to(indices[None], (values.shape[0],) + indices.shape)
    return jnp.take_along_axis(values, wide, axis=-1)

def extend(places, tangent, maps, axis, coord):
    displace = (jnp.arange(3) == coord).astype(jnp.float32).reshape(3, 1, 1, 1, 1)
    down_places = take_rows(places, maps[..., 0, :])
    up_places = take_rows(places, maps[..., 1, :])
    down_tangent = take_rows(tangent, maps[..., 0, :])
    up_tangent = take_rows(tangent, maps[..., 1, :])
    places = jnp.concatenate([places, jnp.roll(up_places, 1, axis) - displace, jnp.roll(down_places, -1, axis) + displace], axis=-1)
    tangent = jnp.concatenate([tangent, jnp.roll(up_tangent, 1, axis), jnp.roll(down_tangent, -1, axis)], axis=-1)
    return (places, tangent)

def add_one(target, indices, values):
    return target.at[:, indices].add(values)

def add_rows(target, indices, values):
    return jax.vmap(add_one, in_axes=(1, 0, 1), out_axes=1)(target, indices, values)

def reverse_section(contributions, maps, axis, current):
    ghosts = maps.shape[-1]
    bricks = GRID_X * GRID_Y * GRID_Z
    holder = contributions[..., :current]
    lower_part = contributions[..., current:current + ghosts]
    upper_part = contributions[..., current + ghosts:]
    from_below = jnp.roll(upper_part, 1, axis).reshape(3, bricks, ghosts)
    from_above = jnp.roll(lower_part, -1, axis).reshape(3, bricks, ghosts)
    flat = holder.reshape(3, bricks, current)
    flat = add_rows(flat, maps[..., 0, :].reshape(bricks, ghosts), from_below)
    flat = add_rows(flat, maps[..., 1, :].reshape(bricks, ghosts), from_above)
    return flat.reshape(holder.shape)

def reference(positions, basis, neighbours, used_count, kinds, map_x, map_y, map_z, table, fit_w1, fit_b1, fit_w2, fit_b2, fit_out):
    highest = lax.Precision.HIGHEST
    places = positions
    tangent = basis[KVEC - 1]
    places, tangent = extend(places, tangent, map_x, 1, 0)
    places, tangent = extend(places, tangent, map_y, 2, 1)
    places, tangent = extend(places, tangent, map_z, 3, 2)
    bricks = GRID_X * GRID_Y * GRID_Z
    extended = places.shape[-1]
    flat_places = jnp.transpose(places.reshape(3, bricks, extended), (1, 0, 2))
    flat_tangent = jnp.transpose(tangent.reshape(3, bricks, extended), (1, 0, 2))
    flat_ids = neighbours.reshape(bricks, ATOMS_DEV, NNEI)
    flat_counts = used_count.reshape(bricks, ATOMS_DEV)
    flat_species = kinds.reshape(bricks, ATOMS_DEV)
    weights = (table, fit_w1, fit_b1, fit_w2, fit_b2, fit_out)

    def per_brick(packed):
        return device_hvp(packed[0], packed[1], packed[2], packed[3], packed[4], weights)
    products = lax.map(per_brick, (flat_places, flat_tangent, flat_ids, flat_counts, flat_species))
    products = jnp.transpose(products, (1, 0, 2)).reshape(3, GRID_X, GRID_Y, GRID_Z, extended)
    products = reverse_section(products, map_z, 3, ATOMS_DEV + 4 * GHOST)
    products = reverse_section(products, map_y, 2, ATOMS_DEV + 2 * GHOST)
    products = reverse_section(products, map_x, 1, ATOMS_DEV)
    entries = 3 * ATOMS_DEV * bricks
    stored = basis.reshape(KVEC, -1)
    hessian_vec = products.reshape(-1)
    correlations = jnp.dot(stored, hessian_vec, precision=highest) / entries
    residual = hessian_vec - jnp.dot(correlations, stored, precision=highest)
    vector_norm = jnp.sqrt(jnp.sum(residual * residual) / entries + 1e-06)
    next_vector = (residual / vector_norm).reshape(positions.shape)
    return (next_vector, correlations, vector_norm)
```

```python
import functools

import jax
import jax.numpy as jnp
from jax import lax
from jax.experimental import pallas as pl
from jax.experimental.pallas import tpu as pltpu
from jax.sharding import PartitionSpec as P

F32 = jnp.float32
BF16 = jnp.bfloat16
LOG2E = 1.4426950408889634
NT = (((1,), (1,)), ((), ()))


def split(x):
    hi = x.astype(BF16)
    return hi, (x - hi.astype(F32)).astype(BF16)


def mm(a, b):
    return jnp.dot(a, b, preferred_element_type=F32)


def dot3(a, b):
    ah, al = a if isinstance(a, tuple) else split(a)
    bh, bl = b if isinstance(b, tuple) else split(b)
    return mm(ah, bh) + (mm(ah, bl) + mm(al, bh))


def lane_pick(table, index):
    return jnp.take_along_axis(table, index, axis=1, mode="promise_in_bounds")


def rows_of(shape, dim=0):
    return lax.broadcasted_iota(jnp.int32, shape, dim)


def prepare_kernel(table, w1, w2, b1, b2, wo, ids, u_hi, u_lo, ut_hi, ut_lo, w2_hi, w2_lo, w2t_hi, w2t_lo, cols, ids_t, ws, ys, us, pad):
    types, levels, width = table.shape
    hidden = w1.shape[1]
    inner = levels * levels
    m2 = w1.shape[0] // width
    rest = hidden - 128
    tall = split(table[...].reshape(types * levels, width))
    ws[0] = w1[:, 0:128]
    ws[1] = jnp.zeros_like(ws[1])
    ws[1, :, 0:rest] = w1[:, 128:hidden]
    for j in range(m2):
        column = jnp.concatenate([ws[0, pl.ds(j, width, stride=m2), :], ws[1, pl.ds(j, width, stride=m2), :]], axis=1)
        part = dot3(tall, column)
        for t in range(types):
            for half in range(2):
                ys[t, half, pl.ds(j, levels, stride=m2), :] = part[t * levels : (t + 1) * levels, half * 128 : (half + 1) * 128]
    r = rows_of((inner, levels))
    spread = (r % levels == rows_of((inner, levels), 1)).astype(BF16)
    r = rows_of((m2, levels * m2), 1)
    tile = (r % m2 == rows_of((m2, levels * m2))).astype(BF16)
    same = rows_of((inner, levels * m2)) // levels == rows_of((inner, levels * m2), 1) // m2
    for t in range(types):
        th, tl = split(table[t][:, 0:m2])
        kh = mm(mm(spread, th).astype(BF16), tile)
        kl = mm(mm(spread, tl).astype(BF16), tile)
        kron = (jnp.where(same, kh, 0.0).astype(BF16), jnp.where(same, kl, 0.0).astype(BF16))
        for half in range(2):
            us[half, t * inner : (t + 1) * inner, :] = dot3(kron, ys[t, half])
    for t in range(types):
        for k in range(levels):
            at = t * inner + k * levels
            for half in range(2):
                block = us[half, at : at + levels, :]
                other = us[half, pl.ds(t * inner + k, levels, stride=levels), :]
                hi, lo = split(0.5 * (block + other))
                u_hi[at : at + levels, half * 128 : (half + 1) * 128] = hi
                u_lo[at : at + levels, half * 128 : (half + 1) * 128] = lo
    full = u_hi[...].astype(F32) + u_lo[...].astype(F32)
    hi, lo = split(full.T)
    ut_hi[...] = hi
    ut_lo[...] = lo
    pad[...] = jnp.zeros_like(pad)
    pad[0:hidden, 0:hidden] = w2[...]
    hi, lo = split(pad[...])
    w2_hi[...] = hi
    w2_lo[...] = lo
    hi, lo = split(pad[...].T)
    w2t_hi[...] = hi
    w2t_lo[...] = lo
    pad[...] = jnp.zeros_like(pad)
    pad[0:1, 0:hidden] = b1[...]
    pad[1:2, 0:hidden] = b2[...]
    pad[2:3, 0:hidden] = wo[...]
    cols[...] = pad[0:128, :].T
    ids_t[...] = ids[0, 0, 0].astype(F32).T.astype(jnp.int32)


def vmem(n):
    return [pl.BlockSpec(memory_space=pltpu.VMEM)] * n


def prepare(table, w1, w2, b1, b2, wo, ids):
    n = ids.shape[-1]
    hp = 256
    inner = table.shape[0] * table.shape[1] ** 2
    shapes = [((inner, hp), BF16)] * 2 + [((hp, inner), BF16)] * 2 + [((hp, hp), BF16)] * 4 + [((hp, 128), F32), ((n, 128), jnp.int32)]
    return pl.pallas_call(
        prepare_kernel,
        out_shape=[jax.ShapeDtypeStruct(s, d) for s, d in shapes],
        in_specs=vmem(7),
        out_specs=vmem(len(shapes)),
        scratch_shapes=[
            pltpu.VMEM((2, w1.shape[0], 128), F32),
            pltpu.VMEM((table.shape[0], 2, inner // table.shape[0], 128), F32),
            pltpu.VMEM((2, inner, 128), F32),
            pltpu.VMEM((hp, hp), F32),
        ],
        name="prepare",
    )(table, w1, w2, b1[None], b2[None], wo[None], ids)


def shifted_ghosts(below, above, coord, rows):
    lower = rows_of((rows, 128), 1) < 64
    step = jnp.where(rows_of((rows, 128)) == coord, 1.0, 0.0)
    return jnp.where(lower, below - step, above + step)


def product_kernel(tiles, below, above, ids_t, counts, kinds, u_hi, u_lo, ut_hi, ut_lo, w2_hi, w2_lo, w2t_hi, w2t_lo, cols, out, xv, edge, phis, acc, pairs, grads, force, lows):
    n_slots = ids_t.shape[0]
    levels = 16
    gap = levels - 1
    blocks = n_slots // 8
    xv[0:3] = tiles[...]
    xv[3] = shifted_ghosts(pltpu.roll(below[...], 64, 1), pltpu.roll(above[...], 64, 1), 2, 8)
    count_row = jnp.broadcast_to(counts[0, 0], (8, 128))

    def geometry(nb, carry):
        rows = pl.ds(pl.multiple_of(nb * 8, 8), 8)
        index = ids_t[rows, :]
        low = index & 127
        high = index >> 7
        lows[rows, :] = low.astype(F32)
        near = []
        for f in range(6):
            picks = [lane_pick(jnp.broadcast_to(xv[q, f : f + 1, :], (8, 128)), low) for q in range(4)]
            value = jnp.where(high < 2, jnp.where(high == 0, picks[0], picks[1]), jnp.where(high == 2, picks[2], picks[3]))
            near.append(value - jnp.broadcast_to(xv[0, f : f + 1, :], (8, 128)))
        d, dd = near[:3], near[3:]
        square = d[0] * d[0] + d[1] * d[1] + d[2] * d[2]
        rate = 2.0 * (d[0] * dd[0] + d[1] * dd[1] + d[2] * dd[2])
        wide = square + 0.01
        inverse = lax.rsqrt(wide)
        half = 0.5 / wide
        live = (rows_of((8, 128)) + nb * 8) < count_row
        s = jnp.where(live, jnp.exp(-square) * inverse, 0.0)
        tau = s * inverse
        sq = -s * (1.0 + half)
        tq = -tau * (1.0 + 2.0 * half)
        share = 1.0 / (1.0 + s)
        us = gap * share * share
        for c in range(3):
            edge[c, rows, :] = d[c]
            edge[3 + c, rows, :] = dd[c]
            edge[9 + c, rows, :] = tau * d[c]
            edge[13 + c, rows, :] = tq * rate * d[c] + tau * dd[c]
        edge[6, rows, :] = gap * s * share
        edge[7, rows, :] = us * sq * rate
        edge[8, rows, :] = s
        edge[12, rows, :] = sq * rate
        edge[16, rows, :] = tau
        edge[17, rows, :] = half
        edge[18, rows, :] = rate
        return carry

    lax.fori_loop(0, blocks, geometry, 0)

    def pooling(kk, carry):
        sums = [[jnp.zeros((8, 128), F32) for _ in range(8)] for _ in range(2)]
        for nb in range(blocks):
            rows = pl.ds(nb * 8, 8)
            u = edge[6, rows, :]
            w = -2.0 * edge[7, rows, :]
            radial = [edge[8 + a, rows, :] for a in range(4)]
            moved = [edge[12 + a, rows, :] for a in range(4)]
            for side in range(2):
                z = u - (2 * kk + side).astype(F32)
                phi = jnp.exp2(z * (z * (-LOG2E)))
                phis[2 * kk + side, rows, :] = phi
                dphi = phi * (z * w)
                for a in range(4):
                    sums[side][a] = sums[side][a] + phi * radial[a]
                    sums[side][4 + a] = sums[side][4 + a] + (dphi * radial[a] + phi * moved[a])
        for side in range(2):
            for a in range(8):
                acc[pl.ds(pl.multiple_of((a * levels + 2 * kk + side) * 8, 8), 8), :] = sums[side][a]
        return carry

    lax.fori_loop(0, levels // 2, pooling, 0)
    pooled = acc[pl.ds(0, 128, stride=8), :]
    for s in range(1, 8):
        pooled = pooled + acc[pl.ds(s, 128, stride=8), :]
    pooled = pooled * (1.0 / n_slots)
    grads[...] = pooled
    second = jnp.broadcast_to(kinds[0, 0], (16, 128)) == 1
    p = [pooled[a * 16 : (a + 1) * 16] for a in range(4)]
    dp = [pooled[64 + a * 16 : 64 + (a + 1) * 16] for a in range(4)]
    for k in range(levels):
        value = jnp.zeros((16, 128), F32)
        moved = jnp.zeros((16, 128), F32)
        for a in range(4):
            value = value + p[a] * jnp.broadcast_to(grads[a * 16 + k : a * 16 + k + 1, :], (16, 128))
            moved = moved + p[a] * jnp.broadcast_to(grads[64 + a * 16 + k : 64 + a * 16 + k + 1, :], (16, 128))
        moved = 2.0 * moved
        pairs[k * 16 : (k + 1) * 16, 0:128] = jnp.where(second, 0.0, value)
        pairs[k * 16 : (k + 1) * 16, 128:256] = jnp.where(second, 0.0, moved)
        pairs[256 + k * 16 : 256 + (k + 1) * 16, 0:128] = jnp.where(second, value, 0.0)
        pairs[256 + k * 16 : 256 + (k + 1) * 16, 128:256] = jnp.where(second, moved, 0.0)
    z1 = dot3((ut_hi[...], ut_lo[...]), pairs[...])
    h1 = jnp.tanh(z1[:, 0:128] + cols[:, 0:1])
    slope1 = 1.0 - h1 * h1
    dh1 = slope1 * z1[:, 128:256]
    z2 = dot3((w2t_hi[...], w2t_lo[...]), jnp.concatenate([h1, dh1], axis=1))
    t2 = jnp.tanh(z2[:, 0:128] + cols[:, 1:2])
    slope2 = 1.0 - t2 * t2
    read = cols[:, 2:3]
    delta2 = slope2 * read
    ddelta2 = -2.0 * t2 * (slope2 * z2[:, 128:256]) * read
    back = dot3((w2_hi[...], w2_lo[...]), jnp.concatenate([delta2, ddelta2], axis=1))
    e1 = back[:, 0:128] + read
    delta1 = slope1 * e1
    ddelta1 = slope1 * back[:, 128:256] - 2.0 * h1 * dh1 * e1
    pairs[...] = dot3((u_hi[...], u_lo[...]), jnp.concatenate([delta1, ddelta1], axis=1))
    g = [jnp.zeros((16, 128), F32) for _ in range(4)]
    dg = [jnp.zeros((16, 128), F32) for _ in range(4)]
    for k in range(levels):
        low, top = pl.ds(k * 16, 16), pl.ds(256 + k * 16, 16)
        m = jnp.where(second, pairs[top, 0:128], pairs[low, 0:128])
        dm = jnp.where(second, pairs[top, 128:256], pairs[low, 128:256])
        for a in range(4):
            row = jnp.broadcast_to(grads[a * 16 + k : a * 16 + k + 1, :], (16, 128))
            drow = jnp.broadcast_to(grads[64 + a * 16 + k : 64 + a * 16 + k + 1, :], (16, 128))
            g[a] = g[a] + m * row
            dg[a] = dg[a] + (dm * row + m * drow)
    scale = 2.0 / n_slots
    for a in range(4):
        grads[a * 16 : (a + 1) * 16, :] = g[a] * scale
        grads[64 + a * 16 : 64 + (a + 1) * 16, :] = dg[a] * scale

    def backward(nb, centre):
        rows = pl.ds(pl.multiple_of(nb * 8, 8), 8)
        u = edge[6, rows, :]
        zero = jnp.zeros((8, 128), F32)
        s0, s1, s2, r0, r1 = ([zero] * 4 for _ in range(5))
        for k in range(levels):
            z = u - float(k)
            phi = phis[k, rows, :]
            phi1 = z * phi
            phi2 = z * phi1
            for a in range(4):
                row = jnp.broadcast_to(grads[a * 16 + k : a * 16 + k + 1, :], (8, 128))
                drow = jnp.broadcast_to(grads[64 + a * 16 + k : 64 + a * 16 + k + 1, :], (8, 128))
                s0[a] = s0[a] + row * phi
                s1[a] = s1[a] + row * phi1
                s2[a] = s2[a] + row * phi2
                r0[a] = r0[a] + drow * phi
                r1[a] = r1[a] + drow * phi1
        d = [edge[c, rows, :] for c in range(3)]
        dd = [edge[3 + c, rows, :] for c in range(3)]
        du = edge[7, rows, :]
        radial = [edge[8 + a, rows, :] for a in range(4)]
        moved = [edge[12 + a, rows, :] for a in range(4)]
        s = radial[0]
        tau = edge[16, rows, :]
        half = edge[17, rows, :]
        rate = edge[18, rows, :]
        one = 1.0 + half
        two = one + half
        sq = -s * one
        sqq = s * (one * one + 2.0 * half * half)
        tq = -tau * two
        tqq = tau * (two * two + 4.0 * half * half)
        share = 1.0 / (1.0 + s)
        us = gap * share * share
        uq = us * sq
        uqq = us * (sqq - 2.0 * share * sq * sq)
        a1 = [-2.0 * v for v in s1]
        da = [r0[a] + a1[a] * du for a in range(4)]
        da1 = [-2.0 * r1[a] + (4.0 * s2[a] - 2.0 * s0[a]) * du for a in range(4)]
        a1r = a1[0] * radial[0] + a1[1] * radial[1] + (a1[2] * radial[2] + a1[3] * radial[3])
        ad = s0[1] * d[0] + s0[2] * d[1] + s0[3] * d[2]
        turned = da1[0] * radial[0] + a1[0] * moved[0]
        for a in range(1, 4):
            turned = turned + (da1[a] * radial[a] + a1[a] * moved[a])
        dad = da[1] * d[0] + s0[1] * dd[0]
        for c in range(1, 3):
            dad = dad + (da[c + 1] * d[c] + s0[c + 1] * dd[c])
        eq = uq * a1r + sq * s0[0] + tq * ad
        deq = rate * (uqq * a1r + sqq * s0[0] + tqq * ad) + uq * turned + sq * da[0] + tq * dad
        dtau = tq * rate
        result = []
        for c in range(3):
            value = 2.0 * (dd[c] * eq + d[c] * deq) + (dtau * s0[c + 1] + tau * da[c + 1])
            hi = value.astype(BF16).astype(F32)
            force[c, rows, :] = hi
            force[3 + c, rows, :] = value - hi
            result.append(centre[c] + value)
        return tuple(result)

    zero = jnp.zeros((8, 128), F32)
    centre = lax.fori_loop(0, blocks, backward, (zero, zero, zero))
    row8 = rows_of((8, 128))
    quarter = row8 & 3
    upper = row8 < 4
    rows16 = [(rows_of((16, 128)) + 16 * rg).astype(F32).astype(BF16) for rg in range(8)]
    chunk = 8

    def scatter(step, total):
        lefts, hots = [], []
        for i in range(chunk):
            n = step * chunk + i
            high = jnp.broadcast_to(ids_t[pl.ds(n, 1), :], (8, 128)) >> 7
            here = high == quarter
            stack = [
                jnp.where(here, jnp.where(upper, jnp.broadcast_to(force[c, pl.ds(n, 1), :], (8, 128)), jnp.broadcast_to(force[3 + c, pl.ds(n, 1), :], (8, 128))), 0.0)
                for c in range(3)
            ]
            lefts.append(jnp.concatenate(stack, axis=0).astype(BF16))
            low = jnp.broadcast_to(lows[pl.ds(n, 1), :], (16, 128)).astype(BF16)
            hots.append(jnp.concatenate([jnp.where(low == r, 1.0, 0.0).astype(BF16) for r in rows16], axis=0))
        return total + lax.dot_general(jnp.concatenate(lefts, axis=1), jnp.concatenate(hots, axis=1), NT, preferred_element_type=F32)

    total = lax.fori_loop(0, n_slots // chunk, scatter, jnp.zeros((24, 128), F32))
    out[...] = jnp.zeros_like(out)
    for c in range(3):
        both = total[c * 8 : c * 8 + 4] + total[c * 8 + 4 : c * 8 + 8]
        for q in range(4):
            row = both[q : q + 1]
            if q == 0:
                row = row - jnp.sum(centre[c], axis=0, keepdims=True)
            out[q, c : c + 1, :] = row


def product(tiles, below, above, prepared, counts, kinds):
    *weights, ids_t = prepared
    n = ids_t.shape[0]
    return pl.pallas_call(
        product_kernel,
        out_shape=jax.ShapeDtypeStruct((4, 8, 128), F32),
        in_specs=vmem(15),
        out_specs=vmem(1)[0],
        scratch_shapes=[
            pltpu.VMEM((4, 8, 128), F32),
            pltpu.VMEM((19, n, 128), F32),
            pltpu.VMEM((16, n, 128), F32),
            pltpu.VMEM((1024, 128), F32),
            pltpu.VMEM((512, 256), F32),
            pltpu.VMEM((128, 128), F32),
            pltpu.VMEM((6, n, 128), F32),
            pltpu.VMEM((n, 128), F32),
        ],
        name="product",
    )(tiles, below, above, ids_t, counts, kinds, *weights)


def halves(ref):
    return jnp.concatenate([ref[0, 0, 0, 0:1, :], ref[0, 0, 0, 1:2, :]], axis=1)


def pack_kernel(places, tangent, map_x, map_y, out):
    rows = [places[c, 0, 0] for c in range(3)] + [tangent[0, c, 0, 0] for c in range(3)]
    rows += [halves(map_x).astype(F32), halves(map_y).astype(F32)]
    out[...] = jnp.broadcast_to(jnp.concatenate(rows, axis=0)[None], out.shape)


def pack(positions, basis, map_x, map_y, bricks):
    last = basis.shape[0] - 1
    whole = lambda a: pl.BlockSpec(a.shape, lambda i: (0,) * a.ndim)
    return pl.pallas_call(
        pack_kernel,
        grid=(1,),
        out_shape=jax.ShapeDtypeStruct((bricks, 8, 128), F32),
        in_specs=[
            whole(positions),
            pl.BlockSpec((1,) + basis.shape[1:], lambda i: (last,) + (0,) * (basis.ndim - 1)),
            whole(map_x),
            whole(map_y),
        ],
        out_specs=pl.BlockSpec((bricks, 8, 128), lambda i: (0, 0, 0)),
        name="pack",
    )(positions, basis, map_x, map_y)


def brick_reader(where, grid):
    nx, ny = grid

    def at(ref, dx, dy):
        x = lax.rem(where[0] + (dx + nx), nx)
        y = lax.rem(where[1] + (dy + ny), ny)
        return ref[x * ny + y]

    return at


def as_index(row):
    return jnp.broadcast_to(row, (8, 128)).astype(jnp.int32)


def turn(x):
    return pltpu.roll(x, 64, 1)


def assemble_kernel(grid, where, got, map_z, tiles, message):
    at = brick_reader(where, grid)
    lower = rows_of((8, 128), 1) < 64
    row = rows_of((8, 128))
    step_x = jnp.where(row == 0, 1.0, 0.0)
    step_y = jnp.where(row == 1, 1.0, 0.0)
    middle, ghosts, index = {}, {}, {}
    for dy in (-1, 0, 1):
        own, low, high = at(got, 0, dy), at(got, -1, dy), at(got, 1, dy)
        from_low = lane_pick(low, turn(as_index(low[6:7])))
        from_high = lane_pick(high, turn(as_index(high[6:7])))
        middle[dy] = own
        ghosts[dy] = jnp.where(lower, from_low - step_x, from_high + step_x)
        index[dy] = turn(as_index(own[7:8]))

    def second(dy):
        low = index[dy] & 127
        return jnp.where(index[dy] < 128, lane_pick(middle[dy], low), lane_pick(ghosts[dy], low))

    third = jnp.where(lower, second(-1) - step_y, second(1) + step_y)
    tiles[0] = middle[0]
    tiles[1] = ghosts[0]
    tiles[2] = third
    chosen = jnp.broadcast_to(halves(map_z), (8, 128))
    low = chosen & 127
    message[...] = jnp.where(
        chosen < 128, lane_pick(middle[0], low), jnp.where(chosen < 256, lane_pick(ghosts[0], low), lane_pick(third, low))
    )


def smem():
    return [pl.BlockSpec(memory_space=pltpu.SMEM)]


def assemble(where, got, map_z, grid):
    return pl.pallas_call(
        functools.partial(assemble_kernel, grid),
        out_shape=[jax.ShapeDtypeStruct((3, 8, 128), F32), jax.ShapeDtypeStruct((8, 128), F32)],
        in_specs=smem() + vmem(2),
        out_specs=vmem(2),
        name="assemble",
    )(where, got, map_z)


def thirds(x):
    hi, rest = x.astype(BF16), x
    rest = x - hi.astype(F32)
    mid = rest.astype(BF16)
    low = (rest - mid.astype(F32)).astype(BF16)
    return jnp.concatenate([hi.astype(F32), mid.astype(F32), low.astype(F32)], axis=0).astype(BF16)


def spread_columns(values, index, columns, first):
    target = rows_of((columns, 128)) + first
    hot = jnp.where(jnp.broadcast_to(index, (columns, 128)) == target, 1.0, 0.0).astype(BF16)
    both = lax.dot_general(thirds(values), hot, NT, preferred_element_type=F32)
    return both[0:8] + (both[8:16] + both[16:24])


def fold_z_kernel(products, below, above, map_z, own, out):
    lower = rows_of((8, 128), 1) < 64
    value = jnp.where(lower, turn(below[...]), turn(above[...]))
    added = spread_columns(value, halves(map_z), 384, 0)
    own[...] = products[0] + added[:, 0:128]
    first = products[1] + added[:, 128:256]
    second = products[2] + added[:, 256:384]
    tile = jnp.concatenate([first[0:3], second[0:3], jnp.zeros((2, 128), F32)], axis=0)
    out[...] = jnp.broadcast_to(tile[None], out.shape)


def fold_z(products, below, above, map_z, bricks):
    return pl.pallas_call(
        fold_z_kernel,
        out_shape=[jax.ShapeDtypeStruct((8, 128), F32), jax.ShapeDtypeStruct((bricks, 8, 128), F32)],
        in_specs=vmem(4),
        out_specs=vmem(2),
        name="fold_z",
    )(products, below, above, map_z)


def gram_kernel(basis, stored, gram):
    count = basis.shape[0]
    stored[...] = jnp.zeros_like(stored)
    total = jnp.zeros((32, 32), F32)
    for c in range(3):
        for k in range(count):
            stored[c, k : k + 1, :] = basis[k, c, 0, 0]
        total = total + lax.dot_general(stored[c], stored[c], NT, precision=lax.Precision.HIGHEST, preferred_element_type=F32)
    gram[...] = jnp.zeros_like(gram)
    gram[:, 0:32] = total


def local_gram(basis):
    return pl.pallas_call(
        gram_kernel,
        out_shape=[jax.ShapeDtypeStruct((3, 32, 128), F32), jax.ShapeDtypeStruct((32, 128), F32)],
        in_specs=vmem(1),
        out_specs=vmem(2),
        name="gram",
    )(basis)


def fold_kernel(grid, where, own, got, maps, stored, gram, product, out):
    at = brick_reader(where, grid)
    lower = rows_of((8, 128), 1) < 64

    def from_y(dx):
        return jnp.where(lower, turn(at(got, dx, -1)), turn(at(got, dx, 1)))

    def second(value):
        return jnp.concatenate([value[3:6], jnp.zeros((5, 128), F32)], axis=0)

    def ghost(dx):
        index = at(maps, dx, 0)[7:8].astype(jnp.int32)
        return at(got, dx, 0) + spread_columns(second(from_y(dx)), index, 128, 128)

    mine = at(maps, 0, 0)
    total = own[...] + spread_columns(second(from_y(0)), mine[7:8].astype(jnp.int32), 128, 0)
    from_x = jnp.where(lower, turn(ghost(-1)), turn(ghost(1)))
    total = total + spread_columns(from_x, mine[6:7].astype(jnp.int32), 128, 0)
    product[...] = total
    last = rows_of((32, 128)) == 30
    column = jnp.zeros((32, 128), F32)
    line = jnp.zeros((8, 32), F32)
    for c in range(3):
        row = total[c : c + 1]
        rows = jnp.where(last, row, stored[c])
        column = column + rows * row
        line = line + lax.dot_general(
            jnp.broadcast_to(row, (8, 128)), rows, NT, precision=lax.Precision.HIGHEST, preferred_element_type=F32
        )
    column = jnp.sum(column, axis=1, keepdims=True)
    line = jnp.concatenate([line[0:1], jnp.zeros((1, 96), F32)], axis=1)
    lane = rows_of((32, 128), 1)
    full = jnp.where(lane == 30, column, jnp.where(last, line, gram[...]))
    tile = full[0:8]
    for b in range(1, 4):
        tile = tile + pltpu.roll(full[8 * b : 8 * b + 8], 32 * b, 1)
    out[...] = jnp.broadcast_to(tile[None], out.shape)


def fold(where, own, got, maps, stored, gram, grid):
    return pl.pallas_call(
        functools.partial(fold_kernel, grid),
        out_shape=[jax.ShapeDtypeStruct((8, 128), F32), jax.ShapeDtypeStruct(got.shape, F32)],
        in_specs=smem() + vmem(5),
        out_specs=vmem(2),
        name="fold",
    )(where, own, got, maps, stored, gram)


def total_kernel(got, out):
    out[...] = jnp.broadcast_to(jnp.sum(got[...], axis=0)[None], out.shape)


def total_of(got, copies):
    return pl.pallas_call(
        total_kernel,
        out_shape=jax.ShapeDtypeStruct((copies,) + got.shape[1:], F32),
        in_specs=vmem(1),
        out_specs=vmem(1)[0],
        name="total",
    )(got)


def finish_kernel(entries, got, product, stored, result, correlations, norm):
    count = correlations.shape[1] - 98
    packed = jnp.sum(got[...], axis=0) * (1.0 / entries)
    full = jnp.concatenate([packed] + [pltpu.roll(packed, 128 - 32 * b, 1) for b in range(1, 4)], axis=0)
    column = full[:, count : count + 1]
    line = full[count : count + 1, :]
    row = rows_of((32, 1))
    lane = rows_of((1, 128), 1)
    down = jnp.where(row < count, column, jnp.where(row == count, -1.0, 0.0))
    across = jnp.where(lane < count, line, jnp.where(lane == count, -1.0, 0.0))
    square = jnp.sum(jnp.where(rows_of((32, 128), 1) <= count, full * across * down, 0.0), axis=1, keepdims=True)
    length = jnp.sqrt(jnp.maximum(jnp.sum(square, axis=0, keepdims=True), 0.0) + 1e-06)
    norm[...] = length
    correlations[...] = line
    share = jnp.where(row < count, column, 0.0)
    for c in range(3):
        taken = jnp.sum(stored[c] * share, axis=0, keepdims=True)
        result[c, 0, 0] = (product[c : c + 1, :] - taken) / length


def finish(got, product, stored, shape, entries):
    return pl.pallas_call(
        functools.partial(finish_kernel, entries),
        out_shape=[
            jax.ShapeDtypeStruct(shape, F32),
            jax.ShapeDtypeStruct((1, 128), F32),
            jax.ShapeDtypeStruct((1, 1), F32),
        ],
        in_specs=vmem(3),
        out_specs=vmem(3),
        name="finish",
    )(got, product, stored)


def on_device(positions, basis, neighbours, used_count, kinds, map_x, map_y, map_z, table, fit_w1, fit_b1, fit_w2, fit_b2, fit_out):
    nx, ny, nz = (lax.axis_size(a) for a in ("gx", "gy", "gz"))
    plane = ("gx", "gy")
    where = jnp.stack([lax.axis_index("gx"), lax.axis_index("gy")]).astype(jnp.int32)
    up = [(i, (i + 1) % nz) for i in range(nz)]
    down = [(j, i) for i, j in up]

    def exchange(x):
        return lax.all_to_all(x, plane, 0, 0)

    raw = exchange(pack(positions, basis, map_x, map_y, nx * ny))
    tiles, message = assemble(where, raw, map_z, (nx, ny))
    below, above = lax.ppermute(message, "gz", up), lax.ppermute(message, "gz", down)
    prepared = prepare(table, fit_w1, fit_w2, fit_b1, fit_b2, fit_out, neighbours)
    stored, gram = local_gram(basis)
    products = product(tiles, below, above, prepared, used_count, kinds)
    outgoing = products[3]
    below, above = lax.ppermute(outgoing, "gz", up), lax.ppermute(outgoing, "gz", down)
    own, shared = fold_z(products, below, above, map_z, nx * ny)
    hessian_vec, summary = fold(where, own, exchange(shared), raw, stored, gram, (nx, ny))
    summary = total_of(exchange(summary), nz)
    summary = lax.all_to_all(summary, "gz", 0, 0)
    entries = 3 * positions.shape[-1] * nx * ny * nz
    next_vector, correlations, vector_norm = finish(summary, hessian_vec, stored, positions.shape, entries)
    return next_vector, correlations[0, : basis.shape[0]], vector_norm[0, 0]


def solution(mesh):
    bricks = P("gx", "gy", "gz", None)
    lists = P("gx", "gy", "gz", None, None)
    vector = P(None, "gx", "gy", "gz", None)
    return jax.shard_map(
        on_device,
        mesh=mesh,
        in_specs=(vector, P(None, None, "gx", "gy", "gz", None), lists, bricks, bricks, lists, lists, lists) + (P(),) * 6,
        out_specs=(vector, P(), P()),
        check_vma=False,
    )
```

```python
import functools

import jax
import jax.numpy as jnp
from jax import lax
from jax.experimental import pallas as pl
from jax.experimental.pallas import tpu as pltpu
from jax.sharding import PartitionSpec as P

F32 = jnp.float32
BF16 = jnp.bfloat16
LOG2E = 1.4426950408889634
NT = (((1,), (1,)), ((), ()))


def split(x):
    hi = x.astype(BF16)
    return hi, (x - hi.astype(F32)).astype(BF16)


def mm(a, b):
    return jnp.dot(a, b, preferred_element_type=F32)


def dot3(a, b):
    ah, al = a if isinstance(a, tuple) else split(a)
    bh, bl = b if isinstance(b, tuple) else split(b)
    return mm(ah, bh) + (mm(ah, bl) + mm(al, bh))


def lane_pick(table, index):
    return jnp.take_along_axis(table, index, axis=1, mode="promise_in_bounds")


def rows_of(shape, dim=0):
    return lax.broadcasted_iota(jnp.int32, shape, dim)


def halves(ref):
    return jnp.concatenate([ref[0, 0, 0, 0:1, :], ref[0, 0, 0, 1:2, :]], axis=1)


def fetch(sources, places, semaphores):
    copies = [pltpu.make_async_copy(x, y, semaphores.at[i]) for i, (x, y) in enumerate(zip(sources, places))]
    for copy in copies:
        copy.start()
    return copies


EXACT = dict(precision=lax.Precision.HIGHEST, preferred_element_type=F32)


def mixing_kernel(table_at, w1_at, map_at, u_hi, u_lo, ut_hi, ut_lo, map_row, table, w1t, map_z, outer, inner, k_hi, k_lo, semaphores):
    copies = fetch((table_at, map_at, w1_at), (table, map_z, w1t), semaphores)
    types, levels, width = table.shape
    hidden = w1t.shape[0]
    m2 = w1t.shape[1] // width
    count = types * levels * levels
    copies[0].wait()
    tall = table[...].reshape(types * levels, width)
    tall = jnp.concatenate([tall, jnp.zeros((types * levels, 128 - width), F32)], axis=1)
    tall = jnp.concatenate([tall, jnp.zeros((128 - types * levels, 128), F32)], axis=0).T
    column = rows_of((128, count), 1)
    row = rows_of((128, count))
    kind = column // (levels * levels)
    first = jnp.where(row == kind * levels + (column // levels) % levels, 1.0, 0.0)
    second = jnp.where(row == kind * levels + column % levels, 1.0, 0.0)
    outer[...] = jnp.dot(tall, first, **EXACT) * 0.5
    inner[...] = jnp.dot(tall, second, **EXACT) * 0.5
    near = inner[0:m2, :] * 2.0
    far = outer[0:m2, :] * 2.0

    def kron(m, carry):
        value = jnp.broadcast_to(outer[pl.ds(m, 1), :], (m2, count)) * near + jnp.broadcast_to(inner[pl.ds(m, 1), :], (m2, count)) * far
        hi, lo = split(value)
        at = pl.ds(pl.multiple_of(m * m2, m2), m2)
        k_hi[at, :] = hi
        k_lo[at, :] = lo
        return carry

    lax.fori_loop(0, width, kron, 0, unroll=4)
    copies[1].wait()
    map_row[...] = halves(map_z)
    copies[2].wait()
    full = dot3(w1t[...], (k_hi[...], k_lo[...]))
    full = jnp.concatenate([full, jnp.zeros((256 - hidden, count), F32)], axis=0)
    hi, lo = split(full)
    ut_hi[...] = hi
    ut_lo[...] = lo
    hi, lo = split(full.T)
    u_hi[...] = hi
    u_lo[...] = lo


def lists_kernel(w2_at, b1_at, b2_at, wo_at, ids_at, counts_at, kinds_at, basis_at, w2_hi, w2_lo, w2t_hi, w2t_lo, cols, ids_t, count_row, kind_row, stored, gram, w2, b1, b2, wo, ids, counts, kinds, basis, pad, semaphores):
    places = (w2, b1, b2, wo, ids, counts, kinds, basis)
    copies = fetch((w2_at, b1_at, b2_at, wo_at, ids_at, counts_at, kinds_at, basis_at), places, semaphores)
    hidden = w2.shape[0]
    pad[...] = jnp.zeros_like(pad)
    stored[...] = jnp.zeros_like(stored)
    gram[...] = jnp.zeros_like(gram)
    for copy in copies:
        copy.wait()
    pad[0:hidden, 0:hidden] = w2[...]
    hi, lo = split(pad[...])
    w2_hi[...] = hi
    w2_lo[...] = lo
    hi, lo = split(pad[...].T)
    w2t_hi[...] = hi
    w2t_lo[...] = lo
    pad[0:128, :] = jnp.zeros((128, pad.shape[1]), F32)
    pad[0:1, 0:hidden] = b1[...]
    pad[1:2, 0:hidden] = b2[...]
    pad[2:3, 0:hidden] = wo[...]
    cols[...] = pad[0:128, :].T
    ids_t[...] = ids[0, 0, 0].astype(F32).T.astype(jnp.int32)
    count_row[...] = counts[0, 0]
    kind_row[...] = kinds[0, 0]
    total = jnp.zeros((32, 32), F32)
    for c in range(3):
        for k in range(basis.shape[0]):
            stored[c, k : k + 1, :] = basis[k, c, 0, 0]
        total = total + lax.dot_general(stored[c], stored[c], NT, **EXACT)
    gram[:, 0:32] = total


def vmem(n):
    return [pl.BlockSpec(memory_space=pltpu.VMEM)] * n


def here(*arrays):
    return [pltpu.with_memory_space_constraint(a, pltpu.VMEM) for a in arrays]


def from_hbm(kernel, name, shapes, scratch, *arrays):
    return pl.pallas_call(
        kernel,
        out_shape=[pltpu.VMEM(s, d) for s, d in shapes],
        in_specs=[pl.BlockSpec(memory_space=pltpu.HBM)] * len(arrays),
        out_specs=vmem(len(shapes)),
        scratch_shapes=[pltpu.VMEM(a.shape, a.dtype) for a in arrays] + scratch + [pltpu.SemaphoreType.DMA((len(arrays),))],
        name=name,
    )(*(pltpu.with_memory_space_constraint(a, pltpu.HBM) for a in arrays))


def mixing(table, w1, map_z):
    hp = 256
    count = table.shape[0] * table.shape[1] ** 2
    shapes = [((count, hp), BF16)] * 2 + [((hp, count), BF16)] * 2 + [((1, 128), jnp.int32)]
    scratch = [pltpu.VMEM((128, count), F32)] * 2 + [pltpu.VMEM((w1.shape[0], count), BF16)] * 2
    *weights, map_row = from_hbm(mixing_kernel, "mixing", shapes, scratch, table, w1.T, map_z)
    return weights, map_row


def lists_of(w2, b1, b2, wo, ids, counts, kinds, basis):
    hp = 256
    row = ((1, 128), jnp.int32)
    shapes = [((hp, hp), BF16)] * 4 + [((hp, 128), F32), ((ids.shape[-1], 128), jnp.int32), row, row, ((3, 32, 128), F32), ((32, 128), F32)]
    scratch = [pltpu.VMEM((hp, hp), F32)]
    done = from_hbm(lists_kernel, "lists", shapes, scratch, w2, b1[None], b2[None], wo[None], ids, counts, kinds, basis)
    return done[:5], done[5:8], done[8], done[9]


def shifted_ghosts(below, above, coord, rows):
    lower = rows_of((rows, 128), 1) < 64
    step = jnp.where(rows_of((rows, 128)) == coord, 1.0, 0.0)
    return jnp.where(lower, below - step, above + step)


def product_kernel(tiles, below, above, ids_t, counts, kinds, u_hi, u_lo, ut_hi, ut_lo, w2_hi, w2_lo, w2t_hi, w2t_lo, cols, out, sent, xv, edge, phis, acc, pairs, grads, force, lows):
    n_slots = ids_t.shape[0]
    levels = 16
    gap = levels - 1
    blocks = n_slots // 8
    xv[0:3] = tiles[...]
    xv[3] = shifted_ghosts(pltpu.roll(below[...], 64, 1), pltpu.roll(above[...], 64, 1), 2, 8)
    count_row = jnp.broadcast_to(counts[...], (8, 128))

    def geometry(nb, carry):
        rows = pl.ds(pl.multiple_of(nb * 8, 8), 8)
        index = ids_t[rows, :]
        low = index & 127
        high = index >> 7
        lows[rows, :] = (index & 63).astype(F32)
        near = []
        for f in range(6):
            picks = [lane_pick(jnp.broadcast_to(xv[q, f : f + 1, :], (8, 128)), low) for q in range(4)]
            value = jnp.where(high < 2, jnp.where(high == 0, picks[0], picks[1]), jnp.where(high == 2, picks[2], picks[3]))
            near.append(value - jnp.broadcast_to(xv[0, f : f + 1, :], (8, 128)))
        d, dd = near[:3], near[3:]
        square = d[0] * d[0] + d[1] * d[1] + d[2] * d[2]
        rate = 2.0 * (d[0] * dd[0] + d[1] * dd[1] + d[2] * dd[2])
        wide = square + 0.01
        inverse = lax.rsqrt(wide)
        half = 0.5 / wide
        live = (rows_of((8, 128)) + nb * 8) < count_row
        s = jnp.where(live, jnp.exp(-square) * inverse, 0.0)
        tau = s * inverse
        sq = -s * (1.0 + half)
        tq = -tau * (1.0 + 2.0 * half)
        share = 1.0 / (1.0 + s)
        us = gap * share * share
        for c in range(3):
            edge[c, rows, :] = d[c]
            edge[3 + c, rows, :] = dd[c]
            edge[9 + c, rows, :] = tau * d[c]
            edge[13 + c, rows, :] = tq * rate * d[c] + tau * dd[c]
        edge[6, rows, :] = gap * s * share
        edge[7, rows, :] = us * sq * rate
        edge[8, rows, :] = s
        edge[12, rows, :] = sq * rate
        edge[16, rows, :] = tau
        edge[17, rows, :] = half
        edge[18, rows, :] = rate
        return carry

    lax.fori_loop(0, blocks, geometry, 0, unroll=2)

    def pooling(kk, carry):
        sums = [[jnp.zeros((8, 128), F32) for _ in range(8)] for _ in range(2)]
        for nb in range(blocks):
            rows = pl.ds(nb * 8, 8)
            u = edge[6, rows, :]
            w = -2.0 * edge[7, rows, :]
            radial = [edge[8 + a, rows, :] for a in range(4)]
            moved = [edge[12 + a, rows, :] for a in range(4)]
            for side in range(2):
                z = u - (2 * kk + side).astype(F32)
                phi = jnp.exp2(z * (z * (-LOG2E)))
                phis[2 * kk + side, rows, :] = phi
                dphi = phi * (z * w)
                for a in range(4):
                    sums[side][a] = sums[side][a] + phi * radial[a]
                    sums[side][4 + a] = sums[side][4 + a] + (dphi * radial[a] + phi * moved[a])
        for side in range(2):
            for a in range(8):
                acc[pl.ds(pl.multiple_of((a * levels + 2 * kk + side) * 8, 8), 8), :] = sums[side][a]
        return carry

    lax.fori_loop(0, levels // 2, pooling, 0)
    pooled = acc[pl.ds(0, 128, stride=8), :]
    for s in range(1, 8):
        pooled = pooled + acc[pl.ds(s, 128, stride=8), :]
    pooled = pooled * (1.0 / n_slots)
    grads[...] = pooled
    second = jnp.broadcast_to(kinds[...], (16, 128)) == 1
    p = [pooled[a * 16 : (a + 1) * 16] for a in range(4)]
    dp = [pooled[64 + a * 16 : 64 + (a + 1) * 16] for a in range(4)]
    for k in range(levels):
        value = jnp.zeros((16, 128), F32)
        moved = jnp.zeros((16, 128), F32)
        for a in range(4):
            value = value + p[a] * jnp.broadcast_to(grads[a * 16 + k : a * 16 + k + 1, :], (16, 128))
            moved = moved + p[a] * jnp.broadcast_to(grads[64 + a * 16 + k : 64 + a * 16 + k + 1, :], (16, 128))
        moved = 2.0 * moved
        pairs[k * 16 : (k + 1) * 16, 0:128] = jnp.where(second, 0.0, value)
        pairs[k * 16 : (k + 1) * 16, 128:256] = jnp.where(second, 0.0, moved)
        pairs[256 + k * 16 : 256 + (k + 1) * 16, 0:128] = jnp.where(second, value, 0.0)
        pairs[256 + k * 16 : 256 + (k + 1) * 16, 128:256] = jnp.where(second, moved, 0.0)
    z1 = dot3((ut_hi[...], ut_lo[...]), pairs[...])
    h1 = jnp.tanh(z1[:, 0:128] + cols[:, 0:1])
    slope1 = 1.0 - h1 * h1
    dh1 = slope1 * z1[:, 128:256]
    z2 = dot3((w2t_hi[...], w2t_lo[...]), jnp.concatenate([h1, dh1], axis=1))
    t2 = jnp.tanh(z2[:, 0:128] + cols[:, 1:2])
    slope2 = 1.0 - t2 * t2
    read = cols[:, 2:3]
    delta2 = slope2 * read
    ddelta2 = -2.0 * t2 * (slope2 * z2[:, 128:256]) * read
    back = dot3((w2_hi[...], w2_lo[...]), jnp.concatenate([delta2, ddelta2], axis=1))
    e1 = back[:, 0:128] + read
    delta1 = slope1 * e1
    ddelta1 = slope1 * back[:, 128:256] - 2.0 * h1 * dh1 * e1
    pairs[...] = dot3((u_hi[...], u_lo[...]), jnp.concatenate([delta1, ddelta1], axis=1))
    g = [jnp.zeros((16, 128), F32) for _ in range(4)]
    dg = [jnp.zeros((16, 128), F32) for _ in range(4)]
    for k in range(levels):
        low, top = pl.ds(k * 16, 16), pl.ds(256 + k * 16, 16)
        m = jnp.where(second, pairs[top, 0:128], pairs[low, 0:128])
        dm = jnp.where(second, pairs[top, 128:256], pairs[low, 128:256])
        for a in range(4):
            row = jnp.broadcast_to(grads[a * 16 + k : a * 16 + k + 1, :], (16, 128))
            drow = jnp.broadcast_to(grads[64 + a * 16 + k : 64 + a * 16 + k + 1, :], (16, 128))
            g[a] = g[a] + m * row
            dg[a] = dg[a] + (dm * row + m * drow)
    scale = 2.0 / n_slots
    for a in range(4):
        grads[a * 16 : (a + 1) * 16, :] = g[a] * scale
        grads[64 + a * 16 : 64 + (a + 1) * 16, :] = dg[a] * scale

    def backward(nb, centre):
        rows = pl.ds(pl.multiple_of(nb * 8, 8), 8)
        u = edge[6, rows, :]
        zero = jnp.zeros((8, 128), F32)
        s0, s1, s2, r0, r1 = ([zero] * 4 for _ in range(5))
        for k in range(levels):
            z = u - float(k)
            phi = phis[k, rows, :]
            phi1 = z * phi
            phi2 = z * phi1
            for a in range(4):
                row = jnp.broadcast_to(grads[a * 16 + k : a * 16 + k + 1, :], (8, 128))
                drow = jnp.broadcast_to(grads[64 + a * 16 + k : 64 + a * 16 + k + 1, :], (8, 128))
                s0[a] = s0[a] + row * phi
                s1[a] = s1[a] + row * phi1
                s2[a] = s2[a] + row * phi2
                r0[a] = r0[a] + drow * phi
                r1[a] = r1[a] + drow * phi1
        d = [edge[c, rows, :] for c in range(3)]
        dd = [edge[3 + c, rows, :] for c in range(3)]
        du = edge[7, rows, :]
        radial = [edge[8 + a, rows, :] for a in range(4)]
        moved = [edge[12 + a, rows, :] for a in range(4)]
        s = radial[0]
        tau = edge[16, rows, :]
        half = edge[17, rows, :]
        rate = edge[18, rows, :]
        one = 1.0 + half
        two = one + half
        sq = -s * one
        sqq = s * (one * one + 2.0 * half * half)
        tq = -tau * two
        tqq = tau * (two * two + 4.0 * half * half)
        share = 1.0 / (1.0 + s)
        us = gap * share * share
        uq = us * sq
        uqq = us * (sqq - 2.0 * share * sq * sq)
        a1 = [-2.0 * v for v in s1]
        da = [r0[a] + a1[a] * du for a in range(4)]
        da1 = [-2.0 * r1[a] + (4.0 * s2[a] - 2.0 * s0[a]) * du for a in range(4)]
        a1r = a1[0] * radial[0] + a1[1] * radial[1] + (a1[2] * radial[2] + a1[3] * radial[3])
        ad = s0[1] * d[0] + s0[2] * d[1] + s0[3] * d[2]
        turned = da1[0] * radial[0] + a1[0] * moved[0]
        for a in range(1, 4):
            turned = turned + (da1[a] * radial[a] + a1[a] * moved[a])
        dad = da[1] * d[0] + s0[1] * dd[0]
        for c in range(1, 3):
            dad = dad + (da[c + 1] * d[c] + s0[c + 1] * dd[c])
        eq = uq * a1r + sq * s0[0] + tq * ad
        deq = rate * (uqq * a1r + sqq * s0[0] + tqq * ad) + uq * turned + sq * da[0] + tq * dad
        dtau = tq * rate
        result = []
        for c in range(3):
            value = 2.0 * (dd[c] * eq + d[c] * deq) + (dtau * s0[c + 1] + tau * da[c + 1])
            hi = value.astype(BF16).astype(F32)
            force[c, rows, :] = hi
            force[3 + c, rows, :] = value - hi
            result.append(centre[c] + value)
        return tuple(result)

    zero = jnp.zeros((8, 128), F32)
    centre = lax.fori_loop(0, blocks, backward, (zero, zero, zero), unroll=2)
    row8 = rows_of((8, 128))
    rows16 = [(rows_of((16, 128)) + 16 * rg).astype(F32).astype(BF16) for rg in range(4)]
    on = jnp.ones((16, 128), BF16)
    off = jnp.zeros((16, 128), BF16)
    chunk = 8

    def scatter(step, total):
        lefts, hots = [], []
        for i in range(chunk):
            n = step * chunk + i
            hit = (jnp.broadcast_to(ids_t[pl.ds(n, 1), :], (8, 128)) >> 6) == row8
            stack = [jnp.where(hit, jnp.broadcast_to(force[c, pl.ds(n, 1), :], (8, 128)), 0.0) for c in range(6)]
            lefts.append(jnp.concatenate(stack, axis=0).astype(BF16))
            low = jnp.broadcast_to(lows[pl.ds(n, 1), :], (16, 128)).astype(BF16)
            hots.append(jnp.concatenate([jnp.where(low == r, on, off) for r in rows16], axis=0))
        return total + lax.dot_general(jnp.concatenate(lefts, axis=1), jnp.concatenate(hots, axis=1), NT, preferred_element_type=F32)

    total = lax.fori_loop(0, n_slots // chunk, scatter, jnp.zeros((48, 64), F32), unroll=2)
    out[...] = jnp.zeros_like(out)
    sent[...] = jnp.zeros_like(sent)
    for c in range(3):
        both = total[c * 8 : c * 8 + 8] + total[24 + c * 8 : 32 + c * 8]
        for q in range(4):
            row = jnp.concatenate([both[2 * q : 2 * q + 1], both[2 * q + 1 : 2 * q + 2]], axis=1)
            if q == 0:
                row = row - jnp.sum(centre[c], axis=0, keepdims=True)
            if q < 3:
                out[q, c : c + 1, :] = row
            else:
                sent[c : c + 1, :] = row


def product(tiles, below, above, lists, weights):
    n = lists[0].shape[0]
    return pl.pallas_call(
        product_kernel,
        out_shape=[pltpu.VMEM((3, 8, 128), F32), pltpu.VMEM((8, 128), F32)],
        in_specs=vmem(15),
        out_specs=vmem(2),
        scratch_shapes=[
            pltpu.VMEM((4, 8, 128), F32),
            pltpu.VMEM((19, n, 128), F32),
            pltpu.VMEM((16, n, 128), F32),
            pltpu.VMEM((1024, 128), F32),
            pltpu.VMEM((512, 256), F32),
            pltpu.VMEM((128, 128), F32),
            pltpu.VMEM((6, n, 128), F32),
            pltpu.VMEM((n, 128), F32),
        ],
        name="product",
    )(*here(tiles, below, above, *lists, *weights))


def pack_kernel(places, tangent, map_x, map_y, out):
    rows = [places[c, 0, 0] for c in range(3)] + [tangent[0, c, 0, 0] for c in range(3)]
    rows += [halves(map_x).astype(F32), halves(map_y).astype(F32)]
    out[...] = jnp.broadcast_to(jnp.concatenate(rows, axis=0)[None], out.shape)


def pack(positions, basis, map_x, map_y, bricks):
    last = basis.shape[0] - 1
    whole = lambda a: pl.BlockSpec(a.shape, lambda i: (0,) * a.ndim)
    return pl.pallas_call(
        pack_kernel,
        grid=(1,),
        out_shape=pltpu.VMEM((bricks, 8, 128), F32),
        in_specs=[
            whole(positions),
            pl.BlockSpec((1,) + basis.shape[1:], lambda i: (last,) + (0,) * (basis.ndim - 1)),
            whole(map_x),
            whole(map_y),
        ],
        out_specs=vmem(1)[0],
        name="pack",
    )(positions, basis, map_x, map_y)


def brick_reader(grid):
    nx, ny = grid
    px, py = lax.axis_index("gx"), lax.axis_index("gy")

    def at(ref, dx, dy):
        x = lax.rem(px + (dx + nx), nx)
        y = lax.rem(py + (dy + ny), ny)
        return ref[x * ny + y]

    return at


def as_index(row):
    return jnp.broadcast_to(row, (8, 128)).astype(jnp.int32)


def turn(x):
    return pltpu.roll(x, 64, 1)


def assemble_kernel(grid, got, map_z, tiles, message):
    at = brick_reader(grid)
    lower = rows_of((8, 128), 1) < 64
    row = rows_of((8, 128))
    step_x = jnp.where(row == 0, 1.0, 0.0)
    step_y = jnp.where(row == 1, 1.0, 0.0)
    middle, ghosts, index = {}, {}, {}
    for dy in (-1, 0, 1):
        own, low, high = at(got, 0, dy), at(got, -1, dy), at(got, 1, dy)
        from_low = lane_pick(low, turn(as_index(low[6:7])))
        from_high = lane_pick(high, turn(as_index(high[6:7])))
        middle[dy] = own
        ghosts[dy] = jnp.where(lower, from_low - step_x, from_high + step_x)
        index[dy] = turn(as_index(own[7:8]))

    def second(dy):
        low = index[dy] & 127
        return jnp.where(index[dy] < 128, lane_pick(middle[dy], low), lane_pick(ghosts[dy], low))

    third = jnp.where(lower, second(-1) - step_y, second(1) + step_y)
    tiles[0] = middle[0]
    tiles[1] = ghosts[0]
    tiles[2] = third
    chosen = jnp.broadcast_to(map_z[...], (8, 128))
    low = chosen & 127
    message[...] = jnp.where(
        chosen < 128, lane_pick(middle[0], low), jnp.where(chosen < 256, lane_pick(ghosts[0], low), lane_pick(third, low))
    )


def assemble(got, map_z, grid):
    return pl.pallas_call(
        functools.partial(assemble_kernel, grid),
        out_shape=[pltpu.VMEM((3, 8, 128), F32), pltpu.VMEM((8, 128), F32)],
        in_specs=vmem(2),
        out_specs=vmem(2),
        name="assemble",
    )(*here(got, map_z))


def thirds(x):
    hi, rest = x.astype(BF16), x
    rest = x - hi.astype(F32)
    mid = rest.astype(BF16)
    low = (rest - mid.astype(F32)).astype(BF16)
    return jnp.concatenate([hi.astype(F32), mid.astype(F32), low.astype(F32)], axis=0).astype(BF16)


def spread_columns(values, index, columns, first):
    target = rows_of((columns, 128)) + first
    hot = jnp.where(jnp.broadcast_to(index, (columns, 128)) == target, 1.0, 0.0).astype(BF16)
    both = lax.dot_general(thirds(values), hot, NT, preferred_element_type=F32)
    return both[0:8] + (both[8:16] + both[16:24])


def fold_z_kernel(products, below, above, map_z, own, out):
    lower = rows_of((8, 128), 1) < 64
    value = jnp.where(lower, turn(below[...]), turn(above[...]))
    added = spread_columns(value, map_z[...], 384, 0)
    own[...] = products[0] + added[:, 0:128]
    first = products[1] + added[:, 128:256]
    second = products[2] + added[:, 256:384]
    tile = jnp.concatenate([first[0:3], second[0:3], jnp.zeros((2, 128), F32)], axis=0)
    out[...] = jnp.broadcast_to(tile[None], out.shape)


def fold_z(products, below, above, map_z, bricks):
    return pl.pallas_call(
        fold_z_kernel,
        out_shape=[pltpu.VMEM((8, 128), F32), pltpu.VMEM((bricks, 8, 128), F32)],
        in_specs=vmem(4),
        out_specs=vmem(2),
        name="fold_z",
    )(*here(products, below, above, map_z))


def fold_kernel(grid, own, got, maps, stored, gram, product, out):
    at = brick_reader(grid)
    lower = rows_of((8, 128), 1) < 64

    def from_y(dx):
        return jnp.where(lower, turn(at(got, dx, -1)), turn(at(got, dx, 1)))

    def second(value):
        return jnp.concatenate([value[3:6], jnp.zeros((5, 128), F32)], axis=0)

    def ghost(dx):
        index = at(maps, dx, 0)[7:8].astype(jnp.int32)
        return at(got, dx, 0) + spread_columns(second(from_y(dx)), index, 128, 128)

    mine = at(maps, 0, 0)
    total = own[...] + spread_columns(second(from_y(0)), mine[7:8].astype(jnp.int32), 128, 0)
    from_x = jnp.where(lower, turn(ghost(-1)), turn(ghost(1)))
    total = total + spread_columns(from_x, mine[6:7].astype(jnp.int32), 128, 0)
    product[...] = total
    last = rows_of((32, 128)) == 30
    column = jnp.zeros((32, 128), F32)
    line = jnp.zeros((8, 32), F32)
    for c in range(3):
        row = total[c : c + 1]
        rows = jnp.where(last, row, stored[c])
        column = column + rows * row
        line = line + lax.dot_general(
            jnp.broadcast_to(row, (8, 128)), rows, NT, precision=lax.Precision.HIGHEST, preferred_element_type=F32
        )
    column = jnp.sum(column, axis=1, keepdims=True)
    line = jnp.concatenate([line[0:1], jnp.zeros((1, 96), F32)], axis=1)
    lane = rows_of((32, 128), 1)
    full = jnp.where(lane == 30, column, jnp.where(last, line, gram[...]))
    tile = full[0:8]
    for b in range(1, 4):
        tile = tile + pltpu.roll(full[8 * b : 8 * b + 8], 32 * b, 1)
    out[...] = jnp.broadcast_to(tile[None], out.shape)


def fold(own, got, maps, stored, gram, grid):
    return pl.pallas_call(
        functools.partial(fold_kernel, grid),
        out_shape=[pltpu.VMEM((8, 128), F32), pltpu.VMEM(got.shape, F32)],
        in_specs=vmem(5),
        out_specs=vmem(2),
        name="fold",
    )(*here(own, got, maps, stored, gram))


def total_kernel(got, out):
    out[...] = jnp.broadcast_to(jnp.sum(got[...], axis=0)[None], out.shape)


def total_of(got, copies):
    return pl.pallas_call(
        total_kernel,
        out_shape=pltpu.VMEM((copies,) + got.shape[1:], F32),
        in_specs=vmem(1),
        out_specs=vmem(1)[0],
        name="total",
    )(*here(got))


def finish_kernel(entries, got, product, stored, result, correlations, norm):
    count = correlations.shape[1]
    packed = jnp.sum(got[...], axis=0) * (1.0 / entries)
    full = jnp.concatenate([packed] + [pltpu.roll(packed, 128 - 32 * b, 1) for b in range(1, 4)], axis=0)
    column = full[:, count : count + 1]
    line = full[count : count + 1, :]
    row = rows_of((32, 1))
    lane = rows_of((1, 128), 1)
    down = jnp.where(row < count, column, jnp.where(row == count, -1.0, 0.0))
    across = jnp.where(lane < count, line, jnp.where(lane == count, -1.0, 0.0))
    square = jnp.sum(jnp.where(rows_of((32, 128), 1) <= count, full * across * down, 0.0), axis=1, keepdims=True)
    length = jnp.sqrt(jnp.maximum(jnp.sum(square, axis=0, keepdims=True), 0.0) + 1e-06)
    norm[...] = length
    correlations[...] = line[:, 0:count]
    share = jnp.where(row < count, column, 0.0)
    for c in range(3):
        taken = jnp.sum(stored[c] * share, axis=0, keepdims=True)
        result[c, 0, 0] = (product[c : c + 1, :] - taken) / length


def finish(got, product, stored, shape, count, entries):
    return pl.pallas_call(
        functools.partial(finish_kernel, entries),
        out_shape=[
            jax.ShapeDtypeStruct(shape, F32),
            jax.ShapeDtypeStruct((1, count), F32),
            jax.ShapeDtypeStruct((1, 1), F32),
        ],
        in_specs=vmem(3),
        out_specs=vmem(3),
        name="finish",
    )(*here(got, product, stored))


def on_device(positions, basis, neighbours, used_count, kinds, map_x, map_y, map_z, table, fit_w1, fit_b1, fit_w2, fit_b2, fit_out):
    nx, ny, nz = (lax.axis_size(a) for a in ("gx", "gy", "gz"))
    plane = ("gx", "gy")
    up = [(i, (i + 1) % nz) for i in range(nz)]
    down = [(j, i) for i, j in up]

    def exchange(x):
        return lax.all_to_all(x, plane, 0, 0)

    packed = pack(positions, basis, map_x, map_y, nx * ny)
    raw = exchange(packed)
    table, _ = lax.optimization_barrier((table, packed))
    mixed, map_row = mixing(table, fit_w1, map_z)
    layers, lists, stored, gram = lists_of(fit_w2, fit_b1, fit_b2, fit_out, neighbours, used_count, kinds, basis)
    raw, map_row = lax.optimization_barrier((raw, map_row))
    tiles, message = assemble(raw, map_row, (nx, ny))
    below, above = lax.ppermute(message, "gz", up), lax.ppermute(message, "gz", down)
    products, outgoing = product(tiles, below, above, lists, (*mixed, *layers))
    below, above = lax.ppermute(outgoing, "gz", up), lax.ppermute(outgoing, "gz", down)
    own, shared = fold_z(products, below, above, map_row, nx * ny)
    hessian_vec, summary = fold(own, exchange(shared), raw, stored, gram, (nx, ny))
    summary = total_of(exchange(summary), nz)
    summary = lax.all_to_all(summary, "gz", 0, 0)
    entries = 3 * positions.shape[-1] * nx * ny * nz
    next_vector, correlations, vector_norm = finish(summary, hessian_vec, stored, positions.shape, basis.shape[0], entries)
    return next_vector, correlations.reshape(-1), vector_norm.reshape(())


def solution(mesh):
    bricks = P("gx", "gy", "gz", None)
    lists = P("gx", "gy", "gz", None, None)
    vector = P(None, "gx", "gy", "gz", None)
    return jax.shard_map(
        on_device,
        mesh=mesh,
        in_specs=(vector, P(None, None, "gx", "gy", "gz", None), lists, bricks, bricks, lists, lists, lists) + (P(),) * 6,
        out_specs=(vector, P(), P()),
        check_vma=False,
    )
```

```python
import functools

import jax
import jax.numpy as jnp
from jax import lax
from jax.experimental import pallas as pl
from jax.experimental.pallas import tpu as pltpu
from jax.sharding import PartitionSpec as P

F32 = jnp.float32
BF16 = jnp.bfloat16
LOG2E = 1.4426950408889634
NT = (((1,), (1,)), ((), ()))


def split(x):
    hi = x.astype(BF16)
    return hi, (x - hi.astype(F32)).astype(BF16)


def mm(a, b):
    return jnp.dot(a, b, preferred_element_type=F32)


def dot3(a, b):
    ah, al = a if isinstance(a, tuple) else split(a)
    bh, bl = b if isinstance(b, tuple) else split(b)
    return mm(ah, bh) + (mm(ah, bl) + mm(al, bh))


def lane_pick(table, index):
    return jnp.take_along_axis(table, index, axis=1, mode="promise_in_bounds")


def rows_of(shape, dim=0):
    return lax.broadcasted_iota(jnp.int32, shape, dim)


def halves(ref):
    return jnp.concatenate([ref[0, 0, 0, 0:1, :], ref[0, 0, 0, 1:2, :]], axis=1)


def fetch(sources, places, semaphores):
    copies = [pltpu.make_async_copy(x, y, semaphores.at[i]) for i, (x, y) in enumerate(zip(sources, places))]
    for copy in copies:
        copy.start()
    return copies


EXACT = dict(precision=lax.Precision.HIGHEST, preferred_element_type=F32)


def mixing_kernel(table_at, w1_at, map_at, u_hi, u_lo, ut_hi, ut_lo, map_row, table, w1t, map_z, outer, inner, k_hi, k_lo, semaphores):
    copies = fetch((table_at, map_at, w1_at), (table, map_z, w1t), semaphores)
    types, levels, width = table.shape
    hidden = w1t.shape[0]
    m2 = w1t.shape[1] // width
    count = types * levels * levels
    copies[0].wait()
    tall = table[...].reshape(types * levels, width)
    tall = jnp.concatenate([tall, jnp.zeros((types * levels, 128 - width), F32)], axis=1)
    tall = jnp.concatenate([tall, jnp.zeros((128 - types * levels, 128), F32)], axis=0).T
    column = rows_of((128, count), 1)
    row = rows_of((128, count))
    kind = column // (levels * levels)
    first = jnp.where(row == kind * levels + (column // levels) % levels, 1.0, 0.0)
    second = jnp.where(row == kind * levels + column % levels, 1.0, 0.0)
    outer[...] = jnp.dot(tall, first, **EXACT) * 0.5
    inner[...] = jnp.dot(tall, second, **EXACT) * 0.5
    near = inner[0:m2, :] * 2.0
    far = outer[0:m2, :] * 2.0

    def kron(m, carry):
        value = jnp.broadcast_to(outer[pl.ds(m, 1), :], (m2, count)) * near + jnp.broadcast_to(inner[pl.ds(m, 1), :], (m2, count)) * far
        hi, lo = split(value)
        at = pl.ds(pl.multiple_of(m * m2, m2), m2)
        k_hi[at, :] = hi
        k_lo[at, :] = lo
        return carry

    lax.fori_loop(0, width, kron, 0, unroll=4)
    copies[1].wait()
    map_row[...] = halves(map_z)
    copies[2].wait()
    full = dot3(w1t[...], (k_hi[...], k_lo[...]))
    full = jnp.concatenate([full, jnp.zeros((256 - hidden, count), F32)], axis=0)
    hi, lo = split(full)
    ut_hi[...] = hi
    ut_lo[...] = lo
    hi, lo = split(full.T)
    u_hi[...] = hi
    u_lo[...] = lo


def lists_kernel(w2_at, b1_at, b2_at, wo_at, ids_at, counts_at, kinds_at, basis_at, w2_hi, w2_lo, w2t_hi, w2t_lo, cols, ids_t, count_row, kind_row, stored, gram, w2, b1, b2, wo, ids, counts, kinds, basis, pad, semaphores):
    places = (w2, b1, b2, wo, ids, counts, kinds, basis)
    copies = fetch((w2_at, b1_at, b2_at, wo_at, ids_at, counts_at, kinds_at, basis_at), places, semaphores)
    hidden = w2.shape[0]
    pad[...] = jnp.zeros_like(pad)
    stored[...] = jnp.zeros_like(stored)
    gram[...] = jnp.zeros_like(gram)
    for copy in copies:
        copy.wait()
    pad[0:hidden, 0:hidden] = w2[...]
    hi, lo = split(pad[...])
    w2_hi[...] = hi
    w2_lo[...] = lo
    hi, lo = split(pad[...].T)
    w2t_hi[...] = hi
    w2t_lo[...] = lo
    pad[0:128, :] = jnp.zeros((128, pad.shape[1]), F32)
    pad[0:1, 0:hidden] = b1[...]
    pad[1:2, 0:hidden] = b2[...]
    pad[2:3, 0:hidden] = wo[...]
    cols[...] = pad[0:128, :].T
    ids_t[...] = ids[0, 0, 0].astype(F32).T.astype(jnp.int32)
    count_row[...] = counts[0, 0]
    kind_row[...] = kinds[0, 0]
    total = jnp.zeros((32, 32), F32)
    for c in range(3):
        for k in range(basis.shape[0]):
            stored[c, k : k + 1, :] = basis[k, c, 0, 0]
        total = total + lax.dot_general(stored[c], stored[c], NT, **EXACT)
    gram[:, 0:32] = total


def vmem(n):
    return [pl.BlockSpec(memory_space=pltpu.VMEM)] * n


def here(*arrays):
    return [pltpu.with_memory_space_constraint(a, pltpu.VMEM) for a in arrays]


def from_hbm(kernel, name, shapes, scratch, *arrays):
    return pl.pallas_call(
        kernel,
        out_shape=[pltpu.VMEM(s, d) for s, d in shapes],
        in_specs=[pl.BlockSpec(memory_space=pltpu.HBM)] * len(arrays),
        out_specs=vmem(len(shapes)),
        scratch_shapes=[pltpu.VMEM(a.shape, a.dtype) for a in arrays] + scratch + [pltpu.SemaphoreType.DMA((len(arrays),))],
        name=name,
    )(*(pltpu.with_memory_space_constraint(a, pltpu.HBM) for a in arrays))


def mixing(table, w1, map_z):
    hp = 256
    count = table.shape[0] * table.shape[1] ** 2
    shapes = [((count, hp), BF16)] * 2 + [((hp, count), BF16)] * 2 + [((1, 128), jnp.int32)]
    scratch = [pltpu.VMEM((128, count), F32)] * 2 + [pltpu.VMEM((w1.shape[0], count), BF16)] * 2
    *weights, map_row = from_hbm(mixing_kernel, "mixing", shapes, scratch, table, w1.T, map_z)
    return weights, map_row


def lists_of(w2, b1, b2, wo, ids, counts, kinds, basis):
    hp = 256
    row = ((1, 128), jnp.int32)
    shapes = [((hp, hp), BF16)] * 4 + [((hp, 128), F32), ((ids.shape[-1], 128), jnp.int32), row, row, ((3, 32, 128), F32), ((32, 128), F32)]
    scratch = [pltpu.VMEM((hp, hp), F32)]
    done = from_hbm(lists_kernel, "lists", shapes, scratch, w2, b1[None], b2[None], wo[None], ids, counts, kinds, basis)
    return done[:5], done[5:8], done[8], done[9]


def shifted_ghosts(below, above, coord, rows):
    lower = rows_of((rows, 128), 1) < 64
    step = jnp.where(rows_of((rows, 128)) == coord, 1.0, 0.0)
    return jnp.where(lower, below - step, above + step)


def product_kernel(tiles, below, above, ids_t, counts, kinds, u_hi, u_lo, ut_hi, ut_lo, w2_hi, w2_lo, w2t_hi, w2t_lo, cols, out, sent, xv, edge, phis, acc, pairs, grads, force, lows):
    n_slots = ids_t.shape[0]
    levels = 16
    gap = levels - 1
    blocks = n_slots // 8
    xv[0:3] = tiles[...]
    xv[3] = shifted_ghosts(pltpu.roll(below[...], 64, 1), pltpu.roll(above[...], 64, 1), 2, 8)
    count_row = jnp.broadcast_to(counts[...], (8, 128))

    def geometry(nb, carry):
        rows = pl.ds(pl.multiple_of(nb * 8, 8), 8)
        index = ids_t[rows, :]
        low = index & 127
        high = index >> 7
        lows[rows, :] = (index & 63).astype(F32)
        near = []
        for f in range(6):
            picks = [lane_pick(jnp.broadcast_to(xv[q, f : f + 1, :], (8, 128)), low) for q in range(4)]
            value = jnp.where(high < 2, jnp.where(high == 0, picks[0], picks[1]), jnp.where(high == 2, picks[2], picks[3]))
            near.append(value - jnp.broadcast_to(xv[0, f : f + 1, :], (8, 128)))
        d, dd = near[:3], near[3:]
        square = d[0] * d[0] + d[1] * d[1] + d[2] * d[2]
        rate = 2.0 * (d[0] * dd[0] + d[1] * dd[1] + d[2] * dd[2])
        wide = square + 0.01
        inverse = lax.rsqrt(wide)
        half = 0.5 / wide
        live = (rows_of((8, 128)) + nb * 8) < count_row
        s = jnp.where(live, jnp.exp(-square) * inverse, 0.0)
        tau = s * inverse
        sq = -s * (1.0 + half)
        tq = -tau * (1.0 + 2.0 * half)
        share = 1.0 / (1.0 + s)
        us = gap * share * share
        for c in range(3):
            edge[c, rows, :] = d[c]
            edge[3 + c, rows, :] = dd[c]
            edge[9 + c, rows, :] = tau * d[c]
            edge[13 + c, rows, :] = tq * rate * d[c] + tau * dd[c]
        edge[6, rows, :] = gap * s * share
        edge[7, rows, :] = us * sq * rate
        edge[8, rows, :] = s
        edge[12, rows, :] = sq * rate
        edge[16, rows, :] = tau
        edge[17, rows, :] = half
        edge[18, rows, :] = rate
        return carry

    lax.fori_loop(0, blocks, geometry, 0, unroll=8)

    def pooling(kk, carry):
        sums = [[jnp.zeros((8, 128), F32) for _ in range(8)] for _ in range(2)]
        for nb in range(blocks):
            rows = pl.ds(nb * 8, 8)
            u = edge[6, rows, :]
            w = -2.0 * edge[7, rows, :]
            radial = [edge[8 + a, rows, :] for a in range(4)]
            moved = [edge[12 + a, rows, :] for a in range(4)]
            for side in range(2):
                z = u - (2 * kk + side).astype(F32)
                phi = jnp.exp2(z * (z * (-LOG2E)))
                phis[2 * kk + side, rows, :] = phi
                dphi = phi * (z * w)
                for a in range(4):
                    sums[side][a] = sums[side][a] + phi * radial[a]
                    sums[side][4 + a] = sums[side][4 + a] + (dphi * radial[a] + phi * moved[a])
        for side in range(2):
            for a in range(8):
                acc[pl.ds(pl.multiple_of((a * levels + 2 * kk + side) * 8, 8), 8), :] = sums[side][a]
        return carry

    lax.fori_loop(0, levels // 2, pooling, 0)
    pooled = acc[pl.ds(0, 128, stride=8), :]
    for s in range(1, 8):
        pooled = pooled + acc[pl.ds(s, 128, stride=8), :]
    pooled = pooled * (1.0 / n_slots)
    grads[...] = pooled
    kind = jnp.concatenate([kinds[...], kinds[...]], axis=1)
    p = [pooled[a * 16 : (a + 1) * 16] for a in range(4)]
    dp = [pooled[64 + a * 16 : 64 + (a + 1) * 16] for a in range(4)]
    for k in range(levels):
        value = jnp.zeros((16, 128), F32)
        moved = jnp.zeros((16, 128), F32)
        for a in range(4):
            value = value + p[a] * jnp.broadcast_to(grads[a * 16 + k : a * 16 + k + 1, :], (16, 128))
            moved = moved + p[a] * jnp.broadcast_to(grads[64 + a * 16 + k : 64 + a * 16 + k + 1, :], (16, 128))
        pairs[k * 16 : (k + 1) * 16, 0:128] = value
        pairs[k * 16 : (k + 1) * 16, 128:256] = 2.0 * moved
    both = split(pairs[...])
    z1 = jnp.where(
        kind == 1,
        dot3((ut_hi[:, 256:512], ut_lo[:, 256:512]), both),
        dot3((ut_hi[:, 0:256], ut_lo[:, 0:256]), both),
    )
    h1 = jnp.tanh(z1[:, 0:128] + cols[:, 0:1])
    slope1 = 1.0 - h1 * h1
    dh1 = slope1 * z1[:, 128:256]
    z2 = dot3((w2t_hi[...], w2t_lo[...]), jnp.concatenate([h1, dh1], axis=1))
    t2 = jnp.tanh(z2[:, 0:128] + cols[:, 1:2])
    slope2 = 1.0 - t2 * t2
    read = cols[:, 2:3]
    delta2 = slope2 * read
    ddelta2 = -2.0 * t2 * (slope2 * z2[:, 128:256]) * read
    back = dot3((w2_hi[...], w2_lo[...]), jnp.concatenate([delta2, ddelta2], axis=1))
    e1 = back[:, 0:128] + read
    delta1 = slope1 * e1
    ddelta1 = slope1 * back[:, 128:256] - 2.0 * h1 * dh1 * e1
    both = split(jnp.concatenate([delta1, ddelta1], axis=1))
    pairs[...] = jnp.where(
        kind == 1,
        dot3((u_hi[256:512, :], u_lo[256:512, :]), both),
        dot3((u_hi[0:256, :], u_lo[0:256, :]), both),
    )
    g = [jnp.zeros((16, 128), F32) for _ in range(4)]
    dg = [jnp.zeros((16, 128), F32) for _ in range(4)]
    for k in range(levels):
        m = pairs[k * 16 : (k + 1) * 16, 0:128]
        dm = pairs[k * 16 : (k + 1) * 16, 128:256]
        for a in range(4):
            row = jnp.broadcast_to(grads[a * 16 + k : a * 16 + k + 1, :], (16, 128))
            drow = jnp.broadcast_to(grads[64 + a * 16 + k : 64 + a * 16 + k + 1, :], (16, 128))
            g[a] = g[a] + m * row
            dg[a] = dg[a] + (dm * row + m * drow)
    scale = 2.0 / n_slots
    for a in range(4):
        grads[a * 16 : (a + 1) * 16, :] = g[a] * scale
        grads[64 + a * 16 : 64 + (a + 1) * 16, :] = dg[a] * scale

    def backward(nb, centre):
        rows = pl.ds(pl.multiple_of(nb * 8, 8), 8)
        u = edge[6, rows, :]
        zero = jnp.zeros((8, 128), F32)
        s0, s1, s2, r0, r1 = ([zero] * 4 for _ in range(5))
        for k in range(levels):
            z = u - float(k)
            phi = phis[k, rows, :]
            phi1 = z * phi
            phi2 = z * phi1
            for a in range(4):
                row = jnp.broadcast_to(grads[a * 16 + k : a * 16 + k + 1, :], (8, 128))
                drow = jnp.broadcast_to(grads[64 + a * 16 + k : 64 + a * 16 + k + 1, :], (8, 128))
                s0[a] = s0[a] + row * phi
                s1[a] = s1[a] + row * phi1
                s2[a] = s2[a] + row * phi2
                r0[a] = r0[a] + drow * phi
                r1[a] = r1[a] + drow * phi1
        d = [edge[c, rows, :] for c in range(3)]
        dd = [edge[3 + c, rows, :] for c in range(3)]
        du = edge[7, rows, :]
        radial = [edge[8 + a, rows, :] for a in range(4)]
        moved = [edge[12 + a, rows, :] for a in range(4)]
        s = radial[0]
        tau = edge[16, rows, :]
        half = edge[17, rows, :]
        rate = edge[18, rows, :]
        one = 1.0 + half
        two = one + half
        sq = -s * one
        sqq = s * (one * one + 2.0 * half * half)
        tq = -tau * two
        tqq = tau * (two * two + 4.0 * half * half)
        share = 1.0 / (1.0 + s)
        us = gap * share * share
        uq = us * sq
        uqq = us * (sqq - 2.0 * share * sq * sq)
        a1 = [-2.0 * v for v in s1]
        da = [r0[a] + a1[a] * du for a in range(4)]
        da1 = [-2.0 * r1[a] + (4.0 * s2[a] - 2.0 * s0[a]) * du for a in range(4)]
        a1r = a1[0] * radial[0] + a1[1] * radial[1] + (a1[2] * radial[2] + a1[3] * radial[3])
        ad = s0[1] * d[0] + s0[2] * d[1] + s0[3] * d[2]
        turned = da1[0] * radial[0] + a1[0] * moved[0]
        for a in range(1, 4):
            turned = turned + (da1[a] * radial[a] + a1[a] * moved[a])
        dad = da[1] * d[0] + s0[1] * dd[0]
        for c in range(1, 3):
            dad = dad + (da[c + 1] * d[c] + s0[c + 1] * dd[c])
        eq = uq * a1r + sq * s0[0] + tq * ad
        deq = rate * (uqq * a1r + sqq * s0[0] + tqq * ad) + uq * turned + sq * da[0] + tq * dad
        dtau = tq * rate
        result = []
        for c in range(3):
            value = 2.0 * (dd[c] * eq + d[c] * deq) + (dtau * s0[c + 1] + tau * da[c + 1])
            hi = value.astype(BF16).astype(F32)
            force[c, rows, :] = hi
            force[3 + c, rows, :] = value - hi
            result.append(centre[c] + value)
        return tuple(result)

    zero = jnp.zeros((8, 128), F32)
    centre = lax.fori_loop(0, blocks, backward, (zero, zero, zero), unroll=2)
    row8 = rows_of((8, 128))
    rows16 = [(rows_of((16, 128)) + 16 * rg).astype(F32).astype(BF16) for rg in range(4)]
    on = jnp.ones((16, 128), BF16)
    off = jnp.zeros((16, 128), BF16)
    chunk = 32

    def scatter(step, total):
        lefts, hots = [], []
        for i in range(chunk):
            n = step * chunk + i
            hit = (jnp.broadcast_to(ids_t[pl.ds(n, 1), :], (8, 128)) >> 6) == row8
            stack = [jnp.where(hit, jnp.broadcast_to(force[c, pl.ds(n, 1), :], (8, 128)), 0.0) for c in range(6)]
            lefts.append(jnp.concatenate(stack, axis=0).astype(BF16))
            low = jnp.broadcast_to(lows[pl.ds(n, 1), :], (16, 128)).astype(BF16)
            hots.append(jnp.concatenate([jnp.where(low == r, on, off) for r in rows16], axis=0))
        return total + lax.dot_general(jnp.concatenate(lefts, axis=1), jnp.concatenate(hots, axis=1), NT, preferred_element_type=F32)

    total = lax.fori_loop(0, n_slots // chunk, scatter, jnp.zeros((48, 64), F32), unroll=2)
    out[...] = jnp.zeros_like(out)
    sent[...] = jnp.zeros_like(sent)
    for c in range(3):
        both = total[c * 8 : c * 8 + 8] + total[24 + c * 8 : 32 + c * 8]
        for q in range(4):
            row = jnp.concatenate([both[2 * q : 2 * q + 1], both[2 * q + 1 : 2 * q + 2]], axis=1)
            if q == 0:
                row = row - jnp.sum(centre[c], axis=0, keepdims=True)
            if q < 3:
                out[q, c : c + 1, :] = row
            else:
                sent[c : c + 1, :] = row


def product(tiles, below, above, lists, weights):
    n = lists[0].shape[0]
    return pl.pallas_call(
        product_kernel,
        out_shape=[pltpu.VMEM((3, 8, 128), F32), pltpu.VMEM((8, 128), F32)],
        in_specs=vmem(15),
        out_specs=vmem(2),
        scratch_shapes=[
            pltpu.VMEM((4, 8, 128), F32),
            pltpu.VMEM((19, n, 128), F32),
            pltpu.VMEM((16, n, 128), F32),
            pltpu.VMEM((1024, 128), F32),
            pltpu.VMEM((256, 256), F32),
            pltpu.VMEM((128, 128), F32),
            pltpu.VMEM((6, n, 128), F32),
            pltpu.VMEM((n, 128), F32),
        ],
        name="product",
    )(*here(tiles, below, above, *lists, *weights))


def pack_kernel(places_at, basis_at, map_x_at, map_y_at, out, places, tangent, map_x, map_y, semaphores):
    last = basis_at.shape[0] - 1
    copies = fetch((places_at, basis_at.at[last], map_x_at, map_y_at), (places, tangent, map_x, map_y), semaphores)
    for copy in copies:
        copy.wait()
    rows = [places[c, 0, 0] for c in range(3)] + [tangent[c, 0, 0] for c in range(3)]
    rows += [halves(map_x).astype(F32), halves(map_y).astype(F32)]
    out[...] = jnp.broadcast_to(jnp.concatenate(rows, axis=0)[None], out.shape)


def pack(positions, basis, map_x, map_y, bricks):
    arrays = (positions, basis, map_x, map_y)
    return pl.pallas_call(
        pack_kernel,
        out_shape=pltpu.VMEM((bricks, 8, 128), F32),
        in_specs=[pl.BlockSpec(memory_space=pltpu.HBM)] * 4,
        out_specs=vmem(1)[0],
        scratch_shapes=[
            pltpu.VMEM(positions.shape, F32),
            pltpu.VMEM(basis.shape[1:], F32),
            pltpu.VMEM(map_x.shape, jnp.int32),
            pltpu.VMEM(map_y.shape, jnp.int32),
            pltpu.SemaphoreType.DMA((4,)),
        ],
        name="pack",
    )(*(pltpu.with_memory_space_constraint(a, pltpu.HBM) for a in arrays))


def brick_reader(grid):
    nx, ny = grid
    px, py = lax.axis_index("gx"), lax.axis_index("gy")

    def at(ref, dx, dy):
        x = lax.rem(px + (dx + nx), nx)
        y = lax.rem(py + (dy + ny), ny)
        return ref[x * ny + y]

    return at


def as_index(row):
    return jnp.broadcast_to(row, (8, 128)).astype(jnp.int32)


def turn(x):
    return pltpu.roll(x, 64, 1)


def assemble_kernel(grid, got, map_z, tiles, message):
    at = brick_reader(grid)
    lower = rows_of((8, 128), 1) < 64
    row = rows_of((8, 128))
    step_x = jnp.where(row == 0, 1.0, 0.0)
    step_y = jnp.where(row == 1, 1.0, 0.0)
    middle, ghosts, index = {}, {}, {}
    for dy in (-1, 0, 1):
        own, low, high = at(got, 0, dy), at(got, -1, dy), at(got, 1, dy)
        from_low = lane_pick(low, turn(as_index(low[6:7])))
        from_high = lane_pick(high, turn(as_index(high[6:7])))
        middle[dy] = own
        ghosts[dy] = jnp.where(lower, from_low - step_x, from_high + step_x)
        index[dy] = turn(as_index(own[7:8]))

    def second(dy):
        low = index[dy] & 127
        return jnp.where(index[dy] < 128, lane_pick(middle[dy], low), lane_pick(ghosts[dy], low))

    third = jnp.where(lower, second(-1) - step_y, second(1) + step_y)
    tiles[0] = middle[0]
    tiles[1] = ghosts[0]
    tiles[2] = third
    chosen = jnp.broadcast_to(map_z[...], (8, 128))
    low = chosen & 127
    message[...] = jnp.where(
        chosen < 128, lane_pick(middle[0], low), jnp.where(chosen < 256, lane_pick(ghosts[0], low), lane_pick(third, low))
    )


def assemble(got, map_z, grid):
    return pl.pallas_call(
        functools.partial(assemble_kernel, grid),
        out_shape=[pltpu.VMEM((3, 8, 128), F32), pltpu.VMEM((8, 128), F32)],
        in_specs=vmem(2),
        out_specs=vmem(2),
        name="assemble",
    )(*here(got, map_z))


def thirds(x):
    hi, rest = x.astype(BF16), x
    rest = x - hi.astype(F32)
    mid = rest.astype(BF16)
    low = (rest - mid.astype(F32)).astype(BF16)
    return jnp.concatenate([hi.astype(F32), mid.astype(F32), low.astype(F32)], axis=0).astype(BF16)


def spread_columns(values, index, columns, first):
    target = rows_of((columns, 128)) + first
    hot = jnp.where(jnp.broadcast_to(index, (columns, 128)) == target, 1.0, 0.0).astype(BF16)
    both = lax.dot_general(thirds(values), hot, NT, preferred_element_type=F32)
    return both[0:8] + (both[8:16] + both[16:24])


def fold_z_kernel(products, below, above, map_z, own, out):
    lower = rows_of((8, 128), 1) < 64
    value = jnp.where(lower, turn(below[...]), turn(above[...]))
    added = spread_columns(value, map_z[...], 384, 0)
    own[...] = products[0] + added[:, 0:128]
    first = products[1] + added[:, 128:256]
    second = products[2] + added[:, 256:384]
    tile = jnp.concatenate([first[0:3], second[0:3], jnp.zeros((2, 128), F32)], axis=0)
    out[...] = jnp.broadcast_to(tile[None], out.shape)


def fold_z(products, below, above, map_z, bricks):
    return pl.pallas_call(
        fold_z_kernel,
        out_shape=[pltpu.VMEM((8, 128), F32), pltpu.VMEM((bricks, 8, 128), F32)],
        in_specs=vmem(4),
        out_specs=vmem(2),
        name="fold_z",
    )(*here(products, below, above, map_z))


def fold_kernel(grid, own, got, maps, stored, gram, product, out):
    at = brick_reader(grid)
    lower = rows_of((8, 128), 1) < 64

    def from_y(dx):
        return jnp.where(lower, turn(at(got, dx, -1)), turn(at(got, dx, 1)))

    def second(value):
        return jnp.concatenate([value[3:6], jnp.zeros((5, 128), F32)], axis=0)

    def ghost(dx):
        index = at(maps, dx, 0)[7:8].astype(jnp.int32)
        return at(got, dx, 0) + spread_columns(second(from_y(dx)), index, 128, 128)

    mine = at(maps, 0, 0)
    total = own[...] + spread_columns(second(from_y(0)), mine[7:8].astype(jnp.int32), 128, 0)
    from_x = jnp.where(lower, turn(ghost(-1)), turn(ghost(1)))
    total = total + spread_columns(from_x, mine[6:7].astype(jnp.int32), 128, 0)
    product[...] = total
    last = rows_of((32, 128)) == 30
    column = jnp.zeros((32, 128), F32)
    for c in range(3):
        row = total[c : c + 1]
        column = column + jnp.where(last, row, stored[c]) * row
    column = jnp.sum(column, axis=1, keepdims=True)
    full = jnp.where(rows_of((32, 128), 1) == 30, column, gram[...])
    tile = full[0:8]
    for b in range(1, 4):
        tile = tile + pltpu.roll(full[8 * b : 8 * b + 8], 32 * b, 1)
    out[...] = jnp.broadcast_to(tile[None], out.shape)


def fold(own, got, maps, stored, gram, grid):
    return pl.pallas_call(
        functools.partial(fold_kernel, grid),
        out_shape=[pltpu.VMEM((8, 128), F32), pltpu.VMEM(got.shape, F32)],
        in_specs=vmem(5),
        out_specs=vmem(2),
        name="fold",
    )(*here(own, got, maps, stored, gram))


def total_kernel(got, out):
    out[...] = jnp.broadcast_to(jnp.sum(got[...], axis=0)[None], out.shape)


def total_of(got, copies):
    return pl.pallas_call(
        total_kernel,
        out_shape=pltpu.VMEM((copies,) + got.shape[1:], F32),
        in_specs=vmem(1),
        out_specs=vmem(1)[0],
        name="total",
    )(*here(got))


def finish_kernel(entries, got, product, stored, result, correlations, norm):
    count = correlations.shape[1]
    packed = jnp.sum(got[...], axis=0) * (1.0 / entries)
    full = jnp.concatenate([packed] + [pltpu.roll(packed, 128 - 32 * b, 1) for b in range(1, 4)], axis=0)
    column = full[:, count : count + 1]
    line = jnp.sum(jnp.where(rows_of((32, 128)) == rows_of((32, 128), 1), column, 0.0), axis=0, keepdims=True)
    row = rows_of((32, 1))
    lane = rows_of((1, 128), 1)
    down = jnp.where(row < count, column, jnp.where(row == count, -1.0, 0.0))
    across = jnp.where(lane < count, line, jnp.where(lane == count, -2.0, 0.0))
    size = jnp.where(row < count, full * across * down, jnp.where((row == count) & (lane == count), full, 0.0))
    size = jnp.where(rows_of((32, 128), 1) <= count, size, 0.0)
    size = jnp.sum(jnp.sum(size, axis=1, keepdims=True), axis=0, keepdims=True)
    length = jnp.sqrt(jnp.maximum(size, 0.0) + 1e-06)
    norm[...] = length
    correlations[...] = line[:, 0:count]
    share = jnp.where(row < count, column, 0.0)
    for c in range(3):
        taken = jnp.sum(stored[c] * share, axis=0, keepdims=True)
        result[c, 0, 0] = (product[c : c + 1, :] - taken) / length


def finish(got, product, stored, shape, count, entries):
    return pl.pallas_call(
        functools.partial(finish_kernel, entries),
        out_shape=[
            jax.ShapeDtypeStruct(shape, F32),
            jax.ShapeDtypeStruct((1, count), F32),
            jax.ShapeDtypeStruct((1, 1), F32),
        ],
        in_specs=vmem(3),
        out_specs=vmem(3),
        name="finish",
    )(*here(got, product, stored))


def on_device(positions, basis, neighbours, used_count, kinds, map_x, map_y, map_z, table, fit_w1, fit_b1, fit_w2, fit_b2, fit_out):
    nx, ny, nz = (lax.axis_size(a) for a in ("gx", "gy", "gz"))
    plane = ("gx", "gy")
    up = [(i, (i + 1) % nz) for i in range(nz)]
    down = [(j, i) for i, j in up]

    def exchange(x):
        return lax.all_to_all(x, plane, 0, 0)

    packed = pack(positions, basis, map_x, map_y, nx * ny)
    raw = exchange(packed)
    table, _ = lax.optimization_barrier((table, packed))
    mixed, map_row = mixing(table, fit_w1, map_z)
    layers, lists, stored, gram = lists_of(fit_w2, fit_b1, fit_b2, fit_out, neighbours, used_count, kinds, basis)
    raw, map_row = lax.optimization_barrier((raw, map_row))
    tiles, message = assemble(raw, map_row, (nx, ny))
    below, above = lax.ppermute(message, "gz", up), lax.ppermute(message, "gz", down)
    products, outgoing = product(tiles, below, above, lists, (*mixed, *layers))
    below, above = lax.ppermute(outgoing, "gz", up), lax.ppermute(outgoing, "gz", down)
    own, shared = fold_z(products, below, above, map_row, nx * ny)
    hessian_vec, summary = fold(own, exchange(shared), raw, stored, gram, (nx, ny))
    summary = total_of(exchange(summary), nz)
    summary = lax.all_to_all(summary, "gz", 0, 0)
    entries = 3 * positions.shape[-1] * nx * ny * nz
    next_vector, correlations, vector_norm = finish(summary, hessian_vec, stored, positions.shape, basis.shape[0], entries)
    return next_vector, correlations.reshape(-1), vector_norm.reshape(())


def solution(mesh):
    bricks = P("gx", "gy", "gz", None)
    lists = P("gx", "gy", "gz", None, None)
    vector = P(None, "gx", "gy", "gz", None)
    return jax.shard_map(
        on_device,
        mesh=mesh,
        in_specs=(vector, P(None, None, "gx", "gy", "gz", None), lists, bricks, bricks, lists, lists, lists) + (P(),) * 6,
        out_specs=(vector, P(), P()),
        check_vma=False,
    )
```

```python
import functools

import jax
import jax.numpy as jnp
from jax import lax
from jax.experimental import pallas as pl
from jax.experimental.pallas import tpu as pltpu
from jax.sharding import PartitionSpec as P

F32 = jnp.float32
BF16 = jnp.bfloat16
LOG2E = 1.4426950408889634
NT = (((1,), (1,)), ((), ()))


def split(x):
    hi = x.astype(BF16)
    return hi, (x - hi.astype(F32)).astype(BF16)


def mm(a, b):
    return jnp.dot(a, b, preferred_element_type=F32)


def dot3(a, b):
    ah, al = a if isinstance(a, tuple) else split(a)
    bh, bl = b if isinstance(b, tuple) else split(b)
    return mm(ah, bh) + (mm(ah, bl) + mm(al, bh))


def lane_pick(table, index):
    return jnp.take_along_axis(table, index, axis=1, mode="promise_in_bounds")


def rows_of(shape, dim=0):
    return lax.broadcasted_iota(jnp.int32, shape, dim)


def halves(ref):
    return jnp.concatenate([ref[0, 0, 0, 0:1, :], ref[0, 0, 0, 1:2, :]], axis=1)


def fetch(sources, places, semaphores):
    copies = [pltpu.make_async_copy(x, y, semaphores.at[i]) for i, (x, y) in enumerate(zip(sources, places))]
    for copy in copies:
        copy.start()
    return copies


EXACT = dict(precision=lax.Precision.HIGHEST, preferred_element_type=F32)


def mixing_kernel(table_at, w1_at, map_at, basis_at, u_hi, u_lo, ut_hi, ut_lo, map_row, stored, table, w1t, map_z, basis, outer, inner, k_hi, k_lo, semaphores):
    copies = fetch((table_at, map_at, w1_at, basis_at), (table, map_z, w1t, basis), semaphores)
    stored[...] = jnp.zeros_like(stored)
    types, levels, width = table.shape
    hidden = w1t.shape[0]
    m2 = w1t.shape[1] // width
    count = types * levels * levels
    copies[0].wait()
    tall = table[...].reshape(types * levels, width)
    tall = jnp.concatenate([tall, jnp.zeros((types * levels, 128 - width), F32)], axis=1)
    tall = jnp.concatenate([tall, jnp.zeros((128 - types * levels, 128), F32)], axis=0).T
    column = rows_of((128, count), 1)
    row = rows_of((128, count))
    kind = column // (levels * levels)
    first = jnp.where(row == kind * levels + (column // levels) % levels, 1.0, 0.0)
    second = jnp.where(row == kind * levels + column % levels, 1.0, 0.0)
    outer[...] = jnp.dot(tall, first, **EXACT) * 0.5
    inner[...] = jnp.dot(tall, second, **EXACT) * 0.5
    near = inner[0:m2, :] * 2.0
    far = outer[0:m2, :] * 2.0

    def kron(m, carry):
        value = jnp.broadcast_to(outer[pl.ds(m, 1), :], (m2, count)) * near + jnp.broadcast_to(inner[pl.ds(m, 1), :], (m2, count)) * far
        hi, lo = split(value)
        at = pl.ds(pl.multiple_of(m * m2, m2), m2)
        k_hi[at, :] = hi
        k_lo[at, :] = lo
        return carry

    lax.fori_loop(0, width, kron, 0, unroll=4)
    copies[1].wait()
    map_row[...] = halves(map_z)
    copies[3].wait()
    for c in range(3):
        for k in range(basis.shape[0]):
            stored[c, k : k + 1, :] = basis[k, c, 0, 0]
    copies[2].wait()
    full = dot3(w1t[...], (k_hi[...], k_lo[...]))
    full = jnp.concatenate([full, jnp.zeros((256 - hidden, count), F32)], axis=0)
    hi, lo = split(full)
    ut_hi[...] = hi
    ut_lo[...] = lo
    hi, lo = split(full.T)
    u_hi[...] = hi
    u_lo[...] = lo


def lists_kernel(w2_at, b1_at, b2_at, wo_at, ids_at, counts_at, kinds_at, stored, w2_hi, w2_lo, w2t_hi, w2t_lo, cols, ids_t, count_row, kind_row, gram, w2, b1, b2, wo, ids, counts, kinds, pad, semaphores):
    places = (w2, b1, b2, wo, ids, counts, kinds)
    copies = fetch((w2_at, b1_at, b2_at, wo_at, ids_at, counts_at, kinds_at), places, semaphores)
    hidden = w2.shape[0]
    pad[...] = jnp.zeros_like(pad)
    gram[...] = jnp.zeros_like(gram)
    for copy in copies:
        copy.wait()
    pad[0:hidden, 0:hidden] = w2[...]
    hi, lo = split(pad[...])
    w2_hi[...] = hi
    w2_lo[...] = lo
    hi, lo = split(pad[...].T)
    w2t_hi[...] = hi
    w2t_lo[...] = lo
    pad[0:128, :] = jnp.zeros((128, pad.shape[1]), F32)
    pad[0:1, 0:hidden] = b1[...]
    pad[1:2, 0:hidden] = b2[...]
    pad[2:3, 0:hidden] = wo[...]
    cols[...] = pad[0:128, :].T
    ids_t[...] = ids[0, 0, 0].astype(F32).T.astype(jnp.int32)
    count_row[...] = counts[0, 0]
    kind_row[...] = kinds[0, 0]
    total = jnp.zeros((32, 32), F32)
    for c in range(3):
        total = total + lax.dot_general(stored[c], stored[c], NT, **EXACT)
    gram[:, 0:32] = total


def vmem(n):
    return [pl.BlockSpec(memory_space=pltpu.VMEM)] * n


def here(*arrays):
    return [pltpu.with_memory_space_constraint(a, pltpu.VMEM) for a in arrays]


def from_hbm(kernel, name, shapes, scratch, *arrays, held=()):
    return pl.pallas_call(
        kernel,
        out_shape=[pltpu.VMEM(s, d) for s, d in shapes],
        in_specs=[pl.BlockSpec(memory_space=pltpu.HBM)] * len(arrays) + vmem(len(held)),
        out_specs=vmem(len(shapes)),
        scratch_shapes=[pltpu.VMEM(a.shape, a.dtype) for a in arrays] + scratch + [pltpu.SemaphoreType.DMA((len(arrays),))],
        name=name,
    )(*(pltpu.with_memory_space_constraint(a, pltpu.HBM) for a in arrays), *here(*held))


def mixing(table, w1, map_z, basis):
    hp = 256
    count = table.shape[0] * table.shape[1] ** 2
    shapes = [((count, hp), BF16)] * 2 + [((hp, count), BF16)] * 2 + [((1, 128), jnp.int32), ((3, 32, 128), F32)]
    scratch = [pltpu.VMEM((128, count), F32)] * 2 + [pltpu.VMEM((w1.shape[0], count), BF16)] * 2
    *weights, map_row, stored = from_hbm(mixing_kernel, "mixing", shapes, scratch, table, w1.T, map_z, basis)
    return weights, map_row, stored


def lists_of(w2, b1, b2, wo, ids, counts, kinds, stored):
    hp = 256
    row = ((1, 128), jnp.int32)
    shapes = [((hp, hp), BF16)] * 4 + [((hp, 128), F32), ((ids.shape[-1], 128), jnp.int32), row, row, ((32, 128), F32)]
    scratch = [pltpu.VMEM((hp, hp), F32)]
    done = from_hbm(lists_kernel, "lists", shapes, scratch, w2, b1[None], b2[None], wo[None], ids, counts, kinds, held=(stored,))
    return done[:5], done[5:8], done[8]


def shifted_ghosts(below, above, coord, rows):
    lower = rows_of((rows, 128), 1) < 64
    step = jnp.where(rows_of((rows, 128)) == coord, 1.0, 0.0)
    return jnp.where(lower, below - step, above + step)


def product_kernel(tiles, below, above, ids_t, counts, kinds, u_hi, u_lo, ut_hi, ut_lo, w2_hi, w2_lo, w2t_hi, w2t_lo, cols, out, sent, xv, edge, phis, acc, pairs, grads, force, lows):
    n_slots = ids_t.shape[0]
    levels = 16
    gap = levels - 1
    blocks = n_slots // 8
    xv[0:3] = tiles[...]
    xv[3] = shifted_ghosts(pltpu.roll(below[0:8, :], 64, 1), pltpu.roll(above[0:8, :], 64, 1), 2, 8)
    count_row = jnp.broadcast_to(counts[...], (8, 128))

    def geometry(nb, carry):
        rows = pl.ds(pl.multiple_of(nb * 8, 8), 8)
        index = ids_t[rows, :]
        low = index & 127
        high = index >> 7
        lows[rows, :] = (index & 63).astype(F32)
        near = []
        for f in range(6):
            picks = [lane_pick(jnp.broadcast_to(xv[q, f : f + 1, :], (8, 128)), low) for q in range(4)]
            value = jnp.where(high < 2, jnp.where(high == 0, picks[0], picks[1]), jnp.where(high == 2, picks[2], picks[3]))
            near.append(value - jnp.broadcast_to(xv[0, f : f + 1, :], (8, 128)))
        d, dd = near[:3], near[3:]
        square = d[0] * d[0] + d[1] * d[1] + d[2] * d[2]
        rate = 2.0 * (d[0] * dd[0] + d[1] * dd[1] + d[2] * dd[2])
        wide = square + 0.01
        inverse = lax.rsqrt(wide)
        half = 0.5 / wide
        live = (rows_of((8, 128)) + nb * 8) < count_row
        s = jnp.where(live, jnp.exp(-square) * inverse, 0.0)
        tau = s * inverse
        sq = -s * (1.0 + half)
        tq = -tau * (1.0 + 2.0 * half)
        share = 1.0 / (1.0 + s)
        us = gap * share * share
        for c in range(3):
            edge[c, rows, :] = d[c]
            edge[3 + c, rows, :] = dd[c]
            edge[9 + c, rows, :] = tau * d[c]
            edge[13 + c, rows, :] = tq * rate * d[c] + tau * dd[c]
        edge[6, rows, :] = gap * s * share
        edge[7, rows, :] = us * sq * rate
        edge[8, rows, :] = s
        edge[12, rows, :] = sq * rate
        edge[16, rows, :] = tau
        edge[17, rows, :] = half
        edge[18, rows, :] = rate
        return carry

    lax.fori_loop(0, blocks, geometry, 0, unroll=8)

    def pooling(kk, carry):
        sums = [[jnp.zeros((8, 128), F32) for _ in range(8)] for _ in range(2)]
        for nb in range(blocks):
            rows = pl.ds(nb * 8, 8)
            u = edge[6, rows, :]
            w = -2.0 * edge[7, rows, :]
            radial = [edge[8 + a, rows, :] for a in range(4)]
            moved = [edge[12 + a, rows, :] for a in range(4)]
            for side in range(2):
                z = u - (2 * kk + side).astype(F32)
                phi = jnp.exp2(z * (z * (-LOG2E)))
                phis[2 * kk + side, rows, :] = phi
                dphi = phi * (z * w)
                for a in range(4):
                    sums[side][a] = sums[side][a] + phi * radial[a]
                    sums[side][4 + a] = sums[side][4 + a] + (dphi * radial[a] + phi * moved[a])
        for side in range(2):
            for a in range(8):
                acc[pl.ds(pl.multiple_of((a * levels + 2 * kk + side) * 8, 8), 8), :] = sums[side][a]
        return carry

    lax.fori_loop(0, levels // 2, pooling, 0)
    pooled = acc[pl.ds(0, 128, stride=8), :]
    for s in range(1, 8):
        pooled = pooled + acc[pl.ds(s, 128, stride=8), :]
    pooled = pooled * (1.0 / n_slots)
    grads[...] = pooled
    kind = jnp.concatenate([kinds[...], kinds[...]], axis=1)
    p = [pooled[a * 16 : (a + 1) * 16] for a in range(4)]
    dp = [pooled[64 + a * 16 : 64 + (a + 1) * 16] for a in range(4)]
    for k in range(levels):
        value = jnp.zeros((16, 128), F32)
        moved = jnp.zeros((16, 128), F32)
        for a in range(4):
            value = value + p[a] * jnp.broadcast_to(grads[a * 16 + k : a * 16 + k + 1, :], (16, 128))
            moved = moved + p[a] * jnp.broadcast_to(grads[64 + a * 16 + k : 64 + a * 16 + k + 1, :], (16, 128))
        pairs[k * 16 : (k + 1) * 16, 0:128] = value
        pairs[k * 16 : (k + 1) * 16, 128:256] = 2.0 * moved
    both = split(pairs[...])
    z1 = jnp.where(
        kind == 1,
        dot3((ut_hi[:, 256:512], ut_lo[:, 256:512]), both),
        dot3((ut_hi[:, 0:256], ut_lo[:, 0:256]), both),
    )
    h1 = jnp.tanh(z1[:, 0:128] + cols[:, 0:1])
    slope1 = 1.0 - h1 * h1
    dh1 = slope1 * z1[:, 128:256]
    z2 = dot3((w2t_hi[...], w2t_lo[...]), jnp.concatenate([h1, dh1], axis=1))
    t2 = jnp.tanh(z2[:, 0:128] + cols[:, 1:2])
    slope2 = 1.0 - t2 * t2
    read = cols[:, 2:3]
    delta2 = slope2 * read
    ddelta2 = -2.0 * t2 * (slope2 * z2[:, 128:256]) * read
    back = dot3((w2_hi[...], w2_lo[...]), jnp.concatenate([delta2, ddelta2], axis=1))
    e1 = back[:, 0:128] + read
    delta1 = slope1 * e1
    ddelta1 = slope1 * back[:, 128:256] - 2.0 * h1 * dh1 * e1
    both = split(jnp.concatenate([delta1, ddelta1], axis=1))
    pairs[...] = jnp.where(
        kind == 1,
        dot3((u_hi[256:512, :], u_lo[256:512, :]), both),
        dot3((u_hi[0:256, :], u_lo[0:256, :]), both),
    )
    g = [jnp.zeros((16, 128), F32) for _ in range(4)]
    dg = [jnp.zeros((16, 128), F32) for _ in range(4)]
    for k in range(levels):
        m = pairs[k * 16 : (k + 1) * 16, 0:128]
        dm = pairs[k * 16 : (k + 1) * 16, 128:256]
        for a in range(4):
            row = jnp.broadcast_to(grads[a * 16 + k : a * 16 + k + 1, :], (16, 128))
            drow = jnp.broadcast_to(grads[64 + a * 16 + k : 64 + a * 16 + k + 1, :], (16, 128))
            g[a] = g[a] + m * row
            dg[a] = dg[a] + (dm * row + m * drow)
    scale = 2.0 / n_slots
    for a in range(4):
        grads[a * 16 : (a + 1) * 16, :] = g[a] * scale
        grads[64 + a * 16 : 64 + (a + 1) * 16, :] = dg[a] * scale

    def backward(nb, centre):
        rows = pl.ds(pl.multiple_of(nb * 8, 8), 8)
        u = edge[6, rows, :]
        zero = jnp.zeros((8, 128), F32)
        s0, s1, s2, r0, r1 = ([zero] * 4 for _ in range(5))
        for k in range(levels):
            z = u - float(k)
            phi = phis[k, rows, :]
            phi1 = z * phi
            phi2 = z * phi1
            for a in range(4):
                row = jnp.broadcast_to(grads[a * 16 + k : a * 16 + k + 1, :], (8, 128))
                drow = jnp.broadcast_to(grads[64 + a * 16 + k : 64 + a * 16 + k + 1, :], (8, 128))
                s0[a] = s0[a] + row * phi
                s1[a] = s1[a] + row * phi1
                s2[a] = s2[a] + row * phi2
                r0[a] = r0[a] + drow * phi
                r1[a] = r1[a] + drow * phi1
        d = [edge[c, rows, :] for c in range(3)]
        dd = [edge[3 + c, rows, :] for c in range(3)]
        du = edge[7, rows, :]
        radial = [edge[8 + a, rows, :] for a in range(4)]
        moved = [edge[12 + a, rows, :] for a in range(4)]
        s = radial[0]
        tau = edge[16, rows, :]
        half = edge[17, rows, :]
        rate = edge[18, rows, :]
        one = 1.0 + half
        two = one + half
        sq = -s * one
        sqq = s * (one * one + 2.0 * half * half)
        tq = -tau * two
        tqq = tau * (two * two + 4.0 * half * half)
        share = 1.0 / (1.0 + s)
        us = gap * share * share
        uq = us * sq
        uqq = us * (sqq - 2.0 * share * sq * sq)
        a1 = [-2.0 * v for v in s1]
        da = [r0[a] + a1[a] * du for a in range(4)]
        da1 = [-2.0 * r1[a] + (4.0 * s2[a] - 2.0 * s0[a]) * du for a in range(4)]
        a1r = a1[0] * radial[0] + a1[1] * radial[1] + (a1[2] * radial[2] + a1[3] * radial[3])
        ad = s0[1] * d[0] + s0[2] * d[1] + s0[3] * d[2]
        turned = da1[0] * radial[0] + a1[0] * moved[0]
        for a in range(1, 4):
            turned = turned + (da1[a] * radial[a] + a1[a] * moved[a])
        dad = da[1] * d[0] + s0[1] * dd[0]
        for c in range(1, 3):
            dad = dad + (da[c + 1] * d[c] + s0[c + 1] * dd[c])
        eq = uq * a1r + sq * s0[0] + tq * ad
        deq = rate * (uqq * a1r + sqq * s0[0] + tqq * ad) + uq * turned + sq * da[0] + tq * dad
        dtau = tq * rate
        result = []
        for c in range(3):
            value = 2.0 * (dd[c] * eq + d[c] * deq) + (dtau * s0[c + 1] + tau * da[c + 1])
            hi = value.astype(BF16).astype(F32)
            force[c, rows, :] = hi
            force[3 + c, rows, :] = value - hi
            result.append(centre[c] + value)
        return tuple(result)

    zero = jnp.zeros((8, 128), F32)
    centre = lax.fori_loop(0, blocks, backward, (zero, zero, zero), unroll=2)
    row8 = rows_of((8, 128))
    rows16 = [(rows_of((16, 128)) + 16 * rg).astype(F32).astype(BF16) for rg in range(4)]
    on = jnp.ones((16, 128), BF16)
    off = jnp.zeros((16, 128), BF16)
    chunk = 32

    def scatter(step, total):
        lefts, hots = [], []
        for i in range(chunk):
            n = step * chunk + i
            hit = (jnp.broadcast_to(ids_t[pl.ds(n, 1), :], (8, 128)) >> 6) == row8
            stack = [jnp.where(hit, jnp.broadcast_to(force[c, pl.ds(n, 1), :], (8, 128)), 0.0) for c in range(6)]
            lefts.append(jnp.concatenate(stack, axis=0).astype(BF16))
            low = jnp.broadcast_to(lows[pl.ds(n, 1), :], (16, 128)).astype(BF16)
            hots.append(jnp.concatenate([jnp.where(low == r, on, off) for r in rows16], axis=0))
        return total + lax.dot_general(jnp.concatenate(lefts, axis=1), jnp.concatenate(hots, axis=1), NT, preferred_element_type=F32)

    total = lax.fori_loop(0, n_slots // chunk, scatter, jnp.zeros((48, 64), F32), unroll=2)
    out[...] = jnp.zeros_like(out)
    rows = {}
    for c in range(3):
        both = total[c * 8 : c * 8 + 8] + total[24 + c * 8 : 32 + c * 8]
        for q in range(4):
            rows[q, c] = jnp.concatenate([both[2 * q : 2 * q + 1], both[2 * q + 1 : 2 * q + 2]], axis=1)
        out[c : c + 1, :] = rows[0, c] - jnp.sum(centre[c], axis=0, keepdims=True)
    tile = [rows[q, c] for q in range(1, 4) for c in range(3)] + [jnp.zeros((7, 128), F32)]
    sent[...] = jnp.broadcast_to(jnp.concatenate(tile, axis=0)[None], sent.shape)


def product(tiles, below, above, lists, weights, bricks):
    n = lists[0].shape[0]
    return pl.pallas_call(
        product_kernel,
        out_shape=[pltpu.VMEM((8, 128), F32), pltpu.VMEM((bricks, 16, 128), F32)],
        in_specs=vmem(15),
        out_specs=vmem(2),
        scratch_shapes=[
            pltpu.VMEM((4, 8, 128), F32),
            pltpu.VMEM((19, n, 128), F32),
            pltpu.VMEM((16, n, 128), F32),
            pltpu.VMEM((1024, 128), F32),
            pltpu.VMEM((256, 256), F32),
            pltpu.VMEM((128, 128), F32),
            pltpu.VMEM((6, n, 128), F32),
            pltpu.VMEM((n, 128), F32),
        ],
        name="product",
    )(*here(tiles, below, above, *lists, *weights))


def pack_kernel(places_at, basis_at, map_x_at, map_y_at, map_z_at, out, places, tangent, map_x, map_y, map_z, semaphores):
    last = basis_at.shape[0] - 1
    copies = fetch((places_at, basis_at.at[last], map_x_at, map_y_at, map_z_at), (places, tangent, map_x, map_y, map_z), semaphores)
    for copy in copies:
        copy.wait()
    rows = [places[c, 0, 0] for c in range(3)] + [tangent[c, 0, 0] for c in range(3)]
    rows += [halves(m).astype(F32) for m in (map_x, map_y, map_z)] + [jnp.zeros((7, 128), F32)]
    out[...] = jnp.broadcast_to(jnp.concatenate(rows, axis=0)[None], out.shape)


def pack(positions, basis, map_x, map_y, map_z, bricks):
    arrays = (positions, basis, map_x, map_y, map_z)
    return pl.pallas_call(
        pack_kernel,
        out_shape=pltpu.VMEM((bricks, 16, 128), F32),
        in_specs=[pl.BlockSpec(memory_space=pltpu.HBM)] * 5,
        out_specs=vmem(1)[0],
        scratch_shapes=[
            pltpu.VMEM(positions.shape, F32),
            pltpu.VMEM(basis.shape[1:], F32),
            pltpu.VMEM(map_x.shape, jnp.int32),
            pltpu.VMEM(map_y.shape, jnp.int32),
            pltpu.VMEM(map_z.shape, jnp.int32),
            pltpu.SemaphoreType.DMA((5,)),
        ],
        name="pack",
    )(*(pltpu.with_memory_space_constraint(a, pltpu.HBM) for a in arrays))


def brick_reader(grid):
    nx, ny = grid
    px, py = lax.axis_index("gx"), lax.axis_index("gy")

    def at(ref, dx, dy):
        x = lax.rem(px + (dx + nx), nx)
        y = lax.rem(py + (dy + ny), ny)
        return ref[x * ny + y]

    return at


def as_index(row):
    return jnp.broadcast_to(row, (8, 128)).astype(jnp.int32)


def turn(x):
    return pltpu.roll(x, 64, 1)


def assemble_kernel(grid, got, map_z, stored, tiles, message):
    at = brick_reader(grid)
    lower = rows_of((8, 128), 1) < 64
    row = rows_of((8, 128))
    step_x = jnp.where(row == 0, 1.0, 0.0)
    step_y = jnp.where(row == 1, 1.0, 0.0)
    middle, ghosts, index = {}, {}, {}
    for dy in (-1, 0, 1):
        own, low, high = (at(got, dx, dy)[0:8] for dx in (0, -1, 1))
        from_low = lane_pick(low, turn(as_index(low[6:7])))
        from_high = lane_pick(high, turn(as_index(high[6:7])))
        middle[dy] = own
        ghosts[dy] = jnp.where(lower, from_low - step_x, from_high + step_x)
        index[dy] = turn(as_index(own[7:8]))

    def second(dy):
        low = index[dy] & 127
        return jnp.where(index[dy] < 128, lane_pick(middle[dy], low), lane_pick(ghosts[dy], low))

    third = jnp.where(lower, second(-1) - step_y, second(1) + step_y)
    tiles[0] = middle[0]
    tiles[1] = ghosts[0]
    tiles[2] = third
    chosen = jnp.broadcast_to(map_z[...], (8, 128))
    low = chosen & 127
    message[0:8, :] = jnp.where(
        chosen < 128, lane_pick(middle[0], low), jnp.where(chosen < 256, lane_pick(ghosts[0], low), lane_pick(third, low))
    )
    maps = [at(got, dx, dy)[8:9] for dx in (-1, 0, 1) for dy in (-1, 0, 1)]
    maps += [at(got, dx, 0)[7:8] for dx in (-1, 0, 1)] + [at(got, 0, 0)[6:7], jnp.zeros((3, 128), F32)]
    message[8:24, :] = jnp.concatenate(maps, axis=0)
    for c in range(3):
        message[24 + 32 * c : 56 + 32 * c, :] = stored[c]


def assemble(got, map_z, stored, grid):
    return pl.pallas_call(
        functools.partial(assemble_kernel, grid),
        out_shape=[pltpu.VMEM((3, 8, 128), F32), pltpu.VMEM((120, 128), F32)],
        in_specs=vmem(3),
        out_specs=vmem(2),
        name="assemble",
    )(*here(got, map_z, stored))


def meet(low, high):
    return jnp.where(rows_of((8, 128), 1) < 64, low, high)


def fold_layers(spread, own, part, maps_at, above, below):
    lower = rows_of((8, 128), 1) < 64

    def pair(low, low_index, high, high_index, base):
        return jnp.concatenate([spread(low, low_index, base + 64, 64), spread(high, high_index, base, 64)], axis=1)

    def folded(home, x_ghosts, y_ghosts, map_x, map_y):
        sides = x_ghosts + pair(y_ghosts[-1], map_y(-1), y_ghosts[1], map_y(1), 128)
        return home + spread(y_ghosts[0], map_y(0), 0, 128) + spread(sides, map_x, 0, 128)

    y_ghosts = {dx: meet(part(dx, -1, 1), part(dx, 1, 1)) for dx in (-1, 0, 1)}
    x_ghosts = meet(part(-1, 0, 0), part(1, 0, 0))
    layers = [folded(own, x_ghosts, y_ghosts, maps_at(0)[6:7], lambda dx: maps_at(dx)[7:8])]
    for message, kept in ((above, lower), (below, jnp.logical_not(lower))):

        def sent(dx, dy, message=message, kept=kept):
            index = message[9 + 3 * (dx + 1) + dy : 10 + 3 * (dx + 1) + dy, :]
            return jnp.where(kept, part(dx, dy, 2), 0.0), index

        y_ghosts = {dx: pair(*sent(dx, -1), *sent(dx, 1), 256) for dx in (-1, 0, 1)}
        x_ghosts = pair(*sent(-1, 0), *sent(1, 0), 128)
        home = spread(*sent(0, 0), 0, 128)
        layers.append(folded(home, x_ghosts, y_ghosts, message[20:21, :], lambda dx, message=message: message[18 + dx : 19 + dx, :]))
    return layers


def fold_kernel(grid, own, got, maps, below, above, stored, gram, out):
    at = brick_reader(grid)
    blank = jnp.zeros((5, 128), F32)
    target = rows_of((128, 128))

    def spread(values, index, first, count):
        hi, lo = split(values)
        left = jnp.concatenate([hi.astype(F32), lo.astype(F32)], axis=0).astype(BF16)
        hot = jnp.where(jnp.broadcast_to(index.astype(jnp.int32) - first, (count, 128)) == target[0:count], 1.0, 0.0).astype(BF16)
        both = lax.dot_general(left, hot, NT, preferred_element_type=F32)
        return both[0:8] + both[8:16]

    def part(dx, dy, q):
        return turn(jnp.concatenate([at(got, dx, dy)[3 * q : 3 * q + 3], blank], axis=0))

    layers = fold_layers(spread, own[...], part, lambda dx: at(maps, dx, 0), above, below)
    column = jnp.zeros((32, 128), F32)
    for c in range(3):
        at_rows = pl.ds(24 + 32 * c, 32)
        bases = (stored[c], above[at_rows, :], below[at_rows, :])
        for layer, vectors in zip(layers, bases):
            column = column + vectors * layer[c : c + 1]
    column = jnp.sum(column, axis=1, keepdims=True)
    lane = rows_of((32, 128), 1)
    full = jnp.where(lane == 30, column, gram[...])
    tail = jnp.where((lane >= 16) & (lane < 32), full, 0.0)
    first = full[0:4]
    for b in range(1, 4):
        first = first + pltpu.roll(full[4 * b : 4 * b + 4], 32 * b, 1)
    second = pltpu.roll(tail[16:18], 112, 1)
    for b in range(1, 8):
        second = second + pltpu.roll(tail[16 + 2 * b : 18 + 2 * b], 16 * (b - 1), 1)
    tile = [first, second] + [layer[0:3] for layer in layers] + [jnp.zeros((1, 128), F32)]
    out[...] = jnp.broadcast_to(jnp.concatenate(tile, axis=0)[None], out.shape)


def fold(own, got, maps, below, above, stored, gram, grid, copies):
    return pl.pallas_call(
        functools.partial(fold_kernel, grid),
        out_shape=pltpu.VMEM((copies, 16, 128), F32),
        in_specs=vmem(7),
        out_specs=vmem(1)[0],
        name="fold",
    )(*here(own, got, maps, below, above, stored, gram))


def column_kernel(got, product, out):
    count = got.shape[0]
    here_z = lax.axis_index("gz")

    def vector(z, before, after):
        return got[z, 6:9, :] + got[before, 9:12, :] + got[after, 12:15, :]

    product[...] = jnp.zeros_like(product)
    product[0:3, :] = vector(here_z, lax.rem(here_z + (count - 1), count), lax.rem(here_z + 1, count))
    squares = jnp.zeros((3, 128), F32)
    for z in range(count):
        value = vector(z, (z - 1) % count, (z + 1) % count)
        squares = squares + value * value
    size = jnp.sum(jnp.sum(squares, axis=1, keepdims=True), axis=0, keepdims=True)
    tile = got[0, 0:8, :]
    for z in range(1, count):
        tile = tile + got[z, 0:8, :]
    spot = (rows_of((8, 128)) == 4) & (rows_of((8, 128), 1) == 126)
    tile = jnp.where(spot, size, tile)
    out[...] = jnp.broadcast_to(tile[None], out.shape)


def column_of(got, bricks):
    return pl.pallas_call(
        column_kernel,
        out_shape=[pltpu.VMEM((8, 128), F32), pltpu.VMEM((bricks, 8, 128), F32)],
        in_specs=vmem(1),
        out_specs=vmem(2),
        name="column",
    )(*here(got))


def finish_kernel(entries, got, product, stored, result, correlations, norm):
    count = correlations.shape[1]
    packed = jnp.sum(got[...], axis=0) * (1.0 / entries)
    parts = [packed[0:4]] + [pltpu.roll(packed[0:4], 128 - 32 * b, 1) for b in range(1, 4)]
    parts += [pltpu.roll(packed[4:6], (144 - 16 * b) % 128, 1) for b in range(8)]
    full = jnp.concatenate(parts, axis=0)
    column = full[:, count : count + 1]
    line = jnp.sum(jnp.where(rows_of((32, 128)) == rows_of((32, 128), 1), column, 0.0), axis=0, keepdims=True)
    row = rows_of((32, 1))
    lane = rows_of((1, 128), 1)
    down = jnp.where(row < count, column, jnp.where(row == count, -1.0, 0.0))
    across = jnp.where(lane < count, line, jnp.where(lane == count, -2.0, 0.0))
    size = jnp.where(row < count, full * across * down, jnp.where((row == count) & (lane == count), full, 0.0))
    wide = rows_of((32, 128), 1)
    twice = jnp.where((row < 16) & (wide >= 16) & (wide < count), 2.0, 1.0)
    size = jnp.where((wide <= count) & ((row < 16) | (wide >= 16)), size * twice, 0.0)
    size = jnp.sum(jnp.sum(size, axis=1, keepdims=True), axis=0, keepdims=True)
    length = jnp.sqrt(jnp.maximum(size, 0.0) + 1e-06)
    norm[...] = length
    correlations[...] = line[:, 0:count]
    share = jnp.where(row < count, column, 0.0)
    for c in range(3):
        taken = jnp.sum(stored[c] * share, axis=0, keepdims=True)
        result[c, 0, 0] = (product[c : c + 1, :] - taken) / length


def finish(got, product, stored, shape, count, entries):
    return pl.pallas_call(
        functools.partial(finish_kernel, entries),
        out_shape=[
            jax.ShapeDtypeStruct(shape, F32),
            jax.ShapeDtypeStruct((1, count), F32),
            jax.ShapeDtypeStruct((1, 1), F32),
        ],
        in_specs=vmem(3),
        out_specs=vmem(3),
        name="finish",
    )(*here(got, product, stored))


def on_device(positions, basis, neighbours, used_count, kinds, map_x, map_y, map_z, table, fit_w1, fit_b1, fit_w2, fit_b2, fit_out):
    nx, ny, nz = (lax.axis_size(a) for a in ("gx", "gy", "gz"))
    plane = ("gx", "gy")
    up = [(i, (i + 1) % nz) for i in range(nz)]
    down = [(j, i) for i, j in up]

    def exchange(x):
        return lax.all_to_all(x, plane, 0, 0)

    packed = pack(positions, basis, map_x, map_y, map_z, nx * ny)
    raw = exchange(packed)
    table, _ = lax.optimization_barrier((table, packed))
    mixed, map_row, stored = mixing(table, fit_w1, map_z, basis)
    layers, lists, gram = lists_of(fit_w2, fit_b1, fit_b2, fit_out, neighbours, used_count, kinds, stored)
    raw, map_row = lax.optimization_barrier((raw, map_row))
    tiles, message = assemble(raw, map_row, stored, (nx, ny))
    below, above = lax.ppermute(message, "gz", up), lax.ppermute(message, "gz", down)
    own, shared = product(tiles, below, above, lists, (*mixed, *layers), nx * ny)
    summary = fold(own, exchange(shared), raw, below, above, stored, gram, (nx, ny), nz)
    hessian_vec, summary = column_of(lax.all_to_all(summary, "gz", 0, 0), nx * ny)
    summary = exchange(summary)
    entries = 3 * positions.shape[-1] * nx * ny * nz
    next_vector, correlations, vector_norm = finish(summary, hessian_vec, stored, positions.shape, basis.shape[0], entries)
    return next_vector, correlations.reshape(-1), vector_norm.reshape(())


def solution(mesh):
    bricks = P("gx", "gy", "gz", None)
    lists = P("gx", "gy", "gz", None, None)
    vector = P(None, "gx", "gy", "gz", None)
    return jax.shard_map(
        on_device,
        mesh=mesh,
        in_specs=(vector, P(None, None, "gx", "gy", "gz", None), lists, bricks, bricks, lists, lists, lists) + (P(),) * 6,
        out_specs=(vector, P(), P()),
        check_vma=False,
    )
```

```python
import functools

import jax
import jax.numpy as jnp
from jax import lax
from jax.experimental import pallas as pl
from jax.experimental.pallas import tpu as pltpu
from jax.sharding import PartitionSpec as P

F32 = jnp.float32
BF16 = jnp.bfloat16
LOG2E = 1.4426950408889634
NT = (((1,), (1,)), ((), ()))


def split(x):
    hi = x.astype(BF16)
    return hi, (x - hi.astype(F32)).astype(BF16)


def mm(a, b):
    return jnp.dot(a, b, preferred_element_type=F32)


def dot3(a, b):
    ah, al = a if isinstance(a, tuple) else split(a)
    bh, bl = b if isinstance(b, tuple) else split(b)
    return mm(ah, bh) + (mm(ah, bl) + mm(al, bh))


def lane_pick(table, index):
    return jnp.take_along_axis(table, index, axis=1, mode="promise_in_bounds")


def rows_of(shape, dim=0):
    return lax.broadcasted_iota(jnp.int32, shape, dim)


def halves(ref):
    return jnp.concatenate([ref[0, 0, 0, 0:1, :], ref[0, 0, 0, 1:2, :]], axis=1)


def fetch(sources, places, semaphores):
    copies = [pltpu.make_async_copy(x, y, semaphores.at[i]) for i, (x, y) in enumerate(zip(sources, places))]
    for copy in copies:
        copy.start()
    return copies


EXACT = dict(precision=lax.Precision.HIGHEST, preferred_element_type=F32)


def mixing_kernel(table_at, w1_at, map_at, basis_at, u_hi, u_lo, ut_hi, ut_lo, map_row, stored, table, w1t, map_z, basis, outer, inner, k_hi, k_lo, semaphores):
    copies = fetch((table_at, map_at, w1_at, basis_at), (table, map_z, w1t, basis), semaphores)
    stored[...] = jnp.zeros_like(stored)
    types, levels, width = table.shape
    hidden = w1t.shape[0]
    m2 = w1t.shape[1] // width
    count = types * levels * levels
    copies[0].wait()
    tall = table[...].reshape(types * levels, width)
    tall = jnp.concatenate([tall, jnp.zeros((types * levels, 128 - width), F32)], axis=1)
    tall = jnp.concatenate([tall, jnp.zeros((128 - types * levels, 128), F32)], axis=0).T
    column = rows_of((128, count), 1)
    row = rows_of((128, count))
    kind = column // (levels * levels)
    first = jnp.where(row == kind * levels + (column // levels) % levels, 1.0, 0.0)
    second = jnp.where(row == kind * levels + column % levels, 1.0, 0.0)
    outer[...] = jnp.dot(tall, first, **EXACT) * 0.5
    inner[...] = jnp.dot(tall, second, **EXACT) * 0.5
    near = inner[0:m2, :] * 2.0
    far = outer[0:m2, :] * 2.0

    def kron(m, carry):
        value = jnp.broadcast_to(outer[pl.ds(m, 1), :], (m2, count)) * near + jnp.broadcast_to(inner[pl.ds(m, 1), :], (m2, count)) * far
        hi, lo = split(value)
        at = pl.ds(pl.multiple_of(m * m2, m2), m2)
        k_hi[at, :] = hi
        k_lo[at, :] = lo
        return carry

    lax.fori_loop(0, width, kron, 0, unroll=4)
    copies[1].wait()
    map_row[...] = halves(map_z)
    copies[3].wait()
    for c in range(3):
        for k in range(basis.shape[0]):
            stored[c, k : k + 1, :] = basis[k, c, 0, 0]
    copies[2].wait()
    full = dot3(w1t[...], (k_hi[...], k_lo[...]))
    full = jnp.concatenate([full, jnp.zeros((256 - hidden, count), F32)], axis=0)
    hi, lo = split(full)
    ut_hi[...] = hi
    ut_lo[...] = lo
    hi, lo = split(full.T)
    u_hi[...] = hi
    u_lo[...] = lo


def lists_kernel(w2_at, b1_at, b2_at, wo_at, ids_at, counts_at, kinds_at, stored, w2_hi, w2_lo, w2t_hi, w2t_lo, cols, ids_t, count_row, kind_row, gram, w2, b1, b2, wo, ids, counts, kinds, pad, semaphores):
    places = (w2, b1, b2, wo, ids, counts, kinds)
    copies = fetch((w2_at, b1_at, b2_at, wo_at, ids_at, counts_at, kinds_at), places, semaphores)
    hidden = w2.shape[0]
    pad[...] = jnp.zeros_like(pad)
    gram[...] = jnp.zeros_like(gram)
    for copy in copies:
        copy.wait()
    pad[0:hidden, 0:hidden] = w2[...]
    hi, lo = split(pad[...])
    w2_hi[...] = hi
    w2_lo[...] = lo
    hi, lo = split(pad[...].T)
    w2t_hi[...] = hi
    w2t_lo[...] = lo
    pad[0:128, :] = jnp.zeros((128, pad.shape[1]), F32)
    pad[0:1, 0:hidden] = b1[...]
    pad[1:2, 0:hidden] = b2[...]
    pad[2:3, 0:hidden] = wo[...]
    cols[...] = pad[0:128, :].T
    ids_t[...] = ids[0, 0, 0].astype(F32).T.astype(jnp.int32)
    count_row[...] = counts[0, 0]
    kind_row[...] = kinds[0, 0]
    total = jnp.zeros((32, 32), F32)
    for c in range(3):
        total = total + lax.dot_general(stored[c], stored[c], NT, **EXACT)
    gram[:, 0:32] = total


def vmem(n):
    return [pl.BlockSpec(memory_space=pltpu.VMEM)] * n


def here(*arrays):
    return [pltpu.with_memory_space_constraint(a, pltpu.VMEM) for a in arrays]


def from_hbm(kernel, name, shapes, scratch, *arrays, held=()):
    return pl.pallas_call(
        kernel,
        out_shape=[pltpu.VMEM(s, d) for s, d in shapes],
        in_specs=[pl.BlockSpec(memory_space=pltpu.HBM)] * len(arrays) + vmem(len(held)),
        out_specs=vmem(len(shapes)),
        scratch_shapes=[pltpu.VMEM(a.shape, a.dtype) for a in arrays] + scratch + [pltpu.SemaphoreType.DMA((len(arrays),))],
        name=name,
    )(*(pltpu.with_memory_space_constraint(a, pltpu.HBM) for a in arrays), *here(*held))


def mixing(table, w1, map_z, basis):
    hp = 256
    count = table.shape[0] * table.shape[1] ** 2
    shapes = [((count, hp), BF16)] * 2 + [((hp, count), BF16)] * 2 + [((1, 128), jnp.int32), ((3, 32, 128), F32)]
    scratch = [pltpu.VMEM((128, count), F32)] * 2 + [pltpu.VMEM((w1.shape[0], count), BF16)] * 2
    *weights, map_row, stored = from_hbm(mixing_kernel, "mixing", shapes, scratch, table, w1.T, map_z, basis)
    return weights, map_row, stored


def lists_of(w2, b1, b2, wo, ids, counts, kinds, stored):
    hp = 256
    row = ((1, 128), jnp.int32)
    shapes = [((hp, hp), BF16)] * 4 + [((hp, 128), F32), ((ids.shape[-1], 128), jnp.int32), row, row, ((32, 128), F32)]
    scratch = [pltpu.VMEM((hp, hp), F32)]
    done = from_hbm(lists_kernel, "lists", shapes, scratch, w2, b1[None], b2[None], wo[None], ids, counts, kinds, held=(stored,))
    return done[:5], done[5:8], done[8]


def shifted_ghosts(below, above, coord, rows):
    lower = rows_of((rows, 128), 1) < 64
    step = jnp.where(rows_of((rows, 128)) == coord, 1.0, 0.0)
    return jnp.where(lower, below - step, above + step)


def product_kernel(tiles, below, above, ids_t, counts, kinds, u_hi, u_lo, ut_hi, ut_lo, w2_hi, w2_lo, w2t_hi, w2t_lo, cols, out, sent, xv, edge, phis, acc, pairs, grads, force, lows):
    n_slots = ids_t.shape[0]
    levels = 16
    gap = levels - 1
    blocks = n_slots // 8
    xv[0:3] = tiles[...]
    xv[3] = shifted_ghosts(pltpu.roll(below[0:8, :], 64, 1), pltpu.roll(above[0:8, :], 64, 1), 2, 8)
    count_row = jnp.broadcast_to(counts[...], (8, 128))

    def geometry(nb, carry):
        rows = pl.ds(pl.multiple_of(nb * 8, 8), 8)
        index = ids_t[rows, :]
        low = index & 127
        high = index >> 7
        lows[rows, :] = (index & 63).astype(F32)
        near = []
        for f in range(6):
            picks = [lane_pick(jnp.broadcast_to(xv[q, f : f + 1, :], (8, 128)), low) for q in range(4)]
            value = jnp.where(high < 2, jnp.where(high == 0, picks[0], picks[1]), jnp.where(high == 2, picks[2], picks[3]))
            near.append(value - jnp.broadcast_to(xv[0, f : f + 1, :], (8, 128)))
        d, dd = near[:3], near[3:]
        square = d[0] * d[0] + d[1] * d[1] + d[2] * d[2]
        rate = 2.0 * (d[0] * dd[0] + d[1] * dd[1] + d[2] * dd[2])
        wide = square + 0.01
        inverse = lax.rsqrt(wide)
        half = 0.5 / wide
        live = (rows_of((8, 128)) + nb * 8) < count_row
        s = jnp.where(live, jnp.exp(-square) * inverse, 0.0)
        tau = s * inverse
        sq = -s * (1.0 + half)
        tq = -tau * (1.0 + 2.0 * half)
        share = 1.0 / (1.0 + s)
        us = gap * share * share
        for c in range(3):
            edge[c, rows, :] = d[c]
            edge[3 + c, rows, :] = dd[c]
            edge[9 + c, rows, :] = tau * d[c]
            edge[13 + c, rows, :] = tq * rate * d[c] + tau * dd[c]
        edge[6, rows, :] = gap * s * share
        edge[7, rows, :] = us * sq * rate
        edge[8, rows, :] = s
        edge[12, rows, :] = sq * rate
        edge[16, rows, :] = tau
        edge[17, rows, :] = half
        edge[18, rows, :] = rate
        return carry

    lax.fori_loop(0, blocks, geometry, 0, unroll=8)

    def pooling(kk, carry):
        sums = [[jnp.zeros((8, 128), F32) for _ in range(8)] for _ in range(2)]
        for nb in range(blocks):
            rows = pl.ds(nb * 8, 8)
            u = edge[6, rows, :]
            w = -2.0 * edge[7, rows, :]
            radial = [edge[8 + a, rows, :] for a in range(4)]
            moved = [edge[12 + a, rows, :] for a in range(4)]
            for side in range(2):
                z = u - (2 * kk + side).astype(F32)
                phi = jnp.exp2(z * (z * (-LOG2E)))
                phis[2 * kk + side, rows, :] = phi
                dphi = phi * (z * w)
                for a in range(4):
                    sums[side][a] = sums[side][a] + phi * radial[a]
                    sums[side][4 + a] = sums[side][4 + a] + (dphi * radial[a] + phi * moved[a])
        for side in range(2):
            for a in range(8):
                acc[pl.ds(pl.multiple_of((a * levels + 2 * kk + side) * 8, 8), 8), :] = sums[side][a]
        return carry

    lax.fori_loop(0, levels // 2, pooling, 0)
    pooled = acc[pl.ds(0, 128, stride=8), :]
    for s in range(1, 8):
        pooled = pooled + acc[pl.ds(s, 128, stride=8), :]
    pooled = pooled * (1.0 / n_slots)
    grads[...] = pooled
    kind = jnp.concatenate([kinds[...], kinds[...]], axis=1)
    p = [pooled[a * 16 : (a + 1) * 16] for a in range(4)]
    dp = [pooled[64 + a * 16 : 64 + (a + 1) * 16] for a in range(4)]
    for k in range(levels):
        value = jnp.zeros((16, 128), F32)
        moved = jnp.zeros((16, 128), F32)
        for a in range(4):
            value = value + p[a] * jnp.broadcast_to(grads[a * 16 + k : a * 16 + k + 1, :], (16, 128))
            moved = moved + p[a] * jnp.broadcast_to(grads[64 + a * 16 + k : 64 + a * 16 + k + 1, :], (16, 128))
        pairs[k * 16 : (k + 1) * 16, 0:128] = value
        pairs[k * 16 : (k + 1) * 16, 128:256] = 2.0 * moved
    both = split(pairs[...])
    z1 = jnp.where(
        kind == 1,
        dot3((ut_hi[:, 256:512], ut_lo[:, 256:512]), both),
        dot3((ut_hi[:, 0:256], ut_lo[:, 0:256]), both),
    )
    h1 = jnp.tanh(z1[:, 0:128] + cols[:, 0:1])
    slope1 = 1.0 - h1 * h1
    dh1 = slope1 * z1[:, 128:256]
    z2 = dot3((w2t_hi[...], w2t_lo[...]), jnp.concatenate([h1, dh1], axis=1))
    t2 = jnp.tanh(z2[:, 0:128] + cols[:, 1:2])
    slope2 = 1.0 - t2 * t2
    read = cols[:, 2:3]
    delta2 = slope2 * read
    ddelta2 = -2.0 * t2 * (slope2 * z2[:, 128:256]) * read
    back = dot3((w2_hi[...], w2_lo[...]), jnp.concatenate([delta2, ddelta2], axis=1))
    e1 = back[:, 0:128] + read
    delta1 = slope1 * e1
    ddelta1 = slope1 * back[:, 128:256] - 2.0 * h1 * dh1 * e1
    both = split(jnp.concatenate([delta1, ddelta1], axis=1))
    pairs[...] = jnp.where(
        kind == 1,
        dot3((u_hi[256:512, :], u_lo[256:512, :]), both),
        dot3((u_hi[0:256, :], u_lo[0:256, :]), both),
    )
    g = [jnp.zeros((16, 128), F32) for _ in range(4)]
    dg = [jnp.zeros((16, 128), F32) for _ in range(4)]
    for k in range(levels):
        m = pairs[k * 16 : (k + 1) * 16, 0:128]
        dm = pairs[k * 16 : (k + 1) * 16, 128:256]
        for a in range(4):
            row = jnp.broadcast_to(grads[a * 16 + k : a * 16 + k + 1, :], (16, 128))
            drow = jnp.broadcast_to(grads[64 + a * 16 + k : 64 + a * 16 + k + 1, :], (16, 128))
            g[a] = g[a] + m * row
            dg[a] = dg[a] + (dm * row + m * drow)
    scale = 2.0 / n_slots
    for a in range(4):
        grads[a * 16 : (a + 1) * 16, :] = g[a] * scale
        grads[64 + a * 16 : 64 + (a + 1) * 16, :] = dg[a] * scale

    def backward(nb, centre):
        rows = pl.ds(pl.multiple_of(nb * 8, 8), 8)
        u = edge[6, rows, :]
        zero = jnp.zeros((8, 128), F32)
        s0, s1, s2, r0, r1 = ([zero] * 4 for _ in range(5))
        for k in range(levels):
            z = u - float(k)
            phi = phis[k, rows, :]
            phi1 = z * phi
            phi2 = z * phi1
            for a in range(4):
                row = jnp.broadcast_to(grads[a * 16 + k : a * 16 + k + 1, :], (8, 128))
                drow = jnp.broadcast_to(grads[64 + a * 16 + k : 64 + a * 16 + k + 1, :], (8, 128))
                s0[a] = s0[a] + row * phi
                s1[a] = s1[a] + row * phi1
                s2[a] = s2[a] + row * phi2
                r0[a] = r0[a] + drow * phi
                r1[a] = r1[a] + drow * phi1
        d = [edge[c, rows, :] for c in range(3)]
        dd = [edge[3 + c, rows, :] for c in range(3)]
        du = edge[7, rows, :]
        radial = [edge[8 + a, rows, :] for a in range(4)]
        moved = [edge[12 + a, rows, :] for a in range(4)]
        s = radial[0]
        tau = edge[16, rows, :]
        half = edge[17, rows, :]
        rate = edge[18, rows, :]
        one = 1.0 + half
        two = one + half
        sq = -s * one
        sqq = s * (one * one + 2.0 * half * half)
        tq = -tau * two
        tqq = tau * (two * two + 4.0 * half * half)
        share = 1.0 / (1.0 + s)
        us = gap * share * share
        uq = us * sq
        uqq = us * (sqq - 2.0 * share * sq * sq)
        a1 = [-2.0 * v for v in s1]
        da = [r0[a] + a1[a] * du for a in range(4)]
        da1 = [-2.0 * r1[a] + (4.0 * s2[a] - 2.0 * s0[a]) * du for a in range(4)]
        a1r = a1[0] * radial[0] + a1[1] * radial[1] + (a1[2] * radial[2] + a1[3] * radial[3])
        ad = s0[1] * d[0] + s0[2] * d[1] + s0[3] * d[2]
        turned = da1[0] * radial[0] + a1[0] * moved[0]
        for a in range(1, 4):
            turned = turned + (da1[a] * radial[a] + a1[a] * moved[a])
        dad = da[1] * d[0] + s0[1] * dd[0]
        for c in range(1, 3):
            dad = dad + (da[c + 1] * d[c] + s0[c + 1] * dd[c])
        eq = uq * a1r + sq * s0[0] + tq * ad
        deq = rate * (uqq * a1r + sqq * s0[0] + tqq * ad) + uq * turned + sq * da[0] + tq * dad
        dtau = tq * rate
        result = []
        for c in range(3):
            value = 2.0 * (dd[c] * eq + d[c] * deq) + (dtau * s0[c + 1] + tau * da[c + 1])
            hi = value.astype(BF16).astype(F32)
            force[c, rows, :] = hi
            force[3 + c, rows, :] = value - hi
            result.append(centre[c] + value)
        return tuple(result)

    zero = jnp.zeros((8, 128), F32)
    centre = lax.fori_loop(0, blocks, backward, (zero, zero, zero), unroll=2)
    row8 = rows_of((8, 128))
    rows16 = [(rows_of((16, 128)) + 16 * rg).astype(F32).astype(BF16) for rg in range(4)]
    on = jnp.ones((16, 128), BF16)
    off = jnp.zeros((16, 128), BF16)
    chunk = 32

    def scatter(step, total):
        lefts, hots = [], []
        for i in range(chunk):
            n = step * chunk + i
            hit = (jnp.broadcast_to(ids_t[pl.ds(n, 1), :], (8, 128)) >> 6) == row8
            stack = [jnp.where(hit, jnp.broadcast_to(force[c, pl.ds(n, 1), :], (8, 128)), 0.0) for c in range(6)]
            lefts.append(jnp.concatenate(stack, axis=0).astype(BF16))
            low = jnp.broadcast_to(lows[pl.ds(n, 1), :], (16, 128)).astype(BF16)
            hots.append(jnp.concatenate([jnp.where(low == r, on, off) for r in rows16], axis=0))
        return total + lax.dot_general(jnp.concatenate(lefts, axis=1), jnp.concatenate(hots, axis=1), NT, preferred_element_type=F32)

    total = lax.fori_loop(0, n_slots // chunk, scatter, jnp.zeros((48, 64), F32), unroll=2)
    out[...] = jnp.zeros_like(out)
    rows = {}
    for c in range(3):
        both = total[c * 8 : c * 8 + 8] + total[24 + c * 8 : 32 + c * 8]
        for q in range(4):
            rows[q, c] = jnp.concatenate([both[2 * q : 2 * q + 1], both[2 * q + 1 : 2 * q + 2]], axis=1)
        out[c : c + 1, :] = rows[0, c] - jnp.sum(centre[c], axis=0, keepdims=True)
    half = rows_of((1, 128), 1) < 64
    tile = [rows[q, c] for q in range(1, 4) for c in range(3)]
    tile += [jnp.where(half, above[10:11, :], below[10:11, :]), above[9:10, :], below[9:10, :], jnp.zeros((4, 128), F32)]
    sent[...] = jnp.broadcast_to(jnp.concatenate(tile, axis=0)[None], sent.shape)


def product(tiles, below, above, lists, weights, bricks):
    n = lists[0].shape[0]
    return pl.pallas_call(
        product_kernel,
        out_shape=[pltpu.VMEM((8, 128), F32), pltpu.VMEM((bricks, 16, 128), F32)],
        in_specs=vmem(15),
        out_specs=vmem(2),
        scratch_shapes=[
            pltpu.VMEM((4, 8, 128), F32),
            pltpu.VMEM((19, n, 128), F32),
            pltpu.VMEM((16, n, 128), F32),
            pltpu.VMEM((1024, 128), F32),
            pltpu.VMEM((256, 256), F32),
            pltpu.VMEM((128, 128), F32),
            pltpu.VMEM((6, n, 128), F32),
            pltpu.VMEM((n, 128), F32),
        ],
        name="product",
    )(*here(tiles, below, above, *lists, *weights))


def pack_kernel(places_at, basis_at, map_x_at, map_y_at, out, places, tangent, map_x, map_y, semaphores):
    last = basis_at.shape[0] - 1
    copies = fetch((places_at, basis_at.at[last], map_x_at, map_y_at), (places, tangent, map_x, map_y), semaphores)
    for copy in copies:
        copy.wait()
    rows = [places[c, 0, 0] for c in range(3)] + [tangent[c, 0, 0] for c in range(3)]
    rows += [halves(m).astype(F32) for m in (map_x, map_y)]
    out[...] = jnp.broadcast_to(jnp.concatenate(rows, axis=0)[None], out.shape)


def pack(positions, basis, map_x, map_y, bricks):
    arrays = (positions, basis, map_x, map_y)
    return pl.pallas_call(
        pack_kernel,
        out_shape=pltpu.VMEM((bricks, 8, 128), F32),
        in_specs=[pl.BlockSpec(memory_space=pltpu.HBM)] * 4,
        out_specs=vmem(1)[0],
        scratch_shapes=[
            pltpu.VMEM(positions.shape, F32),
            pltpu.VMEM(basis.shape[1:], F32),
            pltpu.VMEM(map_x.shape, jnp.int32),
            pltpu.VMEM(map_y.shape, jnp.int32),
            pltpu.SemaphoreType.DMA((4,)),
        ],
        name="pack",
    )(*(pltpu.with_memory_space_constraint(a, pltpu.HBM) for a in arrays))


def brick_reader(grid):
    nx, ny = grid
    px, py = lax.axis_index("gx"), lax.axis_index("gy")

    def at(ref, dx, dy):
        x = lax.rem(px + (dx + nx), nx)
        y = lax.rem(py + (dy + ny), ny)
        return ref[x * ny + y]

    return at


def as_index(row):
    return jnp.broadcast_to(row, (8, 128)).astype(jnp.int32)


def turn(x):
    return pltpu.roll(x, 64, 1)


def assemble_kernel(grid, got, map_z, stored, tiles, message):
    at = brick_reader(grid)
    lower = rows_of((8, 128), 1) < 64
    row = rows_of((8, 128))
    step_x = jnp.where(row == 0, 1.0, 0.0)
    step_y = jnp.where(row == 1, 1.0, 0.0)
    middle, ghosts, index = {}, {}, {}
    for dy in (-1, 0, 1):
        own, low, high = (at(got, dx, dy) for dx in (0, -1, 1))
        from_low = lane_pick(low, turn(as_index(low[6:7])))
        from_high = lane_pick(high, turn(as_index(high[6:7])))
        middle[dy] = own
        ghosts[dy] = jnp.where(lower, from_low - step_x, from_high + step_x)
        index[dy] = turn(as_index(own[7:8]))

    def second(dy):
        low = index[dy] & 127
        return jnp.where(index[dy] < 128, lane_pick(middle[dy], low), lane_pick(ghosts[dy], low))

    third = jnp.where(lower, second(-1) - step_y, second(1) + step_y)
    tiles[0] = middle[0]
    tiles[1] = ghosts[0]
    tiles[2] = third
    chosen = jnp.broadcast_to(map_z[...], (8, 128))
    low = chosen & 127
    message[0:8, :] = jnp.where(
        chosen < 128, lane_pick(middle[0], low), jnp.where(chosen < 256, lane_pick(ghosts[0], low), lane_pick(third, low))
    )
    message[8:16, :] = jnp.concatenate([middle[0][6:8], map_z[...].astype(F32), jnp.zeros((5, 128), F32)], axis=0)
    for c in range(3):
        message[16 + 32 * c : 48 + 32 * c, :] = stored[c]


def assemble(got, map_z, stored, grid):
    return pl.pallas_call(
        functools.partial(assemble_kernel, grid),
        out_shape=[pltpu.VMEM((3, 8, 128), F32), pltpu.VMEM((112, 128), F32)],
        in_specs=vmem(3),
        out_specs=vmem(2),
        name="assemble",
    )(*here(got, map_z, stored))


def meet(low, high):
    return jnp.where(rows_of((8, 128), 1) < 64, low, high)


def fold_layers(spread, own, part, row_at, maps_at, above, below):
    lower = rows_of((8, 128), 1) < 64

    def pair(low, low_index, high, high_index, base):
        return jnp.concatenate([spread(low, low_index, base + 64, 64), spread(high, high_index, base, 64)], axis=1)

    def folded(home, x_ghosts, y_ghosts, map_x, map_y):
        sides = x_ghosts + pair(y_ghosts[-1], map_y(-1), y_ghosts[1], map_y(1), 128)
        return home + spread(y_ghosts[0], map_y(0), 0, 128) + spread(sides, map_x, 0, 128)

    y_ghosts = {dx: meet(part(dx, -1, 1), part(dx, 1, 1)) for dx in (-1, 0, 1)}
    x_ghosts = meet(part(-1, 0, 0), part(1, 0, 0))
    layers = [folded(own, x_ghosts, y_ghosts, maps_at(0)[6:7], lambda dx: maps_at(dx)[7:8])]
    for message, kept, at_row in ((above, lower, 10), (below, jnp.logical_not(lower), 11)):

        def sent(dx, dy, kept=kept):
            return jnp.where(kept, part(dx, dy, 2), 0.0), row_at(dx, dy, 9)

        y_ghosts = {dx: pair(*sent(dx, -1), *sent(dx, 1), 256) for dx in (-1, 0, 1)}
        x_ghosts = pair(*sent(-1, 0), *sent(1, 0), 128)
        home = spread(*sent(0, 0), 0, 128)
        layers.append(folded(home, x_ghosts, y_ghosts, message[8:9, :], lambda dx, at_row=at_row: row_at(dx, 0, at_row)))
    return layers


def fold_kernel(grid, own, got, maps, below, above, stored, gram, out):
    at = brick_reader(grid)
    blank = jnp.zeros((5, 128), F32)
    target = rows_of((128, 128))

    def spread(values, index, first, count):
        hi, lo = split(values)
        left = jnp.concatenate([hi.astype(F32), lo.astype(F32)], axis=0).astype(BF16)
        hot = jnp.where(jnp.broadcast_to(index.astype(jnp.int32) - first, (count, 128)) == target[0:count], 1.0, 0.0).astype(BF16)
        both = lax.dot_general(left, hot, NT, preferred_element_type=F32)
        return both[0:8] + both[8:16]

    def part(dx, dy, q):
        return turn(jnp.concatenate([at(got, dx, dy)[3 * q : 3 * q + 3], blank], axis=0))

    layers = fold_layers(
        spread, own[...], part, lambda dx, dy, r: at(got, dx, dy)[r : r + 1], lambda dx: at(maps, dx, 0), above, below
    )
    column = jnp.zeros((32, 128), F32)
    for c in range(3):
        at_rows = pl.ds(16 + 32 * c, 32)
        bases = (stored[c], above[at_rows, :], below[at_rows, :])
        for layer, vectors in zip(layers, bases):
            column = column + vectors * layer[c : c + 1]
    column = jnp.sum(column, axis=1, keepdims=True)
    lane = rows_of((32, 128), 1)
    full = jnp.where(lane == 30, column, gram[...])
    tail = jnp.where((lane >= 16) & (lane < 32), full, 0.0)
    first = full[0:4]
    for b in range(1, 4):
        first = first + pltpu.roll(full[4 * b : 4 * b + 4], 32 * b, 1)
    second = pltpu.roll(tail[16:18], 112, 1)
    for b in range(1, 8):
        second = second + pltpu.roll(tail[16 + 2 * b : 18 + 2 * b], 16 * (b - 1), 1)
    tile = [first, second] + [layer[0:3] for layer in layers] + [jnp.zeros((1, 128), F32)]
    out[...] = jnp.broadcast_to(jnp.concatenate(tile, axis=0)[None], out.shape)


def fold(own, got, maps, below, above, stored, gram, grid, copies):
    return pl.pallas_call(
        functools.partial(fold_kernel, grid),
        out_shape=pltpu.VMEM((copies, 16, 128), F32),
        in_specs=vmem(7),
        out_specs=vmem(1)[0],
        name="fold",
    )(*here(own, got, maps, below, above, stored, gram))


def column_kernel(got, product, out):
    count = got.shape[0]
    here_z = lax.axis_index("gz")

    def vector(z, before, after):
        return got[z, 6:9, :] + got[before, 9:12, :] + got[after, 12:15, :]

    product[...] = jnp.zeros_like(product)
    product[0:3, :] = vector(here_z, lax.rem(here_z + (count - 1), count), lax.rem(here_z + 1, count))
    squares = jnp.zeros((3, 128), F32)
    for z in range(count):
        value = vector(z, (z - 1) % count, (z + 1) % count)
        squares = squares + value * value
    size = jnp.sum(jnp.sum(squares, axis=1, keepdims=True), axis=0, keepdims=True)
    tile = got[0, 0:8, :]
    for z in range(1, count):
        tile = tile + got[z, 0:8, :]
    spot = (rows_of((8, 128)) == 4) & (rows_of((8, 128), 1) == 126)
    tile = jnp.where(spot, size, tile)
    out[...] = jnp.broadcast_to(tile[None], out.shape)


def column_of(got, bricks):
    return pl.pallas_call(
        column_kernel,
        out_shape=[pltpu.VMEM((8, 128), F32), pltpu.VMEM((bricks, 8, 128), F32)],
        in_specs=vmem(1),
        out_specs=vmem(2),
        name="column",
    )(*here(got))


def finish_kernel(entries, got, product, stored, result, correlations, norm):
    count = correlations.shape[1]
    packed = jnp.sum(got[...], axis=0) * (1.0 / entries)
    parts = [packed[0:4]] + [pltpu.roll(packed[0:4], 128 - 32 * b, 1) for b in range(1, 4)]
    parts += [pltpu.roll(packed[4:6], (144 - 16 * b) % 128, 1) for b in range(8)]
    full = jnp.concatenate(parts, axis=0)
    column = full[:, count : count + 1]
    line = jnp.sum(jnp.where(rows_of((32, 128)) == rows_of((32, 128), 1), column, 0.0), axis=0, keepdims=True)
    row = rows_of((32, 1))
    lane = rows_of((1, 128), 1)
    down = jnp.where(row < count, column, jnp.where(row == count, -1.0, 0.0))
    across = jnp.where(lane < count, line, jnp.where(lane == count, -2.0, 0.0))
    size = jnp.where(row < count, full * across * down, jnp.where((row == count) & (lane == count), full, 0.0))
    wide = rows_of((32, 128), 1)
    twice = jnp.where((row < 16) & (wide >= 16) & (wide < count), 2.0, 1.0)
    size = jnp.where((wide <= count) & ((row < 16) | (wide >= 16)), size * twice, 0.0)
    size = jnp.sum(jnp.sum(size, axis=1, keepdims=True), axis=0, keepdims=True)
    length = jnp.sqrt(jnp.maximum(size, 0.0) + 1e-06)
    norm[...] = length
    correlations[...] = line[:, 0:count]
    share = jnp.where(row < count, column, 0.0)
    for c in range(3):
        taken = jnp.sum(stored[c] * share, axis=0, keepdims=True)
        result[c, 0, 0] = (product[c : c + 1, :] - taken) / length


def finish(got, product, stored, shape, count, entries):
    return pl.pallas_call(
        functools.partial(finish_kernel, entries),
        out_shape=[
            jax.ShapeDtypeStruct(shape, F32),
            jax.ShapeDtypeStruct((1, count), F32),
            jax.ShapeDtypeStruct((1, 1), F32),
        ],
        in_specs=vmem(3),
        out_specs=vmem(3),
        name="finish",
    )(*here(got, product, stored))


def on_device(positions, basis, neighbours, used_count, kinds, map_x, map_y, map_z, table, fit_w1, fit_b1, fit_w2, fit_b2, fit_out):
    nx, ny, nz = (lax.axis_size(a) for a in ("gx", "gy", "gz"))
    plane = ("gx", "gy")
    up = [(i, (i + 1) % nz) for i in range(nz)]
    down = [(j, i) for i, j in up]

    def exchange(x):
        return lax.all_to_all(x, plane, 0, 0)

    packed = pack(positions, basis, map_x, map_y, nx * ny)
    raw = exchange(packed)
    table, _ = lax.optimization_barrier((table, packed))
    mixed, map_row, stored = mixing(table, fit_w1, map_z, basis)
    layers, lists, gram = lists_of(fit_w2, fit_b1, fit_b2, fit_out, neighbours, used_count, kinds, stored)
    raw, map_row = lax.optimization_barrier((raw, map_row))
    tiles, message = assemble(raw, map_row, stored, (nx, ny))
    below, above = lax.ppermute(message, "gz", up), lax.ppermute(message, "gz", down)
    own, shared = product(tiles, below, above, lists, (*mixed, *layers), nx * ny)
    summary = fold(own, exchange(shared), raw, below, above, stored, gram, (nx, ny), nz)
    hessian_vec, summary = column_of(lax.all_to_all(summary, "gz", 0, 0), nx * ny)
    summary = exchange(summary)
    entries = 3 * positions.shape[-1] * nx * ny * nz
    next_vector, correlations, vector_norm = finish(summary, hessian_vec, stored, positions.shape, basis.shape[0], entries)
    return next_vector, correlations.reshape(-1), vector_norm.reshape(())


def solution(mesh):
    bricks = P("gx", "gy", "gz", None)
    lists = P("gx", "gy", "gz", None, None)
    vector = P(None, "gx", "gy", "gz", None)
    return jax.shard_map(
        on_device,
        mesh=mesh,
        in_specs=(vector, P(None, None, "gx", "gy", "gz", None), lists, bricks, bricks, lists, lists, lists) + (P(),) * 6,
        out_specs=(vector, P(), P()),
        check_vma=False,
    )
```

```python
import functools

import jax
import jax.numpy as jnp
from jax import lax
from jax.experimental import pallas as pl
from jax.experimental.pallas import tpu as pltpu
from jax.sharding import PartitionSpec as P

F32 = jnp.float32
BF16 = jnp.bfloat16
LOG2E = 1.4426950408889634
NT = (((1,), (1,)), ((), ()))


def split(x):
    hi = x.astype(BF16)
    return hi, (x - hi.astype(F32)).astype(BF16)


def mm(a, b):
    return jnp.dot(a, b, preferred_element_type=F32)


def dot3(a, b):
    ah, al = a if isinstance(a, tuple) else split(a)
    bh, bl = b if isinstance(b, tuple) else split(b)
    return mm(ah, bh) + (mm(ah, bl) + mm(al, bh))


def lane_pick(table, index):
    return jnp.take_along_axis(table, index, axis=1, mode="promise_in_bounds")


def rows_of(shape, dim=0):
    return lax.broadcasted_iota(jnp.int32, shape, dim)


def halves(ref):
    return jnp.concatenate([ref[0, 0, 0, 0:1, :], ref[0, 0, 0, 1:2, :]], axis=1)


def fetch(sources, places, semaphores):
    copies = [pltpu.make_async_copy(x, y, semaphores.at[i]) for i, (x, y) in enumerate(zip(sources, places))]
    for copy in copies:
        copy.start()
    return copies


EXACT = dict(precision=lax.Precision.HIGHEST, preferred_element_type=F32)


def mixing_kernel(table_at, w1_at, map_at, basis_at, u_hi, u_lo, ut_hi, ut_lo, map_row, stored, table, w1t, map_z, basis, outer, inner, k_hi, k_lo, semaphores):
    copies = fetch((table_at, map_at, w1_at, basis_at), (table, map_z, w1t, basis), semaphores)
    stored[...] = jnp.zeros_like(stored)
    types, levels, width = table.shape
    hidden = w1t.shape[0]
    m2 = w1t.shape[1] // width
    count = types * levels * levels
    copies[0].wait()
    tall = table[...].reshape(types * levels, width)
    tall = jnp.concatenate([tall, jnp.zeros((types * levels, 128 - width), F32)], axis=1)
    tall = jnp.concatenate([tall, jnp.zeros((128 - types * levels, 128), F32)], axis=0).T
    column = rows_of((128, count), 1)
    row = rows_of((128, count))
    kind = column // (levels * levels)
    first = jnp.where(row == kind * levels + (column // levels) % levels, 1.0, 0.0)
    second = jnp.where(row == kind * levels + column % levels, 1.0, 0.0)
    outer[...] = jnp.dot(tall, first, **EXACT) * 0.5
    inner[...] = jnp.dot(tall, second, **EXACT) * 0.5
    near = inner[0:m2, :] * 2.0
    far = outer[0:m2, :] * 2.0

    def kron(m, carry):
        value = jnp.broadcast_to(outer[pl.ds(m, 1), :], (m2, count)) * near + jnp.broadcast_to(inner[pl.ds(m, 1), :], (m2, count)) * far
        hi, lo = split(value)
        at = pl.ds(pl.multiple_of(m * m2, m2), m2)
        k_hi[at, :] = hi
        k_lo[at, :] = lo
        return carry

    lax.fori_loop(0, width, kron, 0, unroll=4)
    copies[1].wait()
    map_row[...] = halves(map_z)
    copies[3].wait()
    for c in range(3):
        for k in range(basis.shape[0]):
            stored[c, k : k + 1, :] = basis[k, c, 0, 0]
    copies[2].wait()
    full = dot3(w1t[...], (k_hi[...], k_lo[...]))
    full = jnp.concatenate([full, jnp.zeros((256 - hidden, count), F32)], axis=0)
    hi, lo = split(full)
    ut_hi[...] = hi
    ut_lo[...] = lo
    hi, lo = split(full.T)
    u_hi[...] = hi
    u_lo[...] = lo


def lists_kernel(w2_at, b1_at, b2_at, wo_at, ids_at, counts_at, kinds_at, stored, w2_hi, w2_lo, w2t_hi, w2t_lo, cols, ids_t, count_row, kind_row, gram, w2, b1, b2, wo, ids, counts, kinds, pad, semaphores):
    places = (w2, b1, b2, wo, ids, counts, kinds)
    copies = fetch((w2_at, b1_at, b2_at, wo_at, ids_at, counts_at, kinds_at), places, semaphores)
    hidden = w2.shape[0]
    pad[...] = jnp.zeros_like(pad)
    gram[...] = jnp.zeros_like(gram)
    for copy in copies:
        copy.wait()
    pad[0:hidden, 0:hidden] = w2[...]
    hi, lo = split(pad[...])
    w2_hi[...] = hi
    w2_lo[...] = lo
    hi, lo = split(pad[...].T)
    w2t_hi[...] = hi
    w2t_lo[...] = lo
    pad[0:128, :] = jnp.zeros((128, pad.shape[1]), F32)
    pad[0:1, 0:hidden] = b1[...]
    pad[1:2, 0:hidden] = b2[...]
    pad[2:3, 0:hidden] = wo[...]
    cols[...] = pad[0:128, :].T
    ids_t[...] = ids[0, 0, 0].astype(F32).T.astype(jnp.int32)
    count_row[...] = counts[0, 0]
    kind_row[...] = kinds[0, 0]
    total = jnp.zeros((32, 32), F32)
    for c in range(3):
        total = total + lax.dot_general(stored[c], stored[c], NT, **EXACT)
    gram[:, 0:32] = total


def vmem(n):
    return [pl.BlockSpec(memory_space=pltpu.VMEM)] * n


def here(*arrays):
    return [pltpu.with_memory_space_constraint(a, pltpu.VMEM) for a in arrays]


def from_hbm(kernel, name, shapes, scratch, *arrays, held=()):
    return pl.pallas_call(
        kernel,
        out_shape=[pltpu.VMEM(s, d) for s, d in shapes],
        in_specs=[pl.BlockSpec(memory_space=pltpu.HBM)] * len(arrays) + vmem(len(held)),
        out_specs=vmem(len(shapes)),
        scratch_shapes=[pltpu.VMEM(a.shape, a.dtype) for a in arrays] + scratch + [pltpu.SemaphoreType.DMA((len(arrays),))],
        name=name,
    )(*(pltpu.with_memory_space_constraint(a, pltpu.HBM) for a in arrays), *here(*held))


def mixing(table, w1, map_z, basis):
    hp = 256
    count = table.shape[0] * table.shape[1] ** 2
    shapes = [((count, hp), BF16)] * 2 + [((hp, count), BF16)] * 2 + [((1, 128), jnp.int32), ((3, 32, 128), F32)]
    scratch = [pltpu.VMEM((128, count), F32)] * 2 + [pltpu.VMEM((w1.shape[0], count), BF16)] * 2
    *weights, map_row, stored = from_hbm(mixing_kernel, "mixing", shapes, scratch, table, w1.T, map_z, basis)
    return weights, map_row, stored


def lists_of(w2, b1, b2, wo, ids, counts, kinds, stored):
    hp = 256
    row = ((1, 128), jnp.int32)
    shapes = [((hp, hp), BF16)] * 4 + [((hp, 128), F32), ((ids.shape[-1], 128), jnp.int32), row, row, ((32, 128), F32)]
    scratch = [pltpu.VMEM((hp, hp), F32)]
    done = from_hbm(lists_kernel, "lists", shapes, scratch, w2, b1[None], b2[None], wo[None], ids, counts, kinds, held=(stored,))
    return done[:5], done[5:8], done[8]


def shifted_ghosts(below, above, coord, rows):
    lower = rows_of((rows, 128), 1) < 64
    step = jnp.where(rows_of((rows, 128)) == coord, 1.0, 0.0)
    return jnp.where(lower, below - step, above + step)


def product_kernel(tiles, below, above, ids_t, counts, kinds, u_hi, u_lo, ut_hi, ut_lo, w2_hi, w2_lo, w2t_hi, w2t_lo, cols, out, sent, xv, edge, phis, acc, pairs, grads, force, lows):
    n_slots = ids_t.shape[0]
    levels = 16
    gap = levels - 1
    blocks = n_slots // 8
    xv[0:3] = tiles[...]
    xv[3] = shifted_ghosts(pltpu.roll(below[0:8, :], 64, 1), pltpu.roll(above[0:8, :], 64, 1), 2, 8)
    count_row = jnp.broadcast_to(counts[...], (8, 128))

    def geometry(nb, carry):
        rows = pl.ds(pl.multiple_of(nb * 8, 8), 8)
        index = ids_t[rows, :]
        low = index & 127
        high = index >> 7
        lows[rows, :] = (index & 63).astype(F32)
        near = []
        for f in range(6):
            picks = [lane_pick(jnp.broadcast_to(xv[q, f : f + 1, :], (8, 128)), low) for q in range(4)]
            value = jnp.where(high < 2, jnp.where(high == 0, picks[0], picks[1]), jnp.where(high == 2, picks[2], picks[3]))
            near.append(value - jnp.broadcast_to(xv[0, f : f + 1, :], (8, 128)))
        d, dd = near[:3], near[3:]
        square = d[0] * d[0] + d[1] * d[1] + d[2] * d[2]
        rate = 2.0 * (d[0] * dd[0] + d[1] * dd[1] + d[2] * dd[2])
        wide = square + 0.01
        inverse = lax.rsqrt(wide)
        half = 0.5 / wide
        live = (rows_of((8, 128)) + nb * 8) < count_row
        s = jnp.where(live, jnp.exp(-square) * inverse, 0.0)
        tau = s * inverse
        sq = -s * (1.0 + half)
        tq = -tau * (1.0 + 2.0 * half)
        share = 1.0 / (1.0 + s)
        us = gap * share * share
        for c in range(3):
            edge[c, rows, :] = d[c]
            edge[3 + c, rows, :] = dd[c]
            edge[9 + c, rows, :] = tau * d[c]
            edge[13 + c, rows, :] = tq * rate * d[c] + tau * dd[c]
        edge[6, rows, :] = gap * s * share
        edge[7, rows, :] = us * sq * rate
        edge[8, rows, :] = s
        edge[12, rows, :] = sq * rate
        edge[16, rows, :] = tau
        edge[17, rows, :] = half
        edge[18, rows, :] = rate
        return carry

    lax.fori_loop(0, blocks, geometry, 0, unroll=16)

    def pooling(kk, carry):
        sums = [[jnp.zeros((8, 128), F32) for _ in range(8)] for _ in range(2)]
        for nb in range(blocks):
            rows = pl.ds(nb * 8, 8)
            u = edge[6, rows, :]
            w = -2.0 * edge[7, rows, :]
            radial = [edge[8 + a, rows, :] for a in range(4)]
            moved = [edge[12 + a, rows, :] for a in range(4)]
            for side in range(2):
                z = u - (2 * kk + side).astype(F32)
                phi = jnp.exp2(z * (z * (-LOG2E)))
                phis[2 * kk + side, rows, :] = phi
                dphi = phi * (z * w)
                for a in range(4):
                    sums[side][a] = sums[side][a] + phi * radial[a]
                    sums[side][4 + a] = sums[side][4 + a] + (dphi * radial[a] + phi * moved[a])
        for side in range(2):
            for a in range(8):
                acc[pl.ds(pl.multiple_of((a * levels + 2 * kk + side) * 8, 8), 8), :] = sums[side][a]
        return carry

    lax.fori_loop(0, levels // 2, pooling, 0)
    pooled = acc[pl.ds(0, 128, stride=8), :]
    for s in range(1, 8):
        pooled = pooled + acc[pl.ds(s, 128, stride=8), :]
    pooled = pooled * (1.0 / n_slots)
    grads[...] = pooled
    kind = jnp.concatenate([kinds[...], kinds[...]], axis=1)
    p = [pooled[a * 16 : (a + 1) * 16] for a in range(4)]
    dp = [pooled[64 + a * 16 : 64 + (a + 1) * 16] for a in range(4)]
    for k in range(levels):
        value = jnp.zeros((16, 128), F32)
        moved = jnp.zeros((16, 128), F32)
        for a in range(4):
            value = value + p[a] * jnp.broadcast_to(grads[a * 16 + k : a * 16 + k + 1, :], (16, 128))
            moved = moved + p[a] * jnp.broadcast_to(grads[64 + a * 16 + k : 64 + a * 16 + k + 1, :], (16, 128))
        pairs[k * 16 : (k + 1) * 16, 0:128] = value
        pairs[k * 16 : (k + 1) * 16, 128:256] = 2.0 * moved
    both = split(pairs[...])
    z1 = jnp.where(
        kind == 1,
        dot3((ut_hi[:, 256:512], ut_lo[:, 256:512]), both),
        dot3((ut_hi[:, 0:256], ut_lo[:, 0:256]), both),
    )
    h1 = jnp.tanh(z1[:, 0:128] + cols[:, 0:1])
    slope1 = 1.0 - h1 * h1
    dh1 = slope1 * z1[:, 128:256]
    z2 = dot3((w2t_hi[...], w2t_lo[...]), jnp.concatenate([h1, dh1], axis=1))
    t2 = jnp.tanh(z2[:, 0:128] + cols[:, 1:2])
    slope2 = 1.0 - t2 * t2
    read = cols[:, 2:3]
    delta2 = slope2 * read
    ddelta2 = -2.0 * t2 * (slope2 * z2[:, 128:256]) * read
    back = dot3((w2_hi[...], w2_lo[...]), jnp.concatenate([delta2, ddelta2], axis=1))
    e1 = back[:, 0:128] + read
    delta1 = slope1 * e1
    ddelta1 = slope1 * back[:, 128:256] - 2.0 * h1 * dh1 * e1
    both = split(jnp.concatenate([delta1, ddelta1], axis=1))
    pairs[...] = jnp.where(
        kind == 1,
        dot3((u_hi[256:512, :], u_lo[256:512, :]), both),
        dot3((u_hi[0:256, :], u_lo[0:256, :]), both),
    )
    g = [jnp.zeros((16, 128), F32) for _ in range(4)]
    dg = [jnp.zeros((16, 128), F32) for _ in range(4)]
    for k in range(levels):
        m = pairs[k * 16 : (k + 1) * 16, 0:128]
        dm = pairs[k * 16 : (k + 1) * 16, 128:256]
        for a in range(4):
            row = jnp.broadcast_to(grads[a * 16 + k : a * 16 + k + 1, :], (16, 128))
            drow = jnp.broadcast_to(grads[64 + a * 16 + k : 64 + a * 16 + k + 1, :], (16, 128))
            g[a] = g[a] + m * row
            dg[a] = dg[a] + (dm * row + m * drow)
    scale = 2.0 / n_slots
    for a in range(4):
        grads[a * 16 : (a + 1) * 16, :] = g[a] * scale
        grads[64 + a * 16 : 64 + (a + 1) * 16, :] = dg[a] * scale

    def backward(nb, centre):
        rows = pl.ds(pl.multiple_of(nb * 8, 8), 8)
        u = edge[6, rows, :]
        zero = jnp.zeros((8, 128), F32)
        s0, s1, s2, r0, r1 = ([zero] * 4 for _ in range(5))
        for k in range(levels):
            z = u - float(k)
            phi = phis[k, rows, :]
            phi1 = z * phi
            phi2 = z * phi1
            for a in range(4):
                row = jnp.broadcast_to(grads[a * 16 + k : a * 16 + k + 1, :], (8, 128))
                drow = jnp.broadcast_to(grads[64 + a * 16 + k : 64 + a * 16 + k + 1, :], (8, 128))
                s0[a] = s0[a] + row * phi
                s1[a] = s1[a] + row * phi1
                s2[a] = s2[a] + row * phi2
                r0[a] = r0[a] + drow * phi
                r1[a] = r1[a] + drow * phi1
        d = [edge[c, rows, :] for c in range(3)]
        dd = [edge[3 + c, rows, :] for c in range(3)]
        du = edge[7, rows, :]
        radial = [edge[8 + a, rows, :] for a in range(4)]
        moved = [edge[12 + a, rows, :] for a in range(4)]
        s = radial[0]
        tau = edge[16, rows, :]
        half = edge[17, rows, :]
        rate = edge[18, rows, :]
        one = 1.0 + half
        two = one + half
        sq = -s * one
        sqq = s * (one * one + 2.0 * half * half)
        tq = -tau * two
        tqq = tau * (two * two + 4.0 * half * half)
        share = 1.0 / (1.0 + s)
        us = gap * share * share
        uq = us * sq
        uqq = us * (sqq - 2.0 * share * sq * sq)
        a1 = [-2.0 * v for v in s1]
        da = [r0[a] + a1[a] * du for a in range(4)]
        da1 = [-2.0 * r1[a] + (4.0 * s2[a] - 2.0 * s0[a]) * du for a in range(4)]
        a1r = a1[0] * radial[0] + a1[1] * radial[1] + (a1[2] * radial[2] + a1[3] * radial[3])
        ad = s0[1] * d[0] + s0[2] * d[1] + s0[3] * d[2]
        turned = da1[0] * radial[0] + a1[0] * moved[0]
        for a in range(1, 4):
            turned = turned + (da1[a] * radial[a] + a1[a] * moved[a])
        dad = da[1] * d[0] + s0[1] * dd[0]
        for c in range(1, 3):
            dad = dad + (da[c + 1] * d[c] + s0[c + 1] * dd[c])
        eq = uq * a1r + sq * s0[0] + tq * ad
        deq = rate * (uqq * a1r + sqq * s0[0] + tqq * ad) + uq * turned + sq * da[0] + tq * dad
        dtau = tq * rate
        result = []
        for c in range(3):
            value = 2.0 * (dd[c] * eq + d[c] * deq) + (dtau * s0[c + 1] + tau * da[c + 1])
            hi = value.astype(BF16).astype(F32)
            force[c, rows, :] = hi
            force[3 + c, rows, :] = value - hi
            result.append(centre[c] + value)
        return tuple(result)

    zero = jnp.zeros((8, 128), F32)
    centre = lax.fori_loop(0, blocks, backward, (zero, zero, zero), unroll=8)
    row8 = rows_of((8, 128))
    rows16 = [(rows_of((16, 128)) + 16 * rg).astype(F32).astype(BF16) for rg in range(4)]
    on = jnp.ones((16, 128), BF16)
    off = jnp.zeros((16, 128), BF16)
    chunk = 32

    def scatter(step, total):
        lefts, hots = [], []
        for i in range(chunk):
            n = step * chunk + i
            hit = (jnp.broadcast_to(ids_t[pl.ds(n, 1), :], (8, 128)) >> 6) == row8
            stack = [jnp.where(hit, jnp.broadcast_to(force[c, pl.ds(n, 1), :], (8, 128)), 0.0) for c in range(6)]
            lefts.append(jnp.concatenate(stack, axis=0).astype(BF16))
            low = jnp.broadcast_to(lows[pl.ds(n, 1), :], (16, 128)).astype(BF16)
            hots.append(jnp.concatenate([jnp.where(low == r, on, off) for r in rows16], axis=0))
        return total + lax.dot_general(jnp.concatenate(lefts, axis=1), jnp.concatenate(hots, axis=1), NT, preferred_element_type=F32)

    total = lax.fori_loop(0, n_slots // chunk, scatter, jnp.zeros((48, 64), F32), unroll=2)
    out[...] = jnp.zeros_like(out)
    rows = {}
    for c in range(3):
        both = total[c * 8 : c * 8 + 8] + total[24 + c * 8 : 32 + c * 8]
        for q in range(4):
            rows[q, c] = jnp.concatenate([both[2 * q : 2 * q + 1], both[2 * q + 1 : 2 * q + 2]], axis=1)
        out[c : c + 1, :] = rows[0, c] - jnp.sum(centre[c], axis=0, keepdims=True)
    half = rows_of((1, 128), 1) < 64
    tile = [rows[q, c] for q in range(1, 4) for c in range(3)]
    tile += [jnp.where(half, above[10:11, :], below[10:11, :]), above[9:10, :], below[9:10, :], jnp.zeros((4, 128), F32)]
    sent[...] = jnp.broadcast_to(jnp.concatenate(tile, axis=0)[None], sent.shape)


def product(tiles, below, above, lists, weights, bricks):
    n = lists[0].shape[0]
    return pl.pallas_call(
        product_kernel,
        out_shape=[pltpu.VMEM((8, 128), F32), pltpu.VMEM((bricks, 16, 128), F32)],
        in_specs=vmem(15),
        out_specs=vmem(2),
        scratch_shapes=[
            pltpu.VMEM((4, 8, 128), F32),
            pltpu.VMEM((19, n, 128), F32),
            pltpu.VMEM((16, n, 128), F32),
            pltpu.VMEM((1024, 128), F32),
            pltpu.VMEM((256, 256), F32),
            pltpu.VMEM((128, 128), F32),
            pltpu.VMEM((6, n, 128), F32),
            pltpu.VMEM((n, 128), F32),
        ],
        name="product",
    )(*here(tiles, below, above, *lists, *weights))


def pack_kernel(places_at, basis_at, map_x_at, map_y_at, out, places, tangent, map_x, map_y, semaphores):
    last = basis_at.shape[0] - 1
    copies = fetch((places_at, basis_at.at[last], map_x_at, map_y_at), (places, tangent, map_x, map_y), semaphores)
    for copy in copies:
        copy.wait()
    rows = [places[c, 0, 0] for c in range(3)] + [tangent[c, 0, 0] for c in range(3)]
    rows += [halves(m).astype(F32) for m in (map_x, map_y)]
    out[...] = jnp.broadcast_to(jnp.concatenate(rows, axis=0)[None], out.shape)


def pack(positions, basis, map_x, map_y, bricks):
    arrays = (positions, basis, map_x, map_y)
    return pl.pallas_call(
        pack_kernel,
        out_shape=pltpu.VMEM((bricks, 8, 128), F32),
        in_specs=[pl.BlockSpec(memory_space=pltpu.HBM)] * 4,
        out_specs=vmem(1)[0],
        scratch_shapes=[
            pltpu.VMEM(positions.shape, F32),
            pltpu.VMEM(basis.shape[1:], F32),
            pltpu.VMEM(map_x.shape, jnp.int32),
            pltpu.VMEM(map_y.shape, jnp.int32),
            pltpu.SemaphoreType.DMA((4,)),
        ],
        name="pack",
    )(*(pltpu.with_memory_space_constraint(a, pltpu.HBM) for a in arrays))


def brick_reader(grid):
    nx, ny = grid
    px, py = lax.axis_index("gx"), lax.axis_index("gy")

    def at(ref, dx, dy):
        x = lax.rem(px + (dx + nx), nx)
        y = lax.rem(py + (dy + ny), ny)
        return ref[x * ny + y]

    return at


def as_index(row):
    return jnp.broadcast_to(row, (8, 128)).astype(jnp.int32)


def turn(x):
    return pltpu.roll(x, 64, 1)


def assemble_kernel(grid, got, map_z, stored, tiles, message):
    at = brick_reader(grid)
    lower = rows_of((8, 128), 1) < 64
    row = rows_of((8, 128))
    step_x = jnp.where(row == 0, 1.0, 0.0)
    step_y = jnp.where(row == 1, 1.0, 0.0)
    middle, ghosts, index = {}, {}, {}
    for dy in (-1, 0, 1):
        own, low, high = (at(got, dx, dy) for dx in (0, -1, 1))
        from_low = lane_pick(low, turn(as_index(low[6:7])))
        from_high = lane_pick(high, turn(as_index(high[6:7])))
        middle[dy] = own
        ghosts[dy] = jnp.where(lower, from_low - step_x, from_high + step_x)
        index[dy] = turn(as_index(own[7:8]))

    def second(dy):
        low = index[dy] & 127
        return jnp.where(index[dy] < 128, lane_pick(middle[dy], low), lane_pick(ghosts[dy], low))

    third = jnp.where(lower, second(-1) - step_y, second(1) + step_y)
    tiles[0] = middle[0]
    tiles[1] = ghosts[0]
    tiles[2] = third
    chosen = jnp.broadcast_to(map_z[...], (8, 128))
    low = chosen & 127
    message[0:8, :] = jnp.where(
        chosen < 128, lane_pick(middle[0], low), jnp.where(chosen < 256, lane_pick(ghosts[0], low), lane_pick(third, low))
    )
    message[8:16, :] = jnp.concatenate([middle[0][6:8], map_z[...].astype(F32), jnp.zeros((5, 128), F32)], axis=0)
    for c in range(3):
        message[16 + 32 * c : 48 + 32 * c, :] = stored[c]


def assemble(got, map_z, stored, grid):
    return pl.pallas_call(
        functools.partial(assemble_kernel, grid),
        out_shape=[pltpu.VMEM((3, 8, 128), F32), pltpu.VMEM((112, 128), F32)],
        in_specs=vmem(3),
        out_specs=vmem(2),
        name="assemble",
    )(*here(got, map_z, stored))


def meet(low, high):
    return jnp.where(rows_of((8, 128), 1) < 64, low, high)


def fold_layers(spread, own, part, row_at, maps_at, above, below):
    lower = rows_of((8, 128), 1) < 64

    def pair(low, low_index, high, high_index, base):
        return jnp.concatenate([spread(low, low_index, base + 64, 64), spread(high, high_index, base, 64)], axis=1)

    def folded(home, x_ghosts, y_ghosts, map_x, map_y):
        sides = x_ghosts + pair(y_ghosts[-1], map_y(-1), y_ghosts[1], map_y(1), 128)
        return home + spread(y_ghosts[0], map_y(0), 0, 128) + spread(sides, map_x, 0, 128)

    y_ghosts = {dx: meet(part(dx, -1, 1), part(dx, 1, 1)) for dx in (-1, 0, 1)}
    x_ghosts = meet(part(-1, 0, 0), part(1, 0, 0))
    layers = [folded(own, x_ghosts, y_ghosts, maps_at(0)[6:7], lambda dx: maps_at(dx)[7:8])]
    for message, kept, at_row in ((above, lower, 10), (below, jnp.logical_not(lower), 11)):

        def sent(dx, dy, kept=kept):
            return jnp.where(kept, part(dx, dy, 2), 0.0), row_at(dx, dy, 9)

        y_ghosts = {dx: pair(*sent(dx, -1), *sent(dx, 1), 256) for dx in (-1, 0, 1)}
        x_ghosts = pair(*sent(-1, 0), *sent(1, 0), 128)
        home = spread(*sent(0, 0), 0, 128)
        layers.append(folded(home, x_ghosts, y_ghosts, message[8:9, :], lambda dx, at_row=at_row: row_at(dx, 0, at_row)))
    return layers


def fold_kernel(grid, own, got, maps, below, above, stored, gram, out):
    at = brick_reader(grid)
    blank = jnp.zeros((5, 128), F32)
    target = rows_of((128, 128))

    def spread(values, index, first, count):
        hi, lo = split(values)
        left = jnp.concatenate([hi.astype(F32), lo.astype(F32)], axis=0).astype(BF16)
        hot = jnp.where(jnp.broadcast_to(index.astype(jnp.int32) - first, (count, 128)) == target[0:count], 1.0, 0.0).astype(BF16)
        both = lax.dot_general(left, hot, NT, preferred_element_type=F32)
        return both[0:8] + both[8:16]

    def part(dx, dy, q):
        return turn(jnp.concatenate([at(got, dx, dy)[3 * q : 3 * q + 3], blank], axis=0))

    layers = fold_layers(
        spread, own[...], part, lambda dx, dy, r: at(got, dx, dy)[r : r + 1], lambda dx: at(maps, dx, 0), above, below
    )
    column = jnp.zeros((32, 128), F32)
    for c in range(3):
        at_rows = pl.ds(16 + 32 * c, 32)
        bases = (stored[c], above[at_rows, :], below[at_rows, :])
        for layer, vectors in zip(layers, bases):
            column = column + vectors * layer[c : c + 1]
    column = jnp.sum(column, axis=1, keepdims=True)
    lane = rows_of((32, 128), 1)
    full = jnp.where(lane == 30, column, gram[...])
    tail = jnp.where((lane >= 16) & (lane < 32), full, 0.0)
    first = full[0:4]
    for b in range(1, 4):
        first = first + pltpu.roll(full[4 * b : 4 * b + 4], 32 * b, 1)
    second = pltpu.roll(tail[16:18], 112, 1)
    for b in range(1, 8):
        second = second + pltpu.roll(tail[16 + 2 * b : 18 + 2 * b], 16 * (b - 1), 1)
    tile = [first, second] + [layer[0:3] for layer in layers] + [jnp.zeros((1, 128), F32)]
    out[...] = jnp.broadcast_to(jnp.concatenate(tile, axis=0)[None], out.shape)


def fold(own, got, maps, below, above, stored, gram, grid, copies):
    return pl.pallas_call(
        functools.partial(fold_kernel, grid),
        out_shape=pltpu.VMEM((copies, 16, 128), F32),
        in_specs=vmem(7),
        out_specs=vmem(1)[0],
        name="fold",
    )(*here(own, got, maps, below, above, stored, gram))


def column_kernel(got, product, out):
    count = got.shape[0]
    here_z = lax.axis_index("gz")

    def vector(z, before, after):
        return got[z, 6:9, :] + got[before, 9:12, :] + got[after, 12:15, :]

    product[...] = jnp.zeros_like(product)
    product[0:3, :] = vector(here_z, lax.rem(here_z + (count - 1), count), lax.rem(here_z + 1, count))
    squares = jnp.zeros((3, 128), F32)
    for z in range(count):
        value = vector(z, (z - 1) % count, (z + 1) % count)
        squares = squares + value * value
    size = jnp.sum(jnp.sum(squares, axis=1, keepdims=True), axis=0, keepdims=True)
    tile = got[0, 0:8, :]
    for z in range(1, count):
        tile = tile + got[z, 0:8, :]
    spot = (rows_of((8, 128)) == 4) & (rows_of((8, 128), 1) == 126)
    tile = jnp.where(spot, size, tile)
    out[...] = jnp.broadcast_to(tile[None], out.shape)


def column_of(got, bricks):
    return pl.pallas_call(
        column_kernel,
        out_shape=[pltpu.VMEM((8, 128), F32), pltpu.VMEM((bricks, 8, 128), F32)],
        in_specs=vmem(1),
        out_specs=vmem(2),
        name="column",
    )(*here(got))


def finish_kernel(entries, got, product, stored, result, correlations, norm):
    count = correlations.shape[1]
    packed = jnp.sum(got[...], axis=0) * (1.0 / entries)
    parts = [packed[0:4]] + [pltpu.roll(packed[0:4], 128 - 32 * b, 1) for b in range(1, 4)]
    parts += [pltpu.roll(packed[4:6], (144 - 16 * b) % 128, 1) for b in range(8)]
    full = jnp.concatenate(parts, axis=0)
    column = full[:, count : count + 1]
    line = jnp.sum(jnp.where(rows_of((32, 128)) == rows_of((32, 128), 1), column, 0.0), axis=0, keepdims=True)
    row = rows_of((32, 1))
    lane = rows_of((1, 128), 1)
    down = jnp.where(row < count, column, jnp.where(row == count, -1.0, 0.0))
    across = jnp.where(lane < count, line, jnp.where(lane == count, -2.0, 0.0))
    size = jnp.where(row < count, full * across * down, jnp.where((row == count) & (lane == count), full, 0.0))
    wide = rows_of((32, 128), 1)
    twice = jnp.where((row < 16) & (wide >= 16) & (wide < count), 2.0, 1.0)
    size = jnp.where((wide <= count) & ((row < 16) | (wide >= 16)), size * twice, 0.0)
    size = jnp.sum(jnp.sum(size, axis=1, keepdims=True), axis=0, keepdims=True)
    length = jnp.sqrt(jnp.maximum(size, 0.0) + 1e-06)
    norm[...] = length
    correlations[...] = line[:, 0:count]
    share = jnp.where(row < count, column, 0.0)
    for c in range(3):
        taken = jnp.sum(stored[c] * share, axis=0, keepdims=True)
        result[c, 0, 0] = (product[c : c + 1, :] - taken) / length


def finish(got, product, stored, shape, count, entries):
    return pl.pallas_call(
        functools.partial(finish_kernel, entries),
        out_shape=[
            jax.ShapeDtypeStruct(shape, F32),
            jax.ShapeDtypeStruct((1, count), F32),
            jax.ShapeDtypeStruct((1, 1), F32),
        ],
        in_specs=vmem(3),
        out_specs=vmem(3),
        name="finish",
    )(*here(got, product, stored))


def on_device(positions, basis, neighbours, used_count, kinds, map_x, map_y, map_z, table, fit_w1, fit_b1, fit_w2, fit_b2, fit_out):
    nx, ny, nz = (lax.axis_size(a) for a in ("gx", "gy", "gz"))
    plane = ("gx", "gy")
    up = [(i, (i + 1) % nz) for i in range(nz)]
    down = [(j, i) for i, j in up]

    def exchange(x):
        return lax.all_to_all(x, plane, 0, 0)

    packed = pack(positions, basis, map_x, map_y, nx * ny)
    raw = exchange(packed)
    table, _ = lax.optimization_barrier((table, packed))
    mixed, map_row, stored = mixing(table, fit_w1, map_z, basis)
    layers, lists, gram = lists_of(fit_w2, fit_b1, fit_b2, fit_out, neighbours, used_count, kinds, stored)
    raw, map_row = lax.optimization_barrier((raw, map_row))
    tiles, message = assemble(raw, map_row, stored, (nx, ny))
    below, above = lax.ppermute(message, "gz", up), lax.ppermute(message, "gz", down)
    own, shared = product(tiles, below, above, lists, (*mixed, *layers), nx * ny)
    summary = fold(own, exchange(shared), raw, below, above, stored, gram, (nx, ny), nz)
    hessian_vec, summary = column_of(lax.all_to_all(summary, "gz", 0, 0), nx * ny)
    summary = exchange(summary)
    entries = 3 * positions.shape[-1] * nx * ny * nz
    next_vector, correlations, vector_norm = finish(summary, hessian_vec, stored, positions.shape, basis.shape[0], entries)
    return next_vector, correlations.reshape(-1), vector_norm.reshape(())


def solution(mesh):
    bricks = P("gx", "gy", "gz", None)
    lists = P("gx", "gy", "gz", None, None)
    vector = P(None, "gx", "gy", "gz", None)
    return jax.shard_map(
        on_device,
        mesh=mesh,
        in_specs=(vector, P(None, None, "gx", "gy", "gz", None), lists, bricks, bricks, lists, lists, lists) + (P(),) * 6,
        out_specs=(vector, P(), P()),
        check_vma=False,
    )
```
